32 devices in a mesh: seq: 8 (over z, x), fsdp: 4 (over y, core).
Axes of the slice: x: 2, y: 2, z: 4, core: 2. Of those that a mesh axis runs over, the one named last changes fastest.
Arguments:
- tokens: bfloat16 [4, 1024, 1536], P('fsdp', 'seq'), may hold values from -6 to 6
- in_weight: bfloat16 [1536, 6400], P('fsdp'), may hold values from -0.15625 to 0.15625
- step_weight: bfloat16 [1536, 48], P('fsdp'), may hold values from -0.15625 to 0.15625
- conv_kernel: bfloat16 [4, 3328], P(None, 'fsdp'), may hold values from -3 to 3
- conv_bias: bfloat16 [3328], P('fsdp'), may hold values from -3 to 3
- step_bias: bfloat16 [48], P('fsdp'), may hold values from -6 to -3
- log_decay: bfloat16 [48], P('fsdp'), may hold values from -7 to 1
- skip_gain: bfloat16 [48], P('fsdp'), may hold values from 0.5 to 1.5
- gate_gain: bfloat16 [3072], P('fsdp'), may hold values from 0.5 to 1.5
- norm_gain: bfloat16 [1536], P('fsdp'), may hold values from 0.5 to 1.5
- out_weight: bfloat16 [3072, 1536], P('fsdp'), may hold values from -0.109375 to 0.109375
- cotangent: bfloat16 [4, 1024, 1536], P('fsdp', 'seq'), may hold values from -6 to 6
Outputs:
- block_out: bfloat16 [4, 1024, 1536], P('fsdp', 'seq')
- input_grad: float32 [4, 1024, 1536], P('fsdp', 'seq')
- in_weight_grad: float32 [1536, 6400], P('fsdp')
- step_weight_grad: float32 [1536, 48], P('fsdp')
- conv_kernel_grad: float32 [4, 3328], P(None, 'fsdp')
- conv_bias_grad: float32 [3328], P('fsdp')
- step_bias_grad: float32 [48], P('fsdp')
- log_decay_grad: float32 [48], P('fsdp')
- skip_gain_grad: float32 [48], P('fsdp')
- gate_gain_grad: float32 [3072], P('fsdp')
- norm_gain_grad: float32 [1536], P('fsdp')
- out_weight_grad: float32 [3072, 1536], P('fsdp')
The draws below stay inside these ranges and needn't reach their ends.
All inputs are finite; a program needn't handle non-finite values.
Results may differ from the reference program's by a relative error of at most 0.012.
The reference program's roundings to bfloat16 on the way (of `hidden`, `projected`, `raw_steps`, `gated_out`, `mixed_norm`, `gated_grad`, `proj_grad` and `raw_step_grad`) count: a program that leaves them out, or rounds other values in their place, can miss the bound.
Values may be sent and summed in bfloat16 or wider, within the bound.
A program may use at most 320 MiB of HBM per device.

```python
import jax
import jax.numpy as jnp
from jax import lax

D = 1536
H = 48
N = 128
KW = 4
BLOCK = 256
DI = 3072
CONV = 3328
PROJ = 6400
SEQS = 4
LEN = 1024


def levels(own_key, dims, cuts, smallest, top_value):
    def one(axis_at, parts):
        heights = jax.random.uniform(jax.random.fold_in(jax.random.fold_in(own_key, 6), axis_at), (parts,), jnp.float32, smallest / len(cuts), top_value / len(cuts))
        return jnp.repeat(jnp.exp(heights), dims[axis_at] // parts).reshape((-1,) + (1,) * (len(dims) - axis_at - 1))

    gain = one(*cuts[0])
    for cut in cuts[1:]:
        gain = gain * one(*cut)
    return gain


def scatter_about(stream_key, dims, width, most, cuts=(), kind=jnp.bfloat16):
    gain = levels(stream_key, dims, cuts, -0.22, 0.18) if cuts else 1.0
    values = jax.random.normal(stream_key, dims, jnp.float32) * width * gain
    return jnp.minimum(jnp.maximum(values, -most), most).astype(kind)


def setup_inputs(seed: int = 0) -> dict:
    streams_of = jax.random.split(jax.random.key(seed), 13)
    tokens = scatter_about(streams_of[0], (SEQS, LEN, D), 1.0, 6.0, ((0, 4), (1, 8)))
    in_weight = scatter_about(streams_of[1], (D, PROJ), D ** -0.5, 0.15625, ((0, 4),))
    step_weight = scatter_about(streams_of[2], (D, H), D ** -0.5, 0.15625, ((0, 4),))
    conv_kernel = scatter_about(streams_of[3], (KW, CONV), 0.5, 3.0, ((1, 4),))
    conv_bias = scatter_about(streams_of[4], (CONV,), 0.5, 3.0, ((0, 4),))
    step_bias = jnp.clip(-6.0 + 3.0 * jax.random.uniform(streams_of[5], (H,), jnp.float32) ** levels(streams_of[5], (H,), ((0, 4),), -0.2, 0.2), -6.0, -3.0).astype(jnp.bfloat16)
    log_decay = jnp.clip(-7.0 + 8.0 * jax.random.uniform(streams_of[6], (H,), jnp.float32) ** levels(streams_of[6], (H,), ((0, 4),), -0.2, 0.2), -7.0, 1.0).astype(jnp.bfloat16)
    skip_gain = jnp.clip(0.5 + 1.0 * jax.random.uniform(streams_of[7], (H,), jnp.float32) ** levels(streams_of[7], (H,), ((0, 4),), -0.2, 0.2), 0.5, 1.5).astype(jnp.bfloat16)
    gate_gain = jnp.clip(1.0 + 0.1 * jax.random.normal(streams_of[8], (DI,), jnp.float32), 0.5, 1.5).astype(jnp.bfloat16)
    norm_gain = jnp.clip(1.0 + 0.1 * jax.random.normal(streams_of[9], (D,), jnp.float32), 0.5, 1.5).astype(jnp.bfloat16)
    out_weight = scatter_about(streams_of[10], (DI, D), DI ** -0.5, 0.109375, ((0, 4),))
    cotangent = scatter_about(streams_of[11], (SEQS, LEN, D), 1.0, 6.0, ((0, 4), (1, 8)))
    return {"tokens": tokens, "in_weight": in_weight, "step_weight": step_weight, "conv_kernel": conv_kernel, "conv_bias": conv_bias, "step_bias": step_bias, "log_decay": log_decay, "skip_gain": skip_gain, "gate_gain": gate_gain, "norm_gain": norm_gain, "out_weight": out_weight, "cotangent": cotangent}


epsilon = 1e-05
highest = lax.Precision.HIGHEST

def block_step(carried, pieces, decay_rate):
    x_blk, step_blk, b_blk, c_blk = pieces
    cumulative = jnp.cumsum(step_blk * decay_rate[None, :], axis=0).T
    positions = jnp.arange(step_blk.shape[0])
    triangle = positions[:, None] >= positions[None, :]
    log_gap = jnp.where(triangle[None], cumulative[:, :, None] - cumulative[:, None, :], -1e+30)
    scores = jnp.dot(c_blk, b_blk.T, precision=highest)
    mixing = jnp.exp(log_gap) * scores[None] * step_blk.T[:, None, :]
    y_inside = jnp.einsum('hij,jhp->ihp', mixing, x_blk, precision=highest)
    y_carried = jnp.exp(cumulative).T[:, :, None] * jnp.einsum('in,hpn->ihp', c_blk, carried, precision=highest)
    weighting = jnp.exp(cumulative[:, -1:] - cumulative) * step_blk.T
    renewed = jnp.exp(cumulative[:, -1])[:, None, None] * carried + jnp.einsum('hj,jhp,jn->hpn', weighting, x_blk, b_blk, precision=highest)
    return (renewed, y_inside + y_carried)

def ssd_scan(x_heads, step_size, decay_rate, b_conv, c_conv, carried):
    length = step_size.shape[0]
    extent = min(BLOCK, length)
    number = length // extent
    pieces = (x_heads.reshape((number, extent) + x_heads.shape[1:]), step_size.reshape((number, extent) + step_size.shape[1:]), b_conv.reshape(number, extent, -1), c_conv.reshape(number, extent, -1))

    def advance(ssm_state, block_in):
        return block_step(ssm_state, block_in, decay_rate)
    finals, outputs = lax.scan(jax.checkpoint(advance), carried, pieces)
    return outputs.reshape(x_heads.shape)

def prepare(extended, raw_steps, conv_kernel, conv_offset, step_bias, log_rates):
    kernel_width = conv_kernel.shape[0]
    length = extended.shape[0] - kernel_width + 1
    summed = conv_offset[None, :] + sum((conv_kernel[offset][None, :] * extended[offset:offset + length] for offset in range(kernel_width)))
    active = jax.nn.silu(summed)
    split_at = active.shape[1] - 2 * N
    step_size = jax.nn.softplus(raw_steps + step_bias[None, :])
    return (active[:, :split_at], active[:, split_at:split_at + N], active[:, split_at + N:], step_size, -jnp.exp(log_rates))

def mix_out(x_conv, b_conv, c_conv, step_size, decay_rate, gate_in, skip_part, carried):
    length, head_count = step_size.shape
    x_heads = x_conv.reshape(length, head_count, -1)
    result = ssd_scan(x_heads, step_size, decay_rate, b_conv, c_conv, carried) + skip_part[None, :, None] * x_heads
    return result.reshape(length, -1) * jax.nn.silu(gate_in)

def rms_forward(values, gains):
    scaling = lax.rsqrt(lax.optimization_barrier(jnp.mean(values * values, axis=-1, keepdims=True)) + epsilon)
    return (values * scaling * gains[None, :], scaling)

def rms_backward(values, gains, scaling, upstream):
    weighted = upstream * gains[None, :]
    gain_grad = lax.optimization_barrier(jnp.sum(upstream * values * scaling, axis=0))
    inner_mean = lax.optimization_barrier(jnp.mean(weighted * values, axis=-1, keepdims=True))
    return (scaling * weighted - scaling ** 3 * values * inner_mean, gain_grad)

def contract(left, right, left_dim, right_dim):
    return lax.dot_general(left, right, (((left_dim,), (right_dim,)), ((), ())), preferred_element_type=jnp.float32)

def layer(seq_tokens, seq_cotangent, in_weight, step_weight, small_params, out_weight):
    kernel_f, bias_f, step_bias_f, decay_f, skip_f, gate_f, norm_f = small_params
    inner_width = out_weight.shape[0]
    kernel_width = kernel_f.shape[0]
    residual = seq_tokens.astype(jnp.float32)
    normed, scale_in = rms_forward(residual, norm_f)
    hidden = normed.astype(jnp.bfloat16)
    projected = jnp.dot(hidden, in_weight, preferred_element_type=jnp.float32).astype(jnp.bfloat16)
    raw_steps = jnp.dot(hidden, step_weight, preferred_element_type=jnp.float32).astype(jnp.bfloat16)
    padding = jnp.zeros((kernel_width - 1, projected.shape[1] - inner_width), jnp.float32)
    extended = jnp.concatenate([padding, projected[:, inner_width:].astype(jnp.float32)], axis=0)
    prepared, pull_prepare = jax.vjp(prepare, extended, raw_steps.astype(jnp.float32), kernel_f, bias_f, step_bias_f, decay_f)
    x_conv, b_conv, c_conv, step_size, decay_rate = prepared
    head_count = step_size.shape[1]
    start_state = jnp.zeros((head_count, inner_width // head_count, N), jnp.float32)
    gated_f, pull_mix = jax.vjp(mix_out, x_conv, b_conv, c_conv, step_size, decay_rate, projected[:, :inner_width].astype(jnp.float32), skip_f, start_state)
    gated_out = lax.optimization_barrier(gated_f.astype(jnp.bfloat16))
    gated_back = gated_out.astype(jnp.float32)
    mixed_f, scale_out = rms_forward(gated_back, gate_f)
    mixed_norm = mixed_f.astype(jnp.bfloat16)
    block_out = (residual + jnp.dot(mixed_norm, out_weight, preferred_element_type=jnp.float32)).astype(jnp.bfloat16)
    out_grad = contract(mixed_norm, seq_cotangent, 0, 0)
    mixed_grad = contract(seq_cotangent, out_weight, 1, 1)
    gated_grad, gate_gain_grad = rms_backward(gated_back, gate_f, scale_out, mixed_grad)
    gated_grad = lax.optimization_barrier(gated_grad.astype(jnp.bfloat16)).astype(jnp.float32)
    x_grad, b_grad, c_grad, step_grad, rate_grad, gate_in_grad, skip_grad, unused = pull_mix(gated_grad)
    ext_grad, raw_grad, kernel_grad, bias_grad, step_bias_grad, decay_grad = pull_prepare((x_grad, b_grad, c_grad, step_grad, rate_grad))
    proj_grad = jnp.concatenate([gate_in_grad, ext_grad[kernel_width - 1:]], axis=1).astype(jnp.bfloat16)
    raw_step_grad = raw_grad.astype(jnp.bfloat16)
    in_grad = contract(hidden, proj_grad, 0, 0)
    step_w_grad = contract(hidden, raw_step_grad, 0, 0)
    hidden_grad = contract(proj_grad, in_weight, 1, 1) + contract(raw_step_grad, step_weight, 1, 1)
    resid_grad, norm_gain_grad = rms_backward(residual, norm_f, scale_in, hidden_grad)
    input_grad = seq_cotangent.astype(jnp.float32) + resid_grad
    gradients = (in_grad, step_w_grad, kernel_grad, bias_grad, step_bias_grad, decay_grad, skip_grad, gate_gain_grad, norm_gain_grad, out_grad)
    return (block_out, input_grad, gradients)

def reference(tokens, in_weight, step_weight, conv_kernel, conv_bias, step_bias, log_decay, skip_gain, gate_gain, norm_gain, out_weight, cotangent):
    small_params = tuple((parameter.astype(jnp.float32) for parameter in (conv_kernel, conv_bias, step_bias, log_decay, skip_gain, gate_gain, norm_gain)))

    def sequence_pass(running, inputs):
        block_out, input_grad, gradients = layer(inputs[0], inputs[1], in_weight, step_weight, small_params, out_weight)
        return (tuple((total + grad_part for total, grad_part in zip(running, gradients))), (block_out, input_grad))
    initial = tuple((jnp.zeros(array_shape, jnp.float32) for array_shape in (in_weight.shape, step_weight.shape, conv_kernel.shape, conv_bias.shape, step_bias.shape, log_decay.shape, skip_gain.shape, gate_gain.shape, norm_gain.shape, out_weight.shape)))
    running, outputs = lax.scan(sequence_pass, initial, (tokens, cotangent))
    return (outputs[0], outputs[1], running[0], running[1], running[2], running[3], running[4], running[5], running[6], running[7], running[8], running[9])
```

```python
import jax
import jax.numpy as jnp
from jax import lax
from jax.sharding import PartitionSpec as P

N = 128
BLOCK = 256


epsilon = 1e-05
bf16 = jnp.bfloat16
f32 = jnp.float32


def block_step(carried, pieces, decay_rate):
    x_blk, step_blk, b_blk, c_blk = pieces
    cumulative = jnp.cumsum(step_blk * decay_rate[None, :], axis=0).T
    positions = jnp.arange(step_blk.shape[0])
    triangle = positions[:, None] >= positions[None, :]
    log_gap = jnp.where(triangle[None], cumulative[:, :, None] - cumulative[:, None, :], -1e30)
    scores = jnp.dot(c_blk, b_blk.T)
    mixing = jnp.exp(log_gap) * scores[None] * step_blk.T[:, None, :]
    y_inside = jnp.einsum("hij,jhp->ihp", mixing, x_blk)
    y_carried = jnp.exp(cumulative).T[:, :, None] * jnp.einsum("in,hpn->ihp", c_blk, carried)
    weighting = jnp.exp(cumulative[:, -1:] - cumulative) * step_blk.T
    renewed = jnp.exp(cumulative[:, -1])[:, None, None] * carried + jnp.einsum(
        "hj,jhp,jn->hpn", weighting, x_blk, b_blk
    )
    return (renewed, y_inside + y_carried)


def ssd_scan(x_heads, step_size, decay_rate, b_conv, c_conv, carried):
    length = step_size.shape[0]
    extent = min(BLOCK, length)
    number = length // extent
    pieces = (
        x_heads.reshape((number, extent) + x_heads.shape[1:]),
        step_size.reshape((number, extent) + step_size.shape[1:]),
        b_conv.reshape(number, extent, -1),
        c_conv.reshape(number, extent, -1),
    )
    outs = []
    for k in range(number):
        carried, out = block_step(carried, tuple(p[k] for p in pieces), decay_rate)
        outs.append(out)
    return jnp.concatenate(outs, 0).reshape(x_heads.shape)


def prepare(extended, raw_steps, conv_kernel, conv_offset, step_bias, log_rates):
    kernel_width = conv_kernel.shape[0]
    length = extended.shape[0] - kernel_width + 1
    summed = conv_offset[None, :] + sum(
        (
            conv_kernel[offset][None, :] * extended[offset : offset + length]
            for offset in range(kernel_width)
        )
    )
    active = jax.nn.silu(summed)
    split_at = active.shape[1] - 2 * N
    step_size = jax.nn.softplus(raw_steps + step_bias[None, :])
    return (
        active[:, :split_at],
        active[:, split_at : split_at + N],
        active[:, split_at + N :],
        step_size,
        -jnp.exp(log_rates),
    )


def mix_out(x_conv, b_conv, c_conv, step_size, decay_rate, gate_in, skip_part, carried):
    length, head_count = step_size.shape
    x_heads = x_conv.reshape(length, head_count, -1)
    result = (
        ssd_scan(x_heads, step_size, decay_rate, b_conv, c_conv, carried)
        + skip_part[None, :, None] * x_heads
    )
    return result.reshape(length, -1) * jax.nn.silu(gate_in)


def contract(left, right, left_dim, right_dim):
    return lax.dot_general(
        left, right, (((left_dim,), (right_dim,)), ((), ())), preferred_element_type=f32
    )


def shards(
    tokens,
    in_weight,
    step_weight,
    conv_kernel,
    conv_bias,
    step_bias,
    log_decay,
    skip_gain,
    gate_gain,
    norm_gain,
    out_weight,
    cotangent,
):
    seqs = lax.axis_size("seq")
    fs = lax.axis_size("fsdp")
    pos = lax.axis_index("seq")
    fpos = lax.axis_index("fsdp")
    heads = step_weight.shape[1]
    inner = out_weight.shape[0] * fs
    width = tokens.shape[-1]
    hg = heads // seqs
    cols = inner // seqs
    col = pos * cols
    KW, conv_l = conv_kernel.shape

    def sl(a, start, size, axis):
        return lax.dynamic_slice_in_dim(a, start, size, axis)

    w_part = jnp.concatenate(
        [
            sl(in_weight, col, cols, 1),
            sl(in_weight, inner + col, cols, 1),
            in_weight[:, 2 * inner :],
            sl(step_weight, pos * hg, hg, 1),
        ],
        axis=1,
    )
    w_g = lax.all_gather(w_part, "fsdp", axis=0, tiled=True)
    small = jnp.concatenate(
        [
            conv_kernel.reshape(-1),
            conv_bias,
            step_bias,
            log_decay,
            skip_gain,
            gate_gain,
            norm_gain,
        ]
    )
    small = lax.all_gather(small, "fsdp", axis=0, tiled=False).astype(f32)
    at = [0]

    def take(n):
        r = small[:, at[0] : at[0] + n]
        at[0] += n
        return r

    kernel_f = take(KW * conv_l).reshape(fs, KW, conv_l).transpose(1, 0, 2).reshape(KW, -1)
    bias_f = take(conv_l).reshape(-1)
    step_bias_f = take(heads // fs).reshape(-1)
    decay_f = take(heads // fs).reshape(-1)
    skip_f = take(heads // fs).reshape(-1)
    gate_f = sl(take(inner // fs).reshape(-1), col, cols, 0)
    norm_f = take(width // fs).reshape(-1)

    tok = lax.all_gather(tokens[0], "seq", axis=0, tiled=True)
    cot = lax.all_gather(cotangent[0], "seq", axis=0, tiled=True)
    w_out = lax.all_gather(out_weight, "fsdp", axis=0, tiled=True)
    w_out_g = sl(w_out, col, cols, 0)
    length = tok.shape[0]
    own = length // seqs

    resid = tok.astype(f32)
    scale_in = lax.rsqrt(jnp.mean(resid * resid, axis=-1, keepdims=True) + epsilon)
    hidden = (resid * scale_in * norm_f[None]).astype(bf16)
    proj = contract(hidden, w_g, 1, 0).astype(bf16).astype(f32)
    gate_in = proj[:, :cols]
    body = proj[:, cols : 2 * cols + 2 * N]
    raw = proj[:, 2 * cols + 2 * N :]
    my_kernel = jnp.concatenate([sl(kernel_f, col, cols, 1), kernel_f[:, inner:]], axis=1)
    my_bias = jnp.concatenate([sl(bias_f, col, cols, 0), bias_f[inner:]], axis=0)
    my_step_bias = sl(step_bias_f, pos * hg, hg, 0)
    my_decay = sl(decay_f, pos * hg, hg, 0)
    my_skip = sl(skip_f, pos * hg, hg, 0)
    extended = jnp.concatenate([jnp.zeros((KW - 1, cols + 2 * N), f32), body], axis=0)
    prepared, pull_prepare = jax.vjp(
        prepare, extended, raw, my_kernel, my_bias, my_step_bias, my_decay
    )
    x_conv, b_conv, c_conv, step_size, decay_rate = prepared
    start = jnp.zeros((hg, cols // hg, N), f32)
    gated_f, pull_mix = jax.vjp(
        mix_out, x_conv, b_conv, c_conv, step_size, decay_rate, gate_in, my_skip, start
    )
    gated_b = gated_f.astype(bf16)
    gated = gated_b.astype(f32)
    mixed_grad = contract(cot, w_out_g, 1, 1)
    g = mixed_grad * gate_f[None]
    stats = jnp.stack([jnp.sum(gated * gated, axis=1), jnp.sum(g * gated, axis=1)])
    stats = lax.psum(stats, "seq") / inner
    scale_out = lax.rsqrt(stats[0] + epsilon)[:, None]
    mixed_norm = (gated * scale_out * gate_f[None]).astype(bf16)
    gate_gain_grad = jnp.sum(mixed_grad * gated * scale_out, axis=0)
    gated_grad = (scale_out * g - scale_out**3 * gated * stats[1][:, None]).astype(bf16)

    mixed_all = lax.all_to_all(mixed_norm, "seq", split_axis=0, concat_axis=1, tiled=True)
    my_tok = tokens[0].astype(f32)
    block_out = (my_tok + contract(mixed_all, w_out, 1, 0)).astype(bf16)
    out_part = contract(mixed_norm, cot, 0, 0)
    x_grad, b_grad, c_grad, step_grad, rate_grad, gate_grad, skip_grad, _ = pull_mix(
        gated_grad.astype(f32)
    )
    ext_grad, raw_grad, kernel_grad, bias_grad, step_bias_grad, decay_grad = pull_prepare(
        (x_grad, b_grad, c_grad, step_grad, rate_grad)
    )
    proj_grad = jnp.concatenate([gate_grad, ext_grad[KW - 1 :], raw_grad], axis=1).astype(bf16)
    hid_part = contract(proj_grad, w_g, 1, 1)
    hidden_grad = lax.psum_scatter(
        hid_part.astype(bf16), "seq", scatter_dimension=0, tiled=True
    ).astype(f32)
    in_part = contract(hidden, proj_grad, 0, 0)
    in_red = lax.psum_scatter(in_part.astype(bf16), "fsdp", scatter_dimension=0, tiled=True)
    in_all = lax.all_gather(in_red, "seq", axis=0, tiled=False).astype(f32)
    in_grad = jnp.concatenate(
        [
            jnp.moveaxis(in_all[:, :, :cols], 0, 1).reshape(-1, inner),
            jnp.moveaxis(in_all[:, :, cols : 2 * cols], 0, 1).reshape(-1, inner),
            jnp.sum(in_all[:, :, 2 * cols : 2 * cols + 2 * N], axis=0),
        ],
        axis=1,
    )
    step_w_grad = jnp.moveaxis(in_all[:, :, 2 * cols + 2 * N :], 0, 1).reshape(-1, heads)
    out_red = lax.psum_scatter(out_part.astype(bf16), "fsdp", scatter_dimension=0, tiled=True)
    out_all = lax.all_gather(out_red, ("seq", "fsdp"), axis=0, tiled=True)
    out_rows = inner // fs
    out_grad = sl(out_all, fpos * out_rows, out_rows, 0).astype(f32)

    own_scale = lax.rsqrt(jnp.mean(my_tok * my_tok, axis=-1, keepdims=True) + epsilon)
    norm_gain_grad = jnp.sum(hidden_grad * my_tok * own_scale, axis=0)
    e = hidden_grad * norm_f[None]
    inner_mean = jnp.mean(e * my_tok, axis=-1, keepdims=True)
    input_grad = cotangent[0].astype(f32) + own_scale * e - own_scale**3 * my_tok * inner_mean

    def put(a, total, start, axis):
        shape = list(a.shape)
        shape[axis] = total
        idx = [0] * a.ndim
        idx[axis] = start
        return lax.dynamic_update_slice(jnp.zeros(shape, f32), a, tuple(idx))

    conv = inner + 2 * N
    kg = jnp.concatenate([put(kernel_grad[:, :cols], inner, col, 1), kernel_grad[:, cols:]], 1)
    bg = jnp.concatenate([put(bias_grad[:cols], inner, col, 0), bias_grad[cols:]], 0)
    packed = jnp.concatenate(
        [
            kg.reshape(-1),
            bg,
            put(step_bias_grad, heads, pos * hg, 0),
            put(decay_grad, heads, pos * hg, 0),
            put(skip_grad, heads, pos * hg, 0),
            put(gate_gain_grad, inner, col, 0),
            norm_gain_grad,
        ]
    )
    packed = lax.psum(packed, ("seq", "fsdp"))
    at[0] = 0

    def grab(n, size, rows=None):
        r = packed[at[0] : at[0] + n]
        at[0] += n
        if rows:
            return sl(r.reshape(rows, -1), fpos * size, size, 1)
        return sl(r, fpos * size, size, 0)

    kernel_out = grab(KW * conv, conv_l, KW)
    bias_out = grab(conv, conv_l)
    sb_out = grab(heads, heads // fs)
    ld_out = grab(heads, heads // fs)
    sk_out = grab(heads, heads // fs)
    gg_out = grab(inner, inner // fs)
    ng_out = grab(width, width // fs)
    return (
        block_out[None],
        input_grad[None],
        in_grad,
        step_w_grad,
        kernel_out,
        bias_out,
        sb_out,
        ld_out,
        sk_out,
        gg_out,
        ng_out,
        out_grad,
    )


def solution(mesh):
    row = P("fsdp", None)
    tok = P("fsdp", "seq", None)
    one = P("fsdp")
    return jax.shard_map(
        shards,
        mesh=mesh,
        in_specs=(tok, row, row, P(None, "fsdp"), one, one, one, one, one, one, row, tok),
        out_specs=(tok, tok, row, row, P(None, "fsdp"), one, one, one, one, one, one, row),
        check_vma=False,
    )
```

```python
from types import SimpleNamespace

import jax
import jax.numpy as jnp
from jax import lax
from jax.experimental import pallas as pl
from jax.experimental.pallas import tpu as pltpu
from jax.sharding import PartitionSpec as P

N = 128
HEAD = 64
Q = 128
epsilon = 1e-05
bf16 = jnp.bfloat16
f32 = jnp.float32
MESH = pl.DeviceIdType.MESH
HI = lax.Precision.HIGHEST
VMEM_LIMIT = 64 * 1024 * 1024 - 65536


def mm(a, b, da=1, db=0, precision=None):
    return lax.dot_general(
        a, b, (((da,), (db,)), ((), ())), preferred_element_type=f32, precision=precision
    )


def rcopy(src, dst, ss, rs, **dev):
    return pltpu.make_async_remote_copy(
        src_ref=src, dst_ref=dst, send_sem=ss, recv_sem=rs, device_id=dev, device_id_type=MESH
    )


class Place:
    def __init__(self, S, F):
        self.S, self.F = S, F
        self.Z = 4
        self.X = S // 4
        self.s = lax.axis_index("seq")
        self.f = lax.axis_index("fsdp")
        self.z = self.s // self.X
        self.x = lax.rem(self.s, self.X)

    def zz(self, k):
        return lax.rem(self.z + k + (k // 2) * (1 - 2 * (k % 2)), self.Z)

    def blk(self, k, q):
        return self.zz(k) * self.X + lax.rem(self.x + q, self.X)

    def barrier(self):
        bar = pltpu.get_barrier_semaphore()
        n = 0
        for k in range(1, self.S):
            pl.semaphore_signal(
                bar, inc=1, device_id={"seq": lax.rem(self.s + k, self.S)}, device_id_type=MESH
            )
            n += 1
        for k in range(1, self.F):
            pl.semaphore_signal(
                bar, inc=1, device_id={"fsdp": lax.rem(self.f + k, self.F)}, device_id_type=MESH
            )
            n += 1
        pl.semaphore_wait(bar, n)


class Gather:
    def __init__(self, pc, src, buf, ss, rs):
        self.pc, self.src, self.buf, self.ss, self.rs = pc, src, buf, ss, rs

    def start(self):
        pc = self.pc
        for k in range(1, pc.Z):
            rcopy(
                self.src, self.buf.at[pc.s], self.ss.at[k - 1], self.rs.at[pc.s],
                seq=pc.zz(k) * pc.X + pc.x,
            ).start()
        self.across(self.src, pc.s, 0)

    def across(self, src, b, k):
        pc = self.pc
        for q in range(1, pc.X):
            rcopy(
                src, self.buf.at[b], self.ss.at[pc.Z - 1 + k * (pc.X - 1) + q - 1], self.rs.at[b],
                seq=pc.z * pc.X + lax.rem(pc.x + q, pc.X),
            ).start()

    def wait(self, b):
        r = self.buf.at[b]
        rcopy(r, r, self.ss.at[0], self.rs.at[b], seq=self.pc.s).wait_recv()

    def drain(self):
        for i in range(self.pc.Z - 1 + self.pc.Z * (self.pc.X - 1)):
            rcopy(self.src, self.src, self.ss.at[i], self.rs.at[0], seq=self.pc.s).wait_send()


def gather_sems(S):
    Z, X = 4, S // 4
    return [pltpu.SemaphoreType.DMA((Z - 1 + Z * (X - 1),)), pltpu.SemaphoreType.DMA((S,))]


def pair(col, p):
    lane = lax.broadcasted_iota(jnp.int32, (col.shape[0], 128), 1)
    return jnp.where(lane < HEAD, col[:, 2 * p : 2 * p + 1], col[:, 2 * p + 1 : 2 * p + 2])


def spread(col, cp):
    return jnp.concatenate([pair(col, p) for p in range(cp // 128)], axis=1)


def sigmoid(v):
    return 1.0 / (1.0 + jnp.exp(-v))


def softplus(v):
    return jnp.maximum(v, 0.0) + jnp.log1p(jnp.exp(-jnp.abs(v)))


def tri(shape, flip=False):
    i = lax.broadcasted_iota(jnp.int32, shape, 0)
    j = lax.broadcasted_iota(jnp.int32, shape, 1)
    return j >= i if flip else i >= j


def split(x2):
    lane = lax.broadcasted_iota(jnp.int32, x2.shape, 1)
    return jnp.concatenate([jnp.where(lane < HEAD, x2, 0), jnp.where(lane >= HEAD, x2, 0)], axis=0)


def chunk_inputs(c, ext, rawb, small, cp):
    r0 = pl.multiple_of(c * Q, Q)
    v = ext[pl.ds(r0, Q + 16), :].astype(f32)
    C = cp + 2 * N
    taps = [pltpu.roll(v, 3 - k, 0)[16:] if k < 3 else v[16:] for k in range(4)]
    summed = small[4:5, :C]
    for k in range(4):
        summed = summed + small[k : k + 1, :C] * taps[k]
    sig = sigmoid(summed)
    raw = rawb[pl.ds(r0, Q), :].astype(f32) + small[7:8, 0:128]
    dt = softplus(raw)
    rate = -jnp.exp(small[7:8, 128:256])
    cum = mm(tri((Q, Q)).astype(f32), dt * rate, precision=HI)
    return taps, summed, sig, raw, dt, rate, cum


def skip_row(small, cp):
    return spread(small[7:8, 256:384], cp)


def body_fwd(cfg, tok, cot, wp, wo, sm, R):
    S, F, T, D, cp, WC = cfg
    L = S * T
    C = cp + 2 * N
    pc = Place(S, F)
    nh = cp // HEAD
    pc.barrier()
    tg = Gather(pc, tok, R.tok_all, R.ss_t, R.rs_t)
    cg = Gather(pc, cot, R.cot_all, R.ss_c, R.rs_c)
    ssw, rsw = R.ss_w, R.rs_w
    owner = pc.s // (S // F)
    tg.start()
    for k in range(1, F):
        to = lax.rem(pc.f + k, F)
        rcopy(sm, R.sm_all.at[pc.f], ssw.at[0, k], rsw.at[0, pc.f], fsdp=to).start()
        rcopy(wp, R.w_all.at[pc.f], ssw.at[1, k], rsw.at[1, pc.f], fsdp=to).start()

    @pl.when(pc.f == owner)
    def _():
        for k in range(1, F):
            to = lax.rem(pc.f + k, F)
            rcopy(wo, R.wo_g, ssw.at[2, k], rsw.at[2, 0], fsdp=to).start()
        pltpu.make_async_copy(wo, R.wo_g, R.wsem.at[1]).start()

    cg.start()
    R.tok_all[pc.s] = tok[...]
    R.cot_all[pc.s] = cot[...]
    pltpu.make_async_copy(wp, R.w_all.at[pc.f], R.wsem.at[0]).start()
    R.sm_all[pc.f] = sm[...]

    for i, (src, dst) in enumerate(((sm, R.sm_all), (wp, R.w_all))):
        for k in range(1, F):
            o = lax.rem(pc.f + k, F)
            rcopy(src, dst.at[o], ssw.at[i, 0], rsw.at[i, o], fsdp=pc.f).wait_recv()
        if i == 0:
            total = R.sm_all[0]
            for k in range(1, F):
                total = total + R.sm_all[k]
            R.small[...] = total
    pltpu.make_async_copy(wp, R.w_all.at[pc.f], R.wsem.at[0]).wait()
    small = R.small
    R.ext[0:16, :] = jnp.zeros((16, C), bf16)

    def project(j, carry):
        k, q = j // pc.X, lax.rem(j, pc.X)
        b = pc.blk(k, q)

        @pl.when(j > 0)
        def _():
            tg.wait(b)

        @pl.when(jnp.logical_and(q == 0, k > 0))
        def _():
            tg.across(R.tok_all.at[b], b, k)

        r = R.tok_all[b].astype(f32)
        scale = lax.rsqrt(jnp.mean(r * r, axis=1, keepdims=True) + epsilon)
        h = r * scale * small[6:7, :]
        r0 = pl.multiple_of(b * T, T)
        R.hid_t[:, pl.ds(r0, T)] = h.T.astype(bf16)
        out = mm(h.astype(bf16), R.w_all[...].reshape(D, WC)).astype(bf16)
        R.zb[pl.ds(r0, T), :] = out[:, :cp]
        R.rawb[pl.ds(r0, T), :] = out[:, 2 * cp + 2 * N :]
        R.ext[pl.ds(r0 + 16, T), :] = out[:, cp : 2 * cp + 2 * N]
        return carry

    lax.fori_loop(0, S, project, 0)
    R.state[...] = jnp.zeros((N, cp), f32)
    ones = jnp.ones((8, cp), f32)

    def forward(c, carry):
        @pl.when(c < pc.Z - 1)
        def _():
            b = pc.blk(c + 1, 0)
            cg.wait(b)
            cg.across(R.cot_all.at[b], b, c + 1)

        r0 = pl.multiple_of(c * Q, Q)
        taps, summed, sig, raw, dt, rate, cum = chunk_inputs(c, R.ext, R.rawb, small, cp)
        act = summed * sig
        x = act[:, :cp]
        bb = act[:, cp : cp + N].astype(bf16)
        cb = act[:, cp + N :].astype(bf16)
        cum_t = cum.T
        dt_t = dt.T
        scores = mm(cb, bb, 1, 1)
        causal = tri((Q, Q))
        parts = []
        for p in range(cp // 128):
            mix = []
            for h in (2 * p, 2 * p + 1):
                gap = jnp.where(causal, cum[:, h : h + 1] - cum_t[h : h + 1, :], -1e30)
                mix.append((jnp.exp(gap) * scores * dt_t[h : h + 1, :]).astype(bf16))
            parts.append(
                mm(jnp.concatenate(mix, axis=1), split(x[:, 128 * p : 128 * p + 128]).astype(bf16))
            )
        state = R.state[...]
        R.states[c] = state
        last = cum[Q - 1 : Q, :]
        y = jnp.concatenate(parts, axis=1) + mm(cb, state.astype(bf16)) * spread(jnp.exp(cum), cp)
        y = y + skip_row(small, cp) * x
        wx = (spread(jnp.exp(last - cum) * dt, cp) * x).astype(bf16)
        R.state[...] = spread(jnp.exp(last), cp) * state + mm(bb, wx, 0, 0)
        R.y[pl.ds(r0, Q), :] = y
        z = R.zb[pl.ds(r0, Q), :].astype(f32)
        gated = (y * (z * sigmoid(z))).astype(bf16)
        R.dpx[pl.ds(r0, Q), :cp] = gated
        g32 = gated.astype(f32)
        R.st[0:1, pl.ds(r0, Q)] = mm(ones, g32 * g32, 1, 1, HI)[0:1]
        return carry

    lax.fori_loop(0, L // Q, forward, 0)

    @pl.when(pc.f != owner)
    def _():
        rcopy(wo, R.wo_g, ssw.at[2, 0], rsw.at[2, 0], fsdp=pc.f).wait_recv()

    @pl.when(pc.f == owner)
    def _():
        pltpu.make_async_copy(wo, R.wo_g, R.wsem.at[1]).wait()

    def mixed(j, carry):
        k, q = j // pc.X, lax.rem(j, pc.X)
        b = pc.blk(k, q)

        @pl.when(q > 0)
        def _():
            cg.wait(b)

        r0 = pl.multiple_of(b * T, T)
        mg = mm(R.cot_all[b], R.wo_g[...], 1, 1)
        R.mg[pl.ds(r0, T), :] = mg
        g = mg * small[5:6, :cp] * R.dpx[pl.ds(r0, T), :cp].astype(f32)
        R.st[1:2, pl.ds(r0, T)] = mm(ones, g, 1, 1, HI)[0:1]
        return carry

    lax.fori_loop(0, S, mixed, 0)
    for k in range(1, S):
        rcopy(
            R.st, R.st_all.at[pc.s], R.ss_s.at[k], R.rs_s.at[pc.s],
            seq=lax.rem(pc.s + k, S),
        ).start()
    R.st_all[pc.s] = R.st[...]
    for k in range(1, S):
        o = lax.rem(pc.s + k, S)
        rcopy(R.st, R.st_all.at[o], R.ss_s.at[0], R.rs_s.at[o], seq=pc.s).wait_recv()
    total = R.st_all[0]
    for k in range(1, S):
        total = total + R.st_all[k]
    R.stats[...] = total

    tg.drain()
    cg.drain()
    for k in range(1, S):
        rcopy(R.st, R.st, R.ss_s.at[k], R.rs_s.at[0], seq=pc.s).wait_send()
    for k in range(1, F):
        rcopy(sm, sm, ssw.at[0, k], rsw.at[0, 0], fsdp=pc.f).wait_send()
        rcopy(wp, wp, ssw.at[1, k], rsw.at[1, 0], fsdp=pc.f).wait_send()

    @pl.when(pc.f == owner)
    def _():
        for k in range(1, F):
            rcopy(wo, wo, ssw.at[2, k], rsw.at[2, 0], fsdp=pc.f).wait_send()


def fwd_scratch(cfg):
    S, F, T, D, cp, WC = cfg
    L = S * T
    Dl = D // F
    C = cp + 2 * N
    V = pltpu.VMEM
    sem = pltpu.SemaphoreType.DMA
    n_ag = 3 + 4 * (S // 4 - 1)
    return SimpleNamespace(
        tok_all=V((S, T, D), bf16),
        cot_all=V((S, T, D), bf16),
        w_all=V((F, Dl, WC), bf16),
        wo_g=V((cp, D), bf16),
        sm_all=V((F, 8, D), f32),
        small=V((8, D), f32),
        hid_t=V((D, L), bf16),
        zb=V((L, cp), bf16),
        rawb=V((L, 128), bf16),
        ext=V((16 + L, C), bf16),
        state=V((N, cp), f32),
        states=V((L // Q, N, cp), f32),
        y=V((L, cp), f32),
        mg=V((L, cp), f32),
        st=V((2, L), f32),
        st_all=V((S, 2, L), f32),
        stats=V((2, L), f32),
        ss_t=sem((n_ag,)),
        rs_t=sem((S,)),
        ss_c=sem((n_ag,)),
        rs_c=sem((S,)),
        ss_w=sem((3, F)),
        rs_w=sem((3, F)),
        wsem=sem((2,)),
        ss_s=sem((S,)),
        rs_s=sem((S,)),
    )


def prep(cfg, in_weight, step_weight, conv_kernel, conv_bias, step_bias, log_decay, skip_gain,
         gate_gain, norm_gain, out_weight):
    S, F, T, D, cp, WC = cfg
    s = lax.axis_index("seq")
    f = lax.axis_index("fsdp")
    heads = step_weight.shape[1]
    hg = heads // S
    inner = out_weight.shape[0] * F
    cols = inner // S
    col = s * cols

    def sl(a, start, size, axis):
        return lax.dynamic_slice_in_dim(a, start, size, axis)

    def padc(a, to):
        return jnp.pad(a, [(0, 0)] * (a.ndim - 1) + [(0, to - a.shape[-1])])

    wp = jnp.concatenate(
        [
            padc(sl(in_weight, col, cols, 1), cp),
            padc(sl(in_weight, inner + col, cols, 1), cp),
            in_weight[:, 2 * inner :],
            padc(sl(step_weight, s * hg, hg, 1), 128),
        ],
        axis=1,
    )
    per = out_weight.shape[0] // cols
    wo = jnp.pad(sl(out_weight, lax.rem(s, per) * cols, cols, 0), [(0, cp - cols), (0, 0)])

    def window(a, start, size, out):
        n = a.shape[-1]
        pad = jnp.pad(a, [(0, 0)] * (a.ndim - 1) + [(size, size)])
        return padc(sl(pad, jnp.clip(start - n * f + size, 0, n + size), size, a.ndim - 1), out)

    def conv_rows(a):
        return jnp.concatenate(
            [window(a, col, cols, cp), window(a, inner, 2 * N, 2 * N)], axis=-1
        )

    def row(a):
        return padc(a.astype(f32), D).reshape(-1, D)

    def head(a):
        return window(a[None], s * hg, hg, 128)

    sm = jnp.concatenate(
        [
            row(conv_rows(conv_kernel)),
            row(conv_rows(conv_bias[None])),
            row(window(gate_gain[None], col, cols, cp)),
            row(window(norm_gain[None], 0, D, D)),
            row(jnp.concatenate([head(step_bias), head(log_decay), head(skip_gain)], axis=-1)),
        ],
        axis=0,
    )
    return wp, wo, sm


class Scatter:
    def __init__(self, pc, part, rx, rz, sems):
        self.pc, self.part, self.rx, self.rz = pc, part, rx, rz
        self.ssx, self.rsx, self.ssz, self.rsz = sems

    def across(self, b):
        pc = self.pc
        zb, xb = b // pc.X, lax.rem(b, pc.X)

        @pl.when(xb != pc.x)
        def _():
            slot = lax.rem(pc.x - xb - 1 + pc.X, pc.X)
            rcopy(
                self.part.at[b], self.rx.at[zb, slot], self.ssx.at[b], self.rsx.at[zb, slot],
                seq=pc.z * pc.X + xb,
            ).start()

    def column(self, zb):
        pc = self.pc
        b = zb * pc.X + pc.x
        total = self.part[b].astype(f32)
        for q in range(pc.X - 1):
            r = self.rx.at[zb, q]
            rcopy(r, r, self.ssx.at[0], self.rsx.at[zb, q], seq=pc.s).wait_recv()
            total = total + self.rx[zb, q].astype(f32)
        self.part[b] = total.astype(bf16)

        @pl.when(zb != pc.z)
        def _():
            slot = lax.rem(pc.z - zb - 1 + pc.Z, pc.Z)
            rcopy(
                self.part.at[b], self.rz.at[slot], self.ssz.at[zb], self.rsz.at[slot], seq=b
            ).start()

    def total(self):
        pc = self.pc
        out = self.part[pc.s].astype(f32)
        for q in range(pc.Z - 1):
            r = self.rz.at[q]
            rcopy(r, r, self.ssz.at[0], self.rsz.at[q], seq=pc.s).wait_recv()
            out = out + self.rz[q].astype(f32)
        return out

    def drain(self):
        pc = self.pc
        r = self.rz.at[0]
        for b in range(pc.S):

            @pl.when(b % pc.X != pc.x)
            def _():
                rcopy(r, r, self.ssx.at[b], self.rsz.at[0], seq=pc.s).wait_send()

        for zb in range(pc.Z):

            @pl.when(zb != pc.z)
            def _():
                rcopy(r, r, self.ssz.at[zb], self.rsz.at[0], seq=pc.s).wait_send()


class Shared:
    def __init__(self, pc, part, recv, ss, rs):
        self.pc, self.part, self.recv, self.ss, self.rs = pc, part, recv, ss, rs

    def send(self, k):
        pc = self.pc
        to = lax.rem(pc.f + k, pc.F)
        rcopy(
            self.part.at[to], self.recv.at[k - 1], self.ss.at[k - 1], self.rs.at[k - 1], fsdp=to
        ).start()

    def total(self):
        pc = self.pc
        out = self.part[pc.f].astype(f32)
        for k in range(1, pc.F):
            r = self.recv.at[k - 1]
            rcopy(r, r, self.ss.at[k - 1], self.rs.at[k - 1], fsdp=pc.f).wait_recv()
            out = out + self.recv[k - 1].astype(f32)
        return out

    def drain(self):
        for k in range(1, self.pc.F):
            r = self.recv.at[k - 1]
            rcopy(r, r, self.ss.at[k - 1], self.rs.at[k - 1], fsdp=self.pc.f).wait_send()


def body_bwd(cfg, inner, tok, cot, R, O):
    S, F, T, D, cp, WC = cfg
    L = S * T
    C = cp + 2 * N
    Dl = D // F
    nc = L // Q
    cr = cp // F
    per = S // F
    pc = Place(S, F)
    small = R.small
    blk = Scatter(pc, R.bp, R.brx, R.brz, (R.bs0, R.bs1, R.bs2, R.bs3))
    hid = Scatter(pc, R.tok_all, R.hrx, R.hrz, (R.hs0, R.hs1, R.hs2, R.hs3))
    zs = Shared(pc, R.zp, R.zr, R.zs0, R.zs1)
    os_ = Shared(pc, R.op, R.orecv, R.os0, R.os1)
    xs = Shared(pc, R.xp, R.xr, R.xs0, R.xs1)
    zg = Gather(pc, R.zred, O.gz, R.gz0, R.gz1)
    og = Gather(pc, R.ored, O.go_s, R.go0, R.go1)
    xg = Gather(pc, R.xred, O.gx, R.gx0, R.gx1)

    def own(src, dst, i):
        return pltpu.make_async_copy(src, dst, R.lsem.at[i])

    gate = small[5:6, :cp]
    R.acc[...] = jnp.zeros((8, D), f32)
    R.hacc[...] = jnp.zeros((2, 8, 128), f32)
    R.dstate[...] = jnp.zeros((N, cp), f32)
    R.head[...] = jnp.zeros((8, C), f32)

    def first(i, carry):
        c = nc - 1 - i
        r0 = pl.multiple_of(c * Q, Q)
        rows = pl.ds(r0, Q)
        st = jnp.concatenate([R.stats[:, rows], jnp.zeros((6, Q), f32)], axis=0).T
        scale = lax.rsqrt(st[:, 0:1] / inner + epsilon)
        mean = st[:, 1:2] / inner
        gated = R.dpx[rows, :cp].astype(f32)
        mg = R.mg[rows, :]
        ng = gated * scale
        mn = ng * gate
        R.acc[5:6, :cp] += jnp.sum(mg * ng, axis=0, keepdims=True)
        gg = (scale * (mg * gate) - scale * scale * scale * gated * mean).astype(bf16).astype(f32)
        z = R.zb[rows, :].astype(f32)
        sz = sigmoid(z)
        R.zb[rows, :] = (gg * R.y[rows, :] * (sz * (1.0 + z * (1.0 - sz)))).astype(bf16)
        R.mg[rows, :] = gg * (z * sz)
        R.mn_t[:, rows] = mn.T.astype(bf16)
        R.dpx[rows, :cp] = mn.astype(bf16)
        return carry

    def block(i, carry):
        c = nc - 1 - i
        rows = pl.ds(pl.multiple_of(c * Q, Q), Q)
        R.bp[c] = mm(R.dpx[rows, :cp], R.wo_g[...]).astype(bf16)
        blk.across(c)
        return carry

    lax.fori_loop(0, nc, first, 0)
    if not tight(cfg):
        lax.fori_loop(0, nc, block, 0)

    def zpart(k, carry):
        to = lax.rem(pc.f + k, F)
        rows = pl.ds(pl.multiple_of(to * Dl, Dl), Dl)
        R.zp[to] = mm(R.hid_t[rows, :], R.zb[...]).astype(bf16)

        @pl.when(k < F)
        def _():
            rcopy(
                R.zp.at[to], R.zr.at[k - 1], R.zs0.at[k - 1], R.zs1.at[k - 1], fsdp=to
            ).start()
        return carry

    lax.fori_loop(1, F + 1, zpart, 0)
    W = 384

    def opart(j, carry):
        cols = pl.ds(pl.multiple_of(j * W, W), W)
        a = R.cot_all[:, :, cols].reshape(L, W)
        R.op[:, :, cols] = mm(R.mn_t[...], a).reshape(F, cr, W).astype(bf16)
        return carry

    lax.fori_loop(0, D // W, opart, 0)
    for k in range(1, F):
        os_.send(k)
    if tight(cfg):
        lax.fori_loop(0, nc, block, 0)

    sel = (
        lax.broadcasted_iota(jnp.int32, (8, cp), 1) // HEAD
        == lax.broadcasted_iota(jnp.int32, (8, cp), 0)
    ).astype(f32)
    sub = lax.broadcasted_iota(jnp.int32, (8, Q), 0)

    def scan(i, carry):
        c = nc - 1 - i
        r0 = pl.multiple_of(c * Q, Q)
        rows = pl.ds(r0, Q)

        @pl.when(i < pc.Z)
        def _():
            blk.column(pc.Z - 1 - i)

        @pl.when(i == 2)
        def _():
            R.zred[...] = zs.total().astype(bf16)
            zg.start()
            own(R.zred, O.gz.at[pc.s], 0).start()

        @pl.when(i == 3)
        def _():
            R.ored[...] = os_.total().astype(bf16)
            og.start()
            own(R.ored, O.go_s.at[pc.s], 4).start()

        @pl.when(jnp.logical_and(i >= 5, i < 5 + pc.Z - 1))
        def _():
            k = i - 4
            b = pc.blk(k, 0)
            zg.wait(b)
            zg.across(O.gz.at[b], b, k)
            og.wait(b)
            og.across(O.go_s.at[b], b, k)

        taps, summed, sig, raw, dt, rate, cum = chunk_inputs(c, R.ext, R.rawb, small, cp)
        act = summed * sig
        x = act[:, :cp]
        xb = x.astype(bf16)
        bb = act[:, cp : cp + N].astype(bf16)
        cb = act[:, cp + N :].astype(bf16)
        cum_t = cum.T
        dt_t = dt.T
        dy = R.mg[rows, :]
        dyb = dy.astype(bf16)
        last = cum[Q - 1 : Q, :]
        edy = spread(jnp.exp(cum), cp) * dy
        edyb = edy.astype(bf16)
        wdec = jnp.exp(last - cum)
        w = wdec * dt
        state = R.states[c]
        sb = state.astype(bf16)
        ds = R.dstate[...]
        dsb = ds.astype(bf16)
        ws = spread(w, cp)
        v = mm(bb, dsb)
        carr = mm(sel, edy * mm(cb, sb), 1, 1, HI)
        dw = mm(sel, x * v, 1, 1, HI)
        db = mm((ws * x).astype(bf16), dsb, 1, 1)
        dc = mm(edyb, sb, 1, 1)
        dlast = mm(sel, jnp.sum(state * ds, axis=0, keepdims=True), 1, 1, HI)
        R.dstate[...] = spread(jnp.exp(last), cp) * ds + mm(cb, edyb, 0, 0)
        scores = mm(bb, cb, 1, 1)
        seen = tri((Q, Q), True)
        dtb = dt_t[0:8].astype(bf16)
        dsc = jnp.zeros((Q, Q), f32)
        direct = jnp.zeros((8, Q), f32)
        onto = jnp.zeros((8, Q), f32)
        parts = []
        for p in range(cp // 128):
            cols = slice(128 * p, 128 * p + 128)
            g2 = mm(split(x[:, cols]).astype(bf16), dyb[:, cols], 1, 1)
            mix = []
            for h in (2 * p, 2 * p + 1):
                g = g2[:Q] if h % 2 == 0 else g2[Q:]
                decay = jnp.exp(jnp.where(seen, cum_t[h : h + 1, :] - cum[:, h : h + 1], -1e30))
                ls = decay * scores
                mix.append((ls * dt[:, h : h + 1]).astype(bf16))
                e = (g * ls).astype(bf16)
                dsc = dsc + g * decay * dt[:, h : h + 1]
                direct = direct + mm(jnp.where(sub == h, 1.0, 0.0).astype(bf16), e, 1, 1)
                onto = onto + mm(jnp.where(sub == h, dtb.astype(f32), 0.0).astype(bf16), e)
            parts.append(mm(jnp.concatenate(mix, axis=1), split(dy[:, cols]).astype(bf16)))
        dscb = dsc.astype(bf16)
        db = db + mm(dscb, cb)
        dc = dc + mm(dscb, bb, 0, 0)
        dx = skip_row(small, cp) * dy + ws * v + jnp.concatenate(parts, axis=1)
        R.acc[7:8, :cp] += jnp.sum(dy * x, axis=0, keepdims=True)
        dt_r = dt_t[0:8]
        wdec_r = wdec.T[0:8]
        w_r = wdec_r * dt_r
        rate_r = jnp.broadcast_to(rate, (128, 128)).T[0:8, 0:1]
        last_r = jnp.exp(cum_t[0:8, Q - 1 : Q])
        dcum = carr + onto - dtb.astype(f32) * direct - w_r * dw
        end = jnp.sum(w_r * dw, axis=1, keepdims=True) + last_r * dlast
        da = mm(dcum, tri((Q, Q)).astype(f32), precision=HI) + end
        ddt = direct + wdec_r * dw + rate_r * da
        draw = ddt * sigmoid(raw).T[0:8]
        R.hacc[0] += draw
        R.hacc[1] += da * dt_r * rate_r
        dact = jnp.concatenate([dx, db, dc], axis=1)
        dsum = dact * (sig * (1.0 + summed * (1.0 - sig)))
        full = jnp.concatenate([dsum, R.head[...]], axis=0)
        dxbc = jnp.zeros((Q, C), f32)
        for k in range(4):
            R.acc[k : k + 1, :C] += jnp.sum(dsum * taps[k], axis=0, keepdims=True)
            moved = pltpu.roll(full, Q + 8 - (3 - k), 0)[:Q] if k < 3 else dsum
            dxbc = dxbc + small[k : k + 1, :C] * moved
        R.acc[4:5, :C] += jnp.sum(dsum, axis=0, keepdims=True)
        R.head[...] = dsum[:8]
        R.dpx[rows, :C] = dxbc.astype(bf16)
        pad = jnp.concatenate([draw, jnp.zeros((120, Q), f32)], axis=0).T
        R.dpx[rows, C:] = pad.astype(bf16)
        grad = jnp.concatenate([R.zb[rows, :], R.dpx[rows, :]], axis=1)
        hp = mm(grad, R.w_all[...].reshape(D, WC), 1, 1)
        r = R.tok_all[c].astype(f32)
        scale = lax.rsqrt(jnp.mean(r * r, axis=1, keepdims=True) + epsilon)
        R.acc[6:7, :] += jnp.sum(hp * r * scale, axis=0, keepdims=True)
        R.tok_all[c] = hp.astype(bf16)
        hid.across(c)
        return carry

    lax.fori_loop(0, nc, scan, 0)

    def xpart(k, carry):
        to = lax.rem(pc.f + k, F)
        rows = pl.ds(pl.multiple_of(to * Dl, Dl), Dl)
        R.xp[to] = mm(R.hid_t[rows, :], R.dpx[...]).astype(bf16)

        @pl.when(k < F)
        def _():
            rcopy(
                R.xp.at[to], R.xr.at[k - 1], R.xs0.at[k - 1], R.xs1.at[k - 1], fsdp=to
            ).start()
        return carry

    lax.fori_loop(1, F + 1, xpart, 0)
    diag = lax.broadcasted_iota(jnp.int32, (8, 128), 0) == lax.broadcasted_iota(
        jnp.int32, (8, 128), 1
    )

    def along(v):
        return jnp.sum(jnp.where(diag, jnp.sum(v, axis=1, keepdims=True), 0.0), axis=0, keepdims=True)

    dskip = jnp.sum(
        jnp.where(diag, mm(sel, R.acc[7:8, :cp], 1, 1, HI), 0.0), axis=0, keepdims=True
    )
    R.acc[7:8, :] = jnp.concatenate(
        [along(R.hacc[0]), along(R.hacc[1]), dskip, jnp.zeros((1, D - 384), f32)], axis=1
    )
    for k in range(1, F):
        to = lax.rem(pc.f + k, F)
        rcopy(
            R.acc, R.ar.at[k - 1], R.as0.at[k - 1], R.as1.at[k - 1], fsdp=to
        ).start()

    def hid_column(i, carry):
        hid.column(pc.Z - 1 - i)
        return carry

    lax.fori_loop(0, pc.Z, hid_column, 0)
    total = R.acc[...]
    for k in range(1, F):
        r = R.ar.at[k - 1]
        rcopy(r, r, R.as0.at[k - 1], R.as1.at[k - 1], fsdp=pc.f).wait_recv()
        total = total + R.ar[k - 1]
    R.asum[...] = total
    for k in range(1, S):
        rcopy(
            R.asum, O.sm.at[pc.s], R.as2.at[k], R.as3.at[pc.s], seq=lax.rem(pc.s + k, S)
        ).start()
    own(R.asum, O.sm.at[pc.s], 1).start()
    R.xred[...] = xs.total().astype(bf16)
    xg.start()
    own(R.xred, O.gx.at[pc.s], 2).start()

    mine = tok[...].astype(f32)
    O.block[...] = (mine + blk.total()).astype(bf16)
    for k in range(pc.Z):
        for q in range(1, pc.X):
            og.wait(pc.blk(k, q))
    own(R.ored, O.go_s.at[pc.s], 4).wait()
    for k in range(1, F):
        to = lax.rem(pc.f + k, F)
        rcopy(
            O.go_s.at[pl.ds(to * per, per)], O.go.at[pc.f], R.gs0.at[k], R.gs1.at[pc.f],
            fsdp=to,
        ).start()
    own(O.go_s.at[pl.ds(pc.f * per, per)], O.go.at[pc.f], 3).start()
    scale = lax.rsqrt(jnp.mean(mine * mine, axis=1, keepdims=True) + epsilon)
    e = hid.total() * small[6:7, :]
    mean = jnp.mean(e * mine, axis=1, keepdims=True)
    O.input[...] = cot[...].astype(f32) + scale * e - scale * scale * scale * mine * mean

    for k in range(1, pc.Z):
        b = pc.blk(k, 0)
        xg.wait(b)
        xg.across(O.gx.at[b], b, k)
    for k in range(pc.Z):
        for q in range(1, pc.X):
            zg.wait(pc.blk(k, q))
    for k in range(1, F):
        o = lax.rem(pc.f + k, F)
        r = O.go.at[o]
        rcopy(r, r, R.gs0.at[0], R.gs1.at[o], fsdp=pc.f).wait_recv()
    for k in range(1, S):
        o = lax.rem(pc.s + k, S)
        r = O.sm.at[o]
        rcopy(r, r, R.as2.at[0], R.as3.at[o], seq=pc.s).wait_recv()
    for k in range(pc.Z):
        for q in range(1, pc.X):
            xg.wait(pc.blk(k, q))
    own(R.zred, O.gz.at[pc.s], 0).wait()
    own(R.asum, O.sm.at[pc.s], 1).wait()
    own(R.xred, O.gx.at[pc.s], 2).wait()
    own(O.go_s.at[pl.ds(pc.f * per, per)], O.go.at[pc.f], 3).wait()
    for a in (blk, hid, zs, os_, xs, zg, og, xg):
        a.drain()
    for k in range(1, F):
        r = R.ar.at[k - 1]
        rcopy(r, r, R.as0.at[k - 1], R.as1.at[0], fsdp=pc.f).wait_send()
        r = O.go.at[0]
        rcopy(r, r, R.gs0.at[k], R.gs1.at[0], fsdp=pc.f).wait_send()
    for k in range(1, S):
        rcopy(R.asum, R.asum, R.as2.at[k], R.as3.at[0], seq=pc.s).wait_send()


def tight(cfg):
    S, F, T, D, cp, WC = cfg
    return S * T * D * 2 > 2**22


def bwd_scratch(cfg):
    S, F, T, D, cp, WC = cfg
    L = S * T
    Dl = D // F
    C = cp + 2 * N
    Z, X = 4, S // 4
    WX = WC - cp
    cr = cp // F
    V = pltpu.VMEM
    sem = pltpu.SemaphoreType.DMA
    n_ag = Z - 1 + Z * (X - 1)
    out = SimpleNamespace(
        acc=V((8, D), f32),
        asum=V((8, D), f32),
        ar=V((F - 1, 8, D), f32),
        hacc=V((2, 8, 128), f32),
        dstate=V((N, cp), f32),
        head=V((8, C), f32),
        mn_t=V((cp, L), bf16),
        dpx=V((L, WX), bf16),
        brx=V((Z, X - 1, T, D), bf16),
        brz=V((Z - 1, T, D), bf16),
        hrx=V((Z, X - 1, T, D), bf16),
        hrz=V((Z - 1, T, D), bf16),
        zp=V((F, Dl, cp), bf16),
        zr=V((F - 1, Dl, cp), bf16),
        zred=V((Dl, cp), bf16),
        op=V((F, cr, D), bf16),
        orecv=V((F - 1, cr, D), bf16),
        ored=V((cr, D), bf16),
        xp=V((F, Dl, WX), bf16),
        xr=V((F - 1, Dl, WX), bf16),
        xred=V((Dl, WX), bf16),
        lsem=sem((5,)),
        as0=sem((F,)), as1=sem((F,)), as2=sem((S,)), as3=sem((S,)),
        gs0=sem((F,)), gs1=sem((F,)),
    )
    if not tight(cfg):
        out.bp = V((S, T, D), bf16)

    def both():
        return sem((S,)), sem((Z, X - 1)), sem((Z,)), sem((Z - 1,))

    out.bs0, out.bs1, out.bs2, out.bs3 = both()
    out.hs0, out.hs1, out.hs2, out.hs3 = both()
    out.zs0, out.zs1, out.gz0, out.gz1 = sem((F,)), sem((F,)), sem((n_ag,)), sem((S,))
    out.os0, out.os1, out.go0, out.go1 = sem((F,)), sem((F,)), sem((n_ag,)), sem((S,))
    out.xs0, out.xs1, out.gx0, out.gx1 = sem((F,)), sem((F,)), sem((n_ag,)), sem((S,))
    return out


def shards(tokens, in_weight, step_weight, conv_kernel, conv_bias, step_bias, log_decay,
           skip_gain, gate_gain, norm_gain, out_weight, cotangent):
    S = lax.axis_size("seq")
    F = lax.axis_size("fsdp")
    _, T, D = tokens.shape
    inner = out_weight.shape[0] * F
    heads = step_weight.shape[1]
    cols = inner // S
    cp = -(-cols // 128) * 128
    C = cp + 2 * N
    WC = 2 * cp + 2 * N + 128
    WX = WC - cp
    Dl = D // F
    cr = cp // F
    per = S // F
    cfg = (S, F, T, D, cp, WC)
    wp, wo, sm = prep(cfg, in_weight, step_weight, conv_kernel, conv_bias, step_bias, log_decay,
                      skip_gain, gate_gain, norm_gain, out_weight)
    scratch = {**vars(fwd_scratch(cfg)), **vars(bwd_scratch(cfg))}
    names = list(scratch)
    outs = dict(
        block=jax.ShapeDtypeStruct((T, D), bf16),
        input=jax.ShapeDtypeStruct((T, D), f32),
        gz=jax.ShapeDtypeStruct((S, Dl, cp), bf16),
        gx=jax.ShapeDtypeStruct((S, Dl, WX), bf16),
        go=jax.ShapeDtypeStruct((F, per, cr, D), bf16),
        go_s=jax.ShapeDtypeStruct((S, cr, D), bf16),
        sm=jax.ShapeDtypeStruct((S, 8, D), f32),
    )
    on = list(outs)

    def kern(tok, cot, wp, wo, sm, *rest):
        O = SimpleNamespace(**dict(zip(on, rest[: len(on)])))
        R = SimpleNamespace(**dict(zip(names, rest[len(on) :])))
        if tight(cfg):
            R.bp = R.cot_all
        body_fwd(cfg, tok, cot, wp, wo, sm, R)
        body_bwd(cfg, float(inner), tok, cot, R, O)

    v = pl.BlockSpec(memory_space=pltpu.VMEM)
    hbm = pl.BlockSpec(memory_space=pl.ANY)
    res = pl.pallas_call(
        kern,
        out_shape=[outs[n] for n in on],
        in_specs=[v, v, hbm, hbm, v],
        out_specs=[v, v, hbm, hbm, hbm, hbm, hbm],
        scratch_shapes=[scratch[n] for n in names],
        compiler_params=pltpu.CompilerParams(
            collective_id=0, has_side_effects=True, vmem_limit_bytes=VMEM_LIMIT
        ),
    )(tokens[0], cotangent[0], wp, wo, sm)
    G = SimpleNamespace(**dict(zip(on, res)))
    gz, gx, go, gs = G.gz, G.gx, G.go, G.sm
    fpos = lax.axis_index("fsdp")

    def join(a, n):
        return jnp.moveaxis(a[..., :n], 0, -2).reshape(a.shape[1:-1] + (-1,))

    hg = heads // S
    in_grad = jnp.concatenate(
        [
            join(gz, cols),
            join(gx, cols),
            jnp.sum(gx[:, :, cp:C].astype(f32), axis=0).astype(bf16),
        ],
        axis=1,
    ).astype(f32)
    step_grad = join(gx[:, :, C:], hg).astype(f32)
    out_grad = (
        jnp.moveaxis(go, 0, 1).reshape(per, cp, D)[:, :cols].reshape(per * cols, D).astype(f32)
    )

    def mine(a, axis):
        n = a.shape[axis] // F
        return lax.dynamic_slice_in_dim(a, fpos * n, n, axis)

    conv = jnp.concatenate(
        [join(gs[:, 0:5], cols), jnp.sum(gs[:, 0:5, cp:C], axis=0)], axis=1
    )
    conv = mine(conv, 1)
    return (
        G.block[None],
        G.input[None],
        in_grad,
        step_grad,
        conv[0:4],
        conv[4],
        mine(join(gs[:, 7], hg), 0),
        mine(join(gs[:, 7, 128:], hg), 0),
        mine(join(gs[:, 7, 256:], hg), 0),
        mine(join(gs[:, 5], cols), 0),
        mine(jnp.sum(gs[:, 6], axis=0), 0),
        out_grad,
    )


def solution(mesh):
    row = P("fsdp", None)
    tok = P("fsdp", "seq", None)
    one = P("fsdp")
    return jax.shard_map(
        shards,
        mesh=mesh,
        in_specs=(tok, row, row, P(None, "fsdp"), one, one, one, one, one, one, row, tok),
        out_specs=(tok, tok, row, row, P(None, "fsdp"), one, one, one, one, one, one, row),
        check_vma=False,
    )
```

```python
from types import SimpleNamespace

import jax
import jax.numpy as jnp
from jax import lax
from jax.experimental import pallas as pl
from jax.experimental.pallas import tpu as pltpu
from jax.sharding import PartitionSpec as P

N = 128
HEAD = 64
Q = 128
epsilon = 1e-05
bf16 = jnp.bfloat16
f32 = jnp.float32
MESH = pl.DeviceIdType.MESH
HI = lax.Precision.HIGHEST
VMEM_LIMIT = 64 * 1024 * 1024 - 65536


def mm(a, b, da=1, db=0, precision=None):
    return lax.dot_general(
        a, b, (((da,), (db,)), ((), ())), preferred_element_type=f32, precision=precision
    )


def rcopy(src, dst, ss, rs, **dev):
    return pltpu.make_async_remote_copy(
        src_ref=src, dst_ref=dst, send_sem=ss, recv_sem=rs, device_id=dev, device_id_type=MESH
    )


class Axis:
    def __init__(self, name, outer, inner):
        self.name, self.outer, self.inner = name, outer, inner
        self.me = lax.axis_index(name)
        self.o = self.me // inner
        self.i = lax.rem(self.me, inner)

    def near(self, k):
        half = self.outer // 2
        side = self.o // half
        m = self.o + side * (self.outer - 1 - 2 * self.o)
        at = jnp.where(k == 0, m, k - m * ((3 - k) // 2))
        return at + side * (self.outer - 1 - 2 * at)

    def blk(self, k, q):
        return self.near(k) * self.inner + lax.rem(self.i + q, self.inner)

    def to(self, d):
        return {self.name: d}


class Place:
    def __init__(self, S, F):
        self.S, self.F = S, F
        self.seq = Axis("seq", 4, S // 4)
        self.fsdp = Axis("fsdp", F // 2, 2)
        self.Z, self.X = 4, S // 4
        self.s, self.z, self.x = self.seq.me, self.seq.o, self.seq.i
        self.f = self.fsdp.me
        self.blk = self.seq.blk

    def barrier(self):
        bar = pltpu.get_barrier_semaphore()
        n = 0
        for k in range(1, self.S):
            pl.semaphore_signal(
                bar, inc=1, device_id={"seq": lax.rem(self.s + k, self.S)}, device_id_type=MESH
            )
            n += 1
        for k in range(1, self.F):
            pl.semaphore_signal(
                bar, inc=1, device_id={"fsdp": lax.rem(self.f + k, self.F)}, device_id_type=MESH
            )
            n += 1
        pl.semaphore_wait(bar, n)


class Gather:
    def __init__(self, ax, src, buf, sems):
        self.ax, self.src, self.buf = ax, src, buf
        self.ss, self.rs = sems

    def send(self, src, b, sem, dst):
        rcopy(src, self.buf.at[b], self.ss.at[sem], self.rs.at[b], **self.ax.to(dst)).start()

    def start(self):
        ax = self.ax
        for sem, d in ((0, 1), (1, -1)):

            @pl.when(jnp.logical_and(ax.o + d >= 0, ax.o + d < ax.outer))
            def _():
                self.send(self.src, ax.me, sem, ax.me + d * ax.inner)

        self.across(self.src, ax.me, 0)

    def across(self, src, b, k):
        ax = self.ax
        for q in range(1, ax.inner):
            sem = ax.outer + 1 + k * (ax.inner - 1) + q - 1
            self.send(src, b, sem, ax.o * ax.inner + lax.rem(ax.i + q, ax.inner))

    def onward(self, k):
        ax = self.ax
        return ax.o + jnp.where(ax.o > ax.near(k), 1, -1)

    def relay(self, k):
        ax = self.ax
        b = ax.blk(k, 0)
        self.wait(b)
        nxt = self.onward(k)

        @pl.when(jnp.logical_and(nxt >= 0, nxt < ax.outer))
        def _():
            self.send(self.buf.at[b], b, 1 + k, nxt * ax.inner + ax.i)

        self.across(self.buf.at[b], b, k)

    def wait(self, b):
        r = self.buf.at[b]
        rcopy(r, r, self.ss.at[0], self.rs.at[b], **self.ax.to(self.ax.me)).wait_recv()

    def wait_across(self):
        for k in range(self.ax.outer):
            for q in range(1, self.ax.inner):
                self.wait(self.ax.blk(k, q))

    def drain(self):
        ax = self.ax

        def done(sem):
            rcopy(
                self.src, self.src, self.ss.at[sem], self.rs.at[0], **ax.to(ax.me)
            ).wait_send()

        for sem, d in ((0, 1), (1, -1)):

            @pl.when(jnp.logical_and(ax.o + d >= 0, ax.o + d < ax.outer))
            def _():
                done(sem)

        for k in range(1, ax.outer):
            nxt = self.onward(k)

            @pl.when(jnp.logical_and(nxt >= 0, nxt < ax.outer))
            def _():
                done(1 + k)

        for sem in range(ax.outer * (ax.inner - 1)):
            done(ax.outer + 1 + sem)


def gather_sems(outer, inner):
    sem = pltpu.SemaphoreType.DMA
    return sem((outer + 1 + outer * (inner - 1),)), sem((outer * inner,))


def pair(col, p):
    lane = lax.broadcasted_iota(jnp.int32, (col.shape[0], 128), 1)
    return jnp.where(lane < HEAD, col[:, 2 * p : 2 * p + 1], col[:, 2 * p + 1 : 2 * p + 2])


def spread(col, cp):
    return jnp.concatenate([pair(col, p) for p in range(cp // 128)], axis=1)


def sigmoid(v):
    return 1.0 / (1.0 + jnp.exp(-v))


def softplus(v):
    return jnp.maximum(v, 0.0) + jnp.log1p(jnp.exp(-jnp.abs(v)))


def tri(shape, flip=False):
    i = lax.broadcasted_iota(jnp.int32, shape, 0)
    j = lax.broadcasted_iota(jnp.int32, shape, 1)
    return j >= i if flip else i >= j


def split(x2):
    lane = lax.broadcasted_iota(jnp.int32, x2.shape, 1)
    return jnp.concatenate([jnp.where(lane < HEAD, x2, 0), jnp.where(lane >= HEAD, x2, 0)], axis=0)


def chunk_inputs(c, ext, rawb, small, cp):
    r0 = pl.multiple_of(c * Q, Q)
    v = ext[pl.ds(r0, Q + 16), :].astype(f32)
    C = cp + 2 * N
    taps = [pltpu.roll(v, 3 - k, 0)[16:] if k < 3 else v[16:] for k in range(4)]
    summed = small[4:5, :C]
    for k in range(4):
        summed = summed + small[k : k + 1, :C] * taps[k]
    sig = sigmoid(summed)
    raw = rawb[pl.ds(r0, Q), :].astype(f32) + small[7:8, 0:128]
    dt = softplus(raw)
    rate = -jnp.exp(small[7:8, 128:256])
    cum = mm(tri((Q, Q)).astype(f32), dt * rate, precision=HI)
    return taps, summed, sig, raw, dt, rate, cum


def skip_row(small, cp):
    return spread(small[7:8, 256:384], cp)


def tight(cfg):
    S, F, T, D, cp, WC = cfg
    return S * T * D * 2 > 2**22


def lanes_from(row, shift, width, size):
    n = row.shape[1]
    if n < width:
        row = jnp.concatenate([row, jnp.zeros((row.shape[0], width - n), f32)], axis=1)
    row = pltpu.roll(row, lax.rem(shift + width, width), 1)
    return row[:, :size]


def small_rows(cfg, dims, flat, pc):
    S, F, T, D, cp, WC = cfg
    inner, heads, cols = dims
    conv = inner + 2 * N
    cl, gl, nl, hl = conv // F, inner // F, D // F, heads // F
    up = lambda n: -(-n // 128) * 128
    at = 0
    parts = []
    for n in [cl] * 5 + [gl, nl, hl, hl, hl]:
        parts.append(flat[:, at : at + up(n)])
        at += up(n)
    rows = jnp.concatenate(parts[:5] + [jnp.zeros((3, up(cl)), f32)], axis=0)
    lane = lax.broadcasted_iota(jnp.int32, (8, cp), 1)
    xs = lanes_from(rows, cl * pc.f - cols * pc.s, conv, cp)
    bc = lanes_from(rows, cl * pc.f - inner, conv, 2 * N)
    gate = lanes_from(parts[5], gl * pc.f - cols * pc.s, inner, cp)
    if cols < cp:
        xs = jnp.where(lane < cols, xs, 0.0)
        gate = jnp.where(lane[0:1] < cols, gate, 0.0)
    norm = lanes_from(parts[6], nl * pc.f, D, D)
    hg = heads // S
    hv = jnp.concatenate(parts[7:10] + [jnp.zeros((5, 128), f32)], axis=0)
    hv = lanes_from(hv, hl * pc.f - hg * pc.s, 128, 128)
    hv = jnp.where(lane[:, :128] < hg, hv, 0.0)

    def wide(v):
        return jnp.concatenate([v, jnp.zeros((v.shape[0], D - v.shape[1]), f32)], axis=1)

    return jnp.concatenate(
        [
            wide(jnp.concatenate([xs, bc], axis=1)[0:5]),
            wide(gate),
            norm,
            wide(jnp.concatenate([hv[0:1], hv[1:2], hv[2:3]], axis=1)),
        ],
        axis=0,
    )


def body_fwd(cfg, dims, tok, cot, wsrc, wo, flat, R):
    S, F, T, D, cp, WC = cfg
    inner, heads, cols = dims
    L = S * T
    C = cp + 2 * N
    per = S // F
    pc = Place(S, F)
    own = R.w_all.at[pc.f]
    if len(wsrc) == 1:
        parts = [(wsrc[0], own)]
    else:
        win, step = wsrc
        col = pl.multiple_of(pc.s * cols, cols)
        parts = [
            (win.at[:, pl.ds(col, cols)], own.at[:, pl.ds(0, cols)]),
            (win.at[:, pl.ds(inner + col, cols)], own.at[:, pl.ds(cols, cols)]),
            (win.at[:, pl.ds(2 * inner, 2 * N)], own.at[:, pl.ds(2 * cols, 2 * N)]),
            (step, own.at[:, pl.ds(2 * cols + 2 * N, 128)]),
        ]
    parts = [pltpu.make_async_copy(a, b, R.wsem.at[i]) for i, (a, b) in enumerate(parts)]
    for c in parts:
        c.start()
    R.sm_own[...] = small_rows(cfg, dims, flat[...].astype(f32), pc)
    pc.barrier()
    tg = Gather(pc.seq, tok, R.tok_all, (R.ss_t, R.rs_t))
    cg = Gather(pc.seq, cot, R.cot_all, (R.ss_c, R.rs_c))
    wg = Gather(pc.fsdp, own, R.w_all, (R.ss_w, R.rs_w))
    first = lax.rem(pc.s, per)
    owner = pc.s // per
    wogs = []
    if not tight(cfg):
        for p in range(per):
            at = lax.rem(first + p, per)
            wogs.append(
                Gather(pc.fsdp, wo.at[at], R.w_out.at[at], (R.ss_o.at[p], R.rs_o.at[p]))
            )
    sm = R.sm_own
    tg.start()
    for k in range(1, F):
        to = lax.rem(pc.f + k, F)
        rcopy(sm, R.sm_all.at[pc.f], R.ss_m.at[k], R.rs_m.at[pc.f], fsdp=to).start()
    for c in parts:
        c.wait()
    wg.start()
    cg.start()
    keep = []
    for p in range(len(wogs)):
        wogs[p].start()
        at = lax.rem(first + p, per)
        keep.append(pltpu.make_async_copy(wo.at[at], R.w_out.at[at, pc.f], R.osem.at[p]))
    if tight(cfg):
        keep.append(pltpu.make_async_copy(wo, R.wo_g, R.osem.at[0]))

        @pl.when(pc.f == owner)
        def _():
            keep[0].start()
            for k in range(1, F):
                to = lax.rem(pc.f + k, F)
                rcopy(wo, R.wo_g, R.ss_o.at[k], R.rs_o.at[0], fsdp=to).start()
    else:
        for c in keep:
            c.start()
    R.tok_all[pc.s] = tok[...]
    R.cot_all[pc.s] = cot[...]
    R.sm_all[pc.f] = sm[...]
    R.ext[0:16, :] = jnp.zeros((16, C), bf16)
    for k in range(1, F):
        o = lax.rem(pc.f + k, F)
        rcopy(sm, R.sm_all.at[o], R.ss_m.at[0], R.rs_m.at[o], fsdp=pc.f).wait_recv()
    total = R.sm_all[0]
    for k in range(1, F):
        total = total + R.sm_all[k]
    R.small[...] = total
    small = R.small
    for k in range(1, F // 2):
        wg.relay(k)
    wg.wait_across()

    def project(j, carry):
        k, q = j // pc.X, lax.rem(j, pc.X)
        b = pc.blk(k, q)

        @pl.when(q > 0)
        def _():
            tg.wait(b)

        @pl.when(jnp.logical_and(q == 0, k > 0))
        def _():
            tg.relay(k)

        @pl.when(j == S - 1)
        def _():
            cg.relay(1)

        r = R.tok_all[b].astype(f32)
        scale = lax.rsqrt(jnp.mean(r * r, axis=1, keepdims=True) + epsilon)
        h = r * scale * small[6:7, :]
        r0 = pl.multiple_of(b * T, T)
        R.hid_t[:, pl.ds(r0, T)] = h.T.astype(bf16)
        out = mm(h.astype(bf16), R.w_all[...].reshape(D, WC)).astype(bf16)
        R.zb[pl.ds(r0, T), :] = out[:, :cp]
        R.rawb[pl.ds(r0, T), :] = out[:, 2 * cp + 2 * N :]
        R.ext[pl.ds(r0 + 16, T), :] = out[:, cp : 2 * cp + 2 * N]
        return carry

    lax.fori_loop(0, S, project, 0)
    R.state[...] = jnp.zeros((N, cp), f32)
    ones = jnp.ones((8, cp), f32)

    def forward(c, carry):
        @pl.when(jnp.logical_or(c == 2, c == 4))
        def _():
            cg.relay(c // 2 + 1)

        r0 = pl.multiple_of(c * Q, Q)
        taps, summed, sig, raw, dt, rate, cum = chunk_inputs(c, R.ext, R.rawb, small, cp)
        act = summed * sig
        x = act[:, :cp]
        bb = act[:, cp : cp + N].astype(bf16)
        cb = act[:, cp + N :].astype(bf16)
        cum_t = cum.T
        dt_t = dt.T
        scores = mm(cb, bb, 1, 1)
        causal = tri((Q, Q))
        parts = []
        for p in range(cp // 128):
            mix = []
            for h in (2 * p, 2 * p + 1):
                gap = jnp.where(causal, cum[:, h : h + 1] - cum_t[h : h + 1, :], -1e30)
                mix.append((jnp.exp(gap) * scores * dt_t[h : h + 1, :]).astype(bf16))
            parts.append(
                mm(jnp.concatenate(mix, axis=1), split(x[:, 128 * p : 128 * p + 128]).astype(bf16))
            )
        state = R.state[...]
        R.states[c] = state
        last = cum[Q - 1 : Q, :]
        y = jnp.concatenate(parts, axis=1) + mm(cb, state.astype(bf16)) * spread(jnp.exp(cum), cp)
        y = y + skip_row(small, cp) * x
        wx = (spread(jnp.exp(last - cum) * dt, cp) * x).astype(bf16)
        R.state[...] = spread(jnp.exp(last), cp) * state + mm(bb, wx, 0, 0)
        R.y[pl.ds(r0, Q), :] = y
        z = R.zb[pl.ds(r0, Q), :].astype(f32)
        gated = (y * (z * sigmoid(z))).astype(bf16)
        R.dpx[pl.ds(r0, Q), :cp] = gated
        g32 = gated.astype(f32)
        R.st[0:1, pl.ds(r0, Q)] = mm(ones, g32 * g32, 1, 1, HI)[0:1]
        return carry

    lax.fori_loop(0, L // Q, forward, 0)

    if tight(cfg):
        group = R.wo_g

        @pl.when(pc.f != owner)
        def _():
            rcopy(wo, R.wo_g, R.ss_o.at[0], R.rs_o.at[0], fsdp=pc.f).wait_recv()

        @pl.when(pc.f == owner)
        def _():
            keep[0].wait()
    else:
        group = R.w_out.at[first, owner]
        for c in keep:
            c.wait()
        for k in range(1, F // 2):
            wogs[0].relay(k)
        wogs[0].wait_across()

    def mixed(j, carry):
        k, q = j // pc.X, lax.rem(j, pc.X)
        b = pc.blk(k, q)

        @pl.when(q > 0)
        def _():
            cg.wait(b)

        r0 = pl.multiple_of(b * T, T)
        mg = mm(R.cot_all[b], group[...], 1, 1)
        R.mg[pl.ds(r0, T), :] = mg
        g = mg * small[5:6, :cp] * R.dpx[pl.ds(r0, T), :cp].astype(f32)
        R.st[1:2, pl.ds(r0, T)] = mm(ones, g, 1, 1, HI)[0:1]
        return carry

    lax.fori_loop(0, S, mixed, 0)
    for k in range(1, S):
        rcopy(
            R.st, R.st_all.at[pc.s], R.ss_s.at[k], R.rs_s.at[pc.s],
            seq=lax.rem(pc.s + k, S),
        ).start()
    R.st_all[pc.s] = R.st[...]
    for k in range(1, S):
        o = lax.rem(pc.s + k, S)
        rcopy(R.st, R.st_all.at[o], R.ss_s.at[0], R.rs_s.at[o], seq=pc.s).wait_recv()
    total = R.st_all[0]
    for k in range(1, S):
        total = total + R.st_all[k]
    R.stats[...] = total

    if not tight(cfg):
        for g in wogs[1:]:
            for k in range(1, F // 2):
                g.relay(k)
            g.wait_across()
    for g in [tg, cg, wg] + wogs:
        g.drain()
    for k in range(1, S):
        rcopy(R.st, R.st, R.ss_s.at[k], R.rs_s.at[0], seq=pc.s).wait_send()
    for k in range(1, F):
        rcopy(sm, sm, R.ss_m.at[k], R.rs_m.at[0], fsdp=pc.f).wait_send()
    if tight(cfg):

        @pl.when(pc.f == owner)
        def _():
            for k in range(1, F):
                rcopy(wo, wo, R.ss_o.at[k], R.rs_o.at[0], fsdp=pc.f).wait_send()


def fwd_scratch(cfg):
    S, F, T, D, cp, WC = cfg
    L = S * T
    Dl = D // F
    C = cp + 2 * N
    V = pltpu.VMEM
    sem = pltpu.SemaphoreType.DMA
    per = S // F
    seq = gather_sems(4, S // 4)
    fsdp = gather_sems(F // 2, 2)
    out = SimpleNamespace(
        tok_all=V((S, T, D), bf16),
        cot_all=V((S, T, D), bf16),
        w_all=V((F, Dl, WC), bf16),
        sm_own=V((8, D), f32),
        sm_all=V((F, 8, D), f32),
        small=V((8, D), f32),
        hid_t=V((D, L), bf16),
        zb=V((L, cp), bf16),
        rawb=V((L, 128), bf16),
        ext=V((16 + L, C), bf16),
        state=V((N, cp), f32),
        states=V((L // Q, N, cp), f32),
        y=V((L, cp), f32),
        mg=V((L, cp), f32),
        st=V((2, L), f32),
        st_all=V((S, 2, L), f32),
        stats=V((2, L), f32),
        ss_t=seq[0],
        rs_t=seq[1],
        ss_c=seq[0],
        rs_c=seq[1],
        ss_w=fsdp[0],
        rs_w=fsdp[1],
        ss_m=sem((F,)),
        rs_m=sem((F,)),
        wsem=sem((4,)),
        osem=sem((per,)),
        ss_s=sem((S,)),
        rs_s=sem((S,)),
    )
    if tight(cfg):
        out.wo_g = V((cp, D), bf16)
        out.ss_o = out.rs_o = sem((F,))
    else:
        out.w_out = V((per, F, cp, D), bf16)
        out.ss_o = sem((per,) + fsdp[0].shape)
        out.rs_o = sem((per,) + fsdp[1].shape)
    return out


class Scatter:
    def __init__(self, pc, part, rx, rz, sems):
        self.pc, self.part, self.rx, self.rz = pc, part, rx, rz
        self.ssx, self.rsx, self.ssz, self.rsz = sems

    def across(self, b):
        pc = self.pc
        zb, xb = b // pc.X, lax.rem(b, pc.X)

        @pl.when(xb != pc.x)
        def _():
            slot = lax.rem(pc.x - xb - 1 + pc.X, pc.X)
            rcopy(
                self.part.at[b], self.rx.at[zb, slot], self.ssx.at[b], self.rsx.at[zb, slot],
                seq=pc.z * pc.X + xb,
            ).start()

    def column(self, zb):
        pc = self.pc
        b = zb * pc.X + pc.x
        total = self.part[b].astype(f32)
        for q in range(pc.X - 1):
            r = self.rx.at[zb, q]
            rcopy(r, r, self.ssx.at[0], self.rsx.at[zb, q], seq=pc.s).wait_recv()
            total = total + self.rx[zb, q].astype(f32)
        self.part[b] = total.astype(bf16)

        @pl.when(zb != pc.z)
        def _():
            slot = lax.rem(pc.z - zb - 1 + pc.Z, pc.Z)
            rcopy(
                self.part.at[b], self.rz.at[slot], self.ssz.at[zb], self.rsz.at[slot], seq=b
            ).start()

    def total(self):
        pc = self.pc
        out = self.part[pc.s].astype(f32)
        for q in range(pc.Z - 1):
            r = self.rz.at[q]
            rcopy(r, r, self.ssz.at[0], self.rsz.at[q], seq=pc.s).wait_recv()
            out = out + self.rz[q].astype(f32)
        return out

    def drain(self):
        pc = self.pc
        r = self.rz.at[0]
        for b in range(pc.S):

            @pl.when(b % pc.X != pc.x)
            def _():
                rcopy(r, r, self.ssx.at[b], self.rsz.at[0], seq=pc.s).wait_send()

        for zb in range(pc.Z):

            @pl.when(zb != pc.z)
            def _():
                rcopy(r, r, self.ssz.at[zb], self.rsz.at[0], seq=pc.s).wait_send()


class Shared:
    def __init__(self, pc, part, recv, ss, rs):
        self.pc, self.part, self.recv, self.ss, self.rs = pc, part, recv, ss, rs

    def send(self, k):
        pc = self.pc
        to = lax.rem(pc.f + k, pc.F)
        rcopy(
            self.part.at[to], self.recv.at[k - 1], self.ss.at[k - 1], self.rs.at[k - 1], fsdp=to
        ).start()

    def total(self):
        pc = self.pc
        out = self.part[pc.f].astype(f32)
        for k in range(1, pc.F):
            r = self.recv.at[k - 1]
            rcopy(r, r, self.ss.at[k - 1], self.rs.at[k - 1], fsdp=pc.f).wait_recv()
            out = out + self.recv[k - 1].astype(f32)
        return out

    def drain(self):
        for k in range(1, self.pc.F):
            r = self.recv.at[k - 1]
            rcopy(r, r, self.ss.at[k - 1], self.rs.at[k - 1], fsdp=self.pc.f).wait_send()


def body_bwd(cfg, dims, tok, cot, R, O):
    S, F, T, D, cp, WC = cfg
    inner = float(dims[0])
    L = S * T
    C = cp + 2 * N
    Dl = D // F
    nc = L // Q
    cr = cp // F
    per = S // F
    bh = Dl // S
    pc = Place(S, F)
    small = R.small
    if tight(cfg):
        blk = Scatter(pc, R.bp, R.brx, R.brz, (R.bs0, R.bs1, R.bs2, R.bs3))
    hid = Scatter(pc, R.tok_all, R.hrx, R.hrz, (R.hs0, R.hs1, R.hs2, R.hs3))
    zs = Shared(pc, R.zp, R.zr, R.zs0, R.zs1)
    os_ = Shared(pc, R.op, R.orecv, R.os0, R.os1)
    xs = Shared(pc, R.xp, R.xr, R.xs0, R.xs1)
    bs = Shared(pc, R.cp_, R.cr_, R.cs0, R.cs1)
    zg = Gather(pc.seq, R.zred, O.gz, (R.gz0, R.gz1))
    og = Gather(pc.seq, R.ored, O.go_s, (R.go0, R.go1))
    xg = Gather(pc.seq, R.xred, O.gx, (R.gx0, R.gx1))
    sg = Gather(pc.seq, R.asum, O.sm, (R.as2, R.as3))

    def direct(src, dst, ss, rs, to):
        rcopy(src, dst.at[pc.s], ss.at[to], rs.at[pc.s], seq=to).start()

    def arrived(dst, ss, rs):
        for k in range(1, S):
            o = lax.rem(pc.s + k, S)
            r = dst.at[o]
            rcopy(r, r, ss.at[0], rs.at[o], seq=pc.s).wait_recv()

    def sent(src, ss, rs):
        for k in range(1, S):
            rcopy(src, src, ss.at[lax.rem(pc.s + k, S)], rs.at[0], seq=pc.s).wait_send()

    def own(src, dst, i):
        return pltpu.make_async_copy(src, dst, R.lsem.at[i])

    gate = small[5:6, :cp]
    R.acc[...] = jnp.zeros((16, D), f32)
    R.hacc[...] = jnp.zeros((2, 8, 128), f32)
    R.dstate[...] = jnp.zeros((N, cp), f32)
    R.head[...] = jnp.zeros((8, C), f32)

    def first(i, carry):
        c = lax.rem(pc.s + 1 + i, nc)
        r0 = pl.multiple_of(c * Q, Q)
        rows = pl.ds(r0, Q)
        st = jnp.concatenate([R.stats[:, rows], jnp.zeros((6, Q), f32)], axis=0).T
        scale = lax.rsqrt(st[:, 0:1] / inner + epsilon)
        mean = st[:, 1:2] / inner
        gated = R.dpx[rows, :cp].astype(f32)
        mg = R.mg[rows, :]
        ng = gated * scale
        mn = ng * gate
        R.acc[5:6, :cp] += jnp.sum(mg * ng, axis=0, keepdims=True)
        gg = (scale * (mg * gate) - scale * scale * scale * gated * mean).astype(bf16).astype(f32)
        z = R.zb[rows, :].astype(f32)
        sz = sigmoid(z)
        R.zb[rows, :] = (gg * R.y[rows, :] * (sz * (1.0 + z * (1.0 - sz)))).astype(bf16)
        R.mg[rows, :] = gg * (z * sz)
        R.mn_t[:, rows] = mn.T.astype(bf16)
        if tight(cfg):
            R.dpx[rows, :cp] = mn.astype(bf16)
        else:
            R.mn[c] = mn.astype(bf16)

            @pl.when(c != pc.s)
            def _():
                direct(R.mn.at[c], R.mall, R.ms0, R.ms1, c)

        return carry

    def block(i, carry):
        c = nc - 1 - i
        rows = pl.ds(pl.multiple_of(c * Q, Q), Q)
        R.bp[c] = mm(R.dpx[rows, :cp], R.wo_g[...]).astype(bf16)
        blk.across(c)
        return carry

    lax.fori_loop(0, nc, first, 0)

    def zpart(k, carry):
        to = lax.rem(pc.f + k, F)
        rows = pl.ds(pl.multiple_of(to * Dl, Dl), Dl)
        R.zp[to] = mm(R.hid_t[rows, :], R.zb[...]).astype(bf16)

        @pl.when(k < F)
        def _():
            rcopy(
                R.zp.at[to], R.zr.at[k - 1], R.zs0.at[k - 1], R.zs1.at[k - 1], fsdp=to
            ).start()
        return carry

    lax.fori_loop(1, F + 1, zpart, 0)
    W = 384

    def opart(j, carry):
        cols = pl.ds(pl.multiple_of(j * W, W), W)
        a = R.cot_all[:, :, cols].reshape(L, W)
        R.op[:, :, cols] = mm(R.mn_t[...], a).reshape(F, cr, W).astype(bf16)
        return carry

    lax.fori_loop(0, D // W, opart, 0)
    for k in range(1, F):
        os_.send(k)
    if tight(cfg):
        lax.fori_loop(0, nc, block, 0)

    sel = (
        lax.broadcasted_iota(jnp.int32, (8, cp), 1) // HEAD
        == lax.broadcasted_iota(jnp.int32, (8, cp), 0)
    ).astype(f32)
    sub = lax.broadcasted_iota(jnp.int32, (8, Q), 0)

    def scan(i, carry):
        c = nc - 1 - i
        r0 = pl.multiple_of(c * Q, Q)
        rows = pl.ds(r0, Q)

        if tight(cfg):

            @pl.when(i < pc.Z)
            def _():
                blk.column(pc.Z - 1 - i)

        @pl.when(i == 1)
        def _():
            R.zred[...] = zs.total().astype(bf16)
            zg.start()
            own(R.zred, O.gz.at[pc.s], 0).start()

        @pl.when(i == 2)
        def _():
            R.ored[...] = os_.total().astype(bf16)
            og.start()
            own(R.ored, O.go_s.at[pc.s], 5).start()

        @pl.when(jnp.logical_and(i >= 3, i < 3 + pc.Z - 1))
        def _():
            zg.relay(i - 2)

        @pl.when(jnp.logical_and(i >= 4, i < 4 + pc.Z - 1))
        def _():
            og.relay(i - 3)

        taps, summed, sig, raw, dt, rate, cum = chunk_inputs(c, R.ext, R.rawb, small, cp)
        act = summed * sig
        x = act[:, :cp]
        xb = x.astype(bf16)
        bb = act[:, cp : cp + N].astype(bf16)
        cb = act[:, cp + N :].astype(bf16)
        cum_t = cum.T
        dt_t = dt.T
        dy = R.mg[rows, :]
        dyb = dy.astype(bf16)
        last = cum[Q - 1 : Q, :]
        edy = spread(jnp.exp(cum), cp) * dy
        edyb = edy.astype(bf16)
        wdec = jnp.exp(last - cum)
        w = wdec * dt
        state = R.states[c]
        sb = state.astype(bf16)
        ds = R.dstate[...]
        dsb = ds.astype(bf16)
        ws = spread(w, cp)
        v = mm(bb, dsb)
        carr = mm(sel, edy * mm(cb, sb), 1, 1, HI)
        dw = mm(sel, x * v, 1, 1, HI)
        db = mm((ws * x).astype(bf16), dsb, 1, 1)
        dc = mm(edyb, sb, 1, 1)
        dlast = mm(sel, jnp.sum(state * ds, axis=0, keepdims=True), 1, 1, HI)
        R.dstate[...] = spread(jnp.exp(last), cp) * ds + mm(cb, edyb, 0, 0)
        scores = mm(bb, cb, 1, 1)
        seen = tri((Q, Q), True)
        dtb = dt_t[0:8].astype(bf16)
        dsc = jnp.zeros((Q, Q), f32)
        direct = jnp.zeros((8, Q), f32)
        onto = jnp.zeros((8, Q), f32)
        parts = []
        for p in range(cp // 128):
            cols = slice(128 * p, 128 * p + 128)
            g2 = mm(split(x[:, cols]).astype(bf16), dyb[:, cols], 1, 1)
            mix = []
            for h in (2 * p, 2 * p + 1):
                g = g2[:Q] if h % 2 == 0 else g2[Q:]
                decay = jnp.exp(jnp.where(seen, cum_t[h : h + 1, :] - cum[:, h : h + 1], -1e30))
                ls = decay * scores
                mix.append((ls * dt[:, h : h + 1]).astype(bf16))
                e = (g * ls).astype(bf16)
                dsc = dsc + g * decay * dt[:, h : h + 1]
                direct = direct + mm(jnp.where(sub == h, 1.0, 0.0).astype(bf16), e, 1, 1)
                onto = onto + mm(jnp.where(sub == h, dtb.astype(f32), 0.0).astype(bf16), e)
            parts.append(mm(jnp.concatenate(mix, axis=1), split(dy[:, cols]).astype(bf16)))
        dscb = dsc.astype(bf16)
        db = db + mm(dscb, cb)
        dc = dc + mm(dscb, bb, 0, 0)
        dx = skip_row(small, cp) * dy + ws * v + jnp.concatenate(parts, axis=1)
        R.acc[7:8, :cp] += jnp.sum(dy * x, axis=0, keepdims=True)
        dt_r = dt_t[0:8]
        wdec_r = wdec.T[0:8]
        w_r = wdec_r * dt_r
        rate_r = jnp.broadcast_to(rate, (128, 128)).T[0:8, 0:1]
        last_r = jnp.exp(cum_t[0:8, Q - 1 : Q])
        dcum = carr + onto - dtb.astype(f32) * direct - w_r * dw
        end = jnp.sum(w_r * dw, axis=1, keepdims=True) + last_r * dlast
        da = mm(dcum, tri((Q, Q)).astype(f32), precision=HI) + end
        ddt = direct + wdec_r * dw + rate_r * da
        draw = ddt * sigmoid(raw).T[0:8]
        R.hacc[0] += draw
        R.hacc[1] += da * dt_r * rate_r
        dact = jnp.concatenate([dx, db, dc], axis=1)
        dsum = dact * (sig * (1.0 + summed * (1.0 - sig)))
        full = jnp.concatenate([dsum, R.head[...]], axis=0)
        dxbc = jnp.zeros((Q, C), f32)
        for k in range(4):
            R.acc[k : k + 1, :C] += jnp.sum(dsum * taps[k], axis=0, keepdims=True)
            moved = pltpu.roll(full, Q + 8 - (3 - k), 0)[:Q] if k < 3 else dsum
            dxbc = dxbc + small[k : k + 1, :C] * moved
        R.acc[4:5, :C] += jnp.sum(dsum, axis=0, keepdims=True)
        R.head[...] = dsum[:8]
        R.dpx[rows, :C] = dxbc.astype(bf16)
        R.acc[8:16, :] += mm(draw.astype(bf16), R.hid_t[:, rows], 1, 1)
        pad = jnp.concatenate([draw, jnp.zeros((120, Q), f32)], axis=0).T
        R.dpx[rows, C:] = pad.astype(bf16)
        grad = jnp.concatenate([R.zb[rows, :], R.dpx[rows, :]], axis=1)
        hp = mm(grad, R.w_all[...].reshape(D, WC), 1, 1)
        r = R.tok_all[c].astype(f32)
        scale = lax.rsqrt(jnp.mean(r * r, axis=1, keepdims=True) + epsilon)
        R.acc[6:7, :] += jnp.sum(hp * r * scale, axis=0, keepdims=True)
        R.tok_all[c] = hp.astype(bf16)
        hid.across(c)
        return carry

    lax.fori_loop(0, nc, scan, 0)

    def lower(k, carry):
        to = lax.rem(pc.f + k, F)
        rows = pl.ds(pl.multiple_of(to * Dl, Dl), Dl)
        R.cp_[to] = mm(R.hid_t[rows, :], R.dpx[:, cp:C]).astype(bf16)

        @pl.when(k < F)
        def _():
            rcopy(
                R.cp_.at[to], R.cr_.at[k - 1], R.cs0.at[k - 1], R.cs1.at[k - 1], fsdp=to
            ).start()
        return carry

    lax.fori_loop(1, F + 1, lower, 0)

    def xpart(k, carry):
        to = lax.rem(pc.f + k, F)
        rows = pl.ds(pl.multiple_of(to * Dl, Dl), Dl)
        R.xp[to] = mm(R.hid_t[rows, :], R.dpx[:, :cp]).astype(bf16)

        @pl.when(k < F)
        def _():
            rcopy(
                R.xp.at[to], R.xr.at[k - 1], R.xs0.at[k - 1], R.xs1.at[k - 1], fsdp=to
            ).start()
        return carry

    lax.fori_loop(1, F + 1, xpart, 0)
    diag = lax.broadcasted_iota(jnp.int32, (8, 128), 0) == lax.broadcasted_iota(
        jnp.int32, (8, 128), 1
    )

    def along(v):
        return jnp.sum(jnp.where(diag, jnp.sum(v, axis=1, keepdims=True), 0.0), axis=0, keepdims=True)

    dskip = jnp.sum(
        jnp.where(diag, mm(sel, R.acc[7:8, :cp], 1, 1, HI), 0.0), axis=0, keepdims=True
    )
    R.acc[7:8, :] = jnp.concatenate(
        [along(R.hacc[0]), along(R.hacc[1]), dskip, jnp.zeros((1, D - 384), f32)], axis=1
    )
    for k in range(1, F):
        to = lax.rem(pc.f + k, F)
        rcopy(
            R.acc, R.ar.at[k - 1], R.as0.at[k - 1], R.as1.at[k - 1], fsdp=to
        ).start()

    low = bs.total()
    for g in range(S):
        R.cb[g] = low[g * bh : (g + 1) * bh].astype(bf16)
    for k in range(1, S):
        to = lax.rem(pc.s + k, S)
        direct(R.cb.at[to], R.cbr, R.cb0, R.cb1, to)

    def hid_column(i, carry):
        hid.column(pc.Z - 1 - i)
        return carry

    lax.fori_loop(0, pc.Z - 2, hid_column, 0)
    R.xred[...] = xs.total().astype(bf16)
    xg.start()
    own(R.xred, O.gx.at[pc.s], 2).start()
    lax.fori_loop(pc.Z - 2, pc.Z, hid_column, 0)
    total = R.acc[...]
    for k in range(1, F):
        r = R.ar.at[k - 1]
        rcopy(r, r, R.as0.at[k - 1], R.as1.at[k - 1], fsdp=pc.f).wait_recv()
        total = total + R.ar[k - 1]
    R.asum[...] = total.astype(bf16)
    sg.start()
    own(R.asum, O.sm.at[pc.s], 1).start()
    arrived(R.cbr, R.cb0, R.cb1)
    R.cbr[pc.s] = R.cb[pc.s]
    low = R.cbr[0].astype(f32)
    for g in range(1, S):
        low = low + R.cbr[g].astype(f32)
    R.cbd[...] = low.astype(bf16)
    for k in range(1, S):
        direct(R.cbd, O.gbc, R.cd0, R.cd1, lax.rem(pc.s + k, S))
    own(R.cbd, O.gbc.at[pc.s], 4).start()
    own(R.ored, O.go_s.at[pc.s], 5).wait()
    og.wait_across()
    for k in range(1, F):
        to = lax.rem(pc.f + k, F)
        rcopy(
            O.go_s.at[pl.ds(to * per, per)], O.go.at[pc.f], R.gs0.at[k], R.gs1.at[pc.f],
            fsdp=to,
        ).start()
    own(O.go_s.at[pl.ds(pc.f * per, per)], O.go.at[pc.f], 3).start()
    xg.relay(1)
    sg.relay(1)

    mine = tok[...].astype(f32)
    if tight(cfg):
        O.block[...] = (mine + blk.total()).astype(bf16)
    else:
        arrived(R.mall, R.ms0, R.ms1)
        R.mall[pc.s] = R.mn[pc.s]
        R.total[...] = mine

        def add(g, carry):
            w = R.w_out[lax.rem(g, per), g // per]
            R.total[...] += mm(R.mall[g], w)
            return carry

        lax.fori_loop(0, S, add, 0)
        O.block[...] = R.total[...].astype(bf16)
    xg.relay(2)
    sg.relay(2)
    scale = lax.rsqrt(jnp.mean(mine * mine, axis=1, keepdims=True) + epsilon)
    e = hid.total() * small[6:7, :]
    mean = jnp.mean(e * mine, axis=1, keepdims=True)
    O.input[...] = cot[...].astype(f32) + scale * e - scale * scale * scale * mine * mean
    xg.relay(3)
    sg.relay(3)

    zg.wait_across()
    for k in range(1, F):
        o = lax.rem(pc.f + k, F)
        r = O.go.at[o]
        rcopy(r, r, R.gs0.at[0], R.gs1.at[o], fsdp=pc.f).wait_recv()
    arrived(O.gbc, R.cd0, R.cd1)
    sg.wait_across()
    xg.wait_across()
    own(R.zred, O.gz.at[pc.s], 0).wait()
    own(R.asum, O.sm.at[pc.s], 1).wait()
    own(R.xred, O.gx.at[pc.s], 2).wait()
    own(O.go_s.at[pl.ds(pc.f * per, per)], O.go.at[pc.f], 3).wait()
    own(R.cbd, O.gbc.at[pc.s], 4).wait()
    if tight(cfg):
        blk.drain()
    else:
        sent(R.mn.at[0], R.ms0, R.ms1)
    sent(R.cb.at[0], R.cb0, R.cb1)
    sent(R.cbd, R.cd0, R.cd1)
    for a in (hid, zs, os_, xs, bs, zg, og, xg, sg):
        a.drain()
    for k in range(1, F):
        r = R.ar.at[k - 1]
        rcopy(r, r, R.as0.at[k - 1], R.as1.at[0], fsdp=pc.f).wait_send()
        r = O.go.at[0]
        rcopy(r, r, R.gs0.at[k], R.gs1.at[0], fsdp=pc.f).wait_send()


def bwd_scratch(cfg):
    S, F, T, D, cp, WC = cfg
    L = S * T
    Dl = D // F
    C = cp + 2 * N
    Z, X = 4, S // 4
    cr = cp // F
    bh = Dl // S
    V = pltpu.VMEM
    sem = pltpu.SemaphoreType.DMA
    seq = gather_sems(4, S // 4)
    out = SimpleNamespace(
        acc=V((16, D), f32),
        asum=V((16, D), bf16),
        ar=V((F - 1, 16, D), f32),
        hacc=V((2, 8, 128), f32),
        dstate=V((N, cp), f32),
        head=V((8, C), f32),
        mn_t=V((cp, L), bf16),
        dpx=V((L, WC - cp), bf16),
        hrx=V((Z, X - 1, T, D), bf16),
        hrz=V((Z - 1, T, D), bf16),
        zp=V((F, Dl, cp), bf16),
        zr=V((F - 1, Dl, cp), bf16),
        zred=V((Dl, cp), bf16),
        op=V((F, cr, D), bf16),
        orecv=V((F - 1, cr, D), bf16),
        ored=V((cr, D), bf16),
        xp=V((F, Dl, cp), bf16),
        xr=V((F - 1, Dl, cp), bf16),
        xred=V((Dl, cp), bf16),
        cp_=V((F, Dl, 2 * N), bf16),
        cr_=V((F - 1, Dl, 2 * N), bf16),
        cb=V((S, bh, 2 * N), bf16),
        cbr=V((S, bh, 2 * N), bf16),
        cbd=V((bh, 2 * N), bf16),
        lsem=sem((6,)),
        as0=sem((F,)), as1=sem((F,)), as2=seq[0], as3=seq[1],
        gs0=sem((F,)), gs1=sem((F,)), cs0=sem((F,)), cs1=sem((F,)),
        cb0=sem((S,)), cb1=sem((S,)), cd0=sem((S,)), cd1=sem((S,)),
        zs0=sem((F,)), zs1=sem((F,)), gz0=seq[0], gz1=seq[1],
        os0=sem((F,)), os1=sem((F,)), go0=seq[0], go1=seq[1],
        xs0=sem((F,)), xs1=sem((F,)), gx0=seq[0], gx1=seq[1],
        hs0=sem((S,)), hs1=sem((Z, X - 1)), hs2=sem((Z,)), hs3=sem((Z - 1,)),
    )
    if tight(cfg):
        out.brx = V((Z, X - 1, T, D), bf16)
        out.brz = V((Z - 1, T, D), bf16)
        out.bs0, out.bs1, out.bs2, out.bs3 = out.hs0, out.hs1, out.hs2, out.hs3
    else:
        out.mn = V((S, T, cp), bf16)
        out.mall = V((S, T, cp), bf16)
        out.total = V((T, D), f32)
        out.ms0 = out.ms1 = sem((S,))
    return out


def assemble(cfg, dims, gz, gx, gbc, go, sm, win, step, conv, bias, gate, norm, heads, wout):
    S, F, T, D, cp, WC = cfg
    inner, nheads, cols = dims
    for g in range(S):
        win[:, g * cols : (g + 1) * cols] = gz[g, :, :cols].astype(f32)
        win[:, inner + g * cols : inner + (g + 1) * cols] = gx[g, :, :cols].astype(f32)
    wout[...] = go[0, 0].astype(f32)
    C = cp + 2 * N
    hg = nheads // S
    Dl = D // F
    win[:, 2 * inner :] = gbc[...].astype(f32)

    @pl.when(pl.program_id(0) == 0)
    def _():
        f = lax.axis_index("fsdp")

        def mine(v, size):
            n = v.shape[1]
            return pltpu.roll(v, lax.rem(n - size * f, n), 1)[:, :size]

        v = [sm[g].astype(f32) for g in range(S)]
        total = v[0]
        for g in range(1, S):
            total = total + v[g]
        xs = jnp.concatenate([a[0:8, :cols] for a in v] + [total[0:8, cp:C]], axis=1)
        xs = mine(xs, (inner + 2 * N) // F)
        conv[...] = xs[0:4]
        bias[...] = xs[4:5]
        gate[...] = mine(jnp.concatenate([a[0:8, :cols] for a in v], axis=1), inner // F)[5:6]
        norm[...] = mine(total[0:8], Dl)[6:7]
        n = nheads // F
        zero = jnp.zeros((8, 128 - nheads), f32)
        for i in range(3):
            hs = [a[0:8, 128 * i : 128 * i + hg] for a in v]
            heads[i : i + 1, :] = mine(jnp.concatenate(hs + [zero], axis=1), n)[7:8]
        cols_t = [mine(a[8:16], Dl).T[:, :hg] for a in v]
        step[...] = jnp.concatenate(cols_t, axis=1)


def shards(tokens, in_weight, step_weight, conv_kernel, conv_bias, step_bias, log_decay,
           skip_gain, gate_gain, norm_gain, out_weight, cotangent):
    S = lax.axis_size("seq")
    F = lax.axis_size("fsdp")
    _, T, D = tokens.shape
    inner = out_weight.shape[0] * F
    heads = step_weight.shape[1]
    cols = inner // S
    cp = -(-cols // 128) * 128
    WC = 2 * cp + 2 * N + 128
    Dl = D // F
    cr = cp // F
    per = S // F
    bh = Dl // S
    cfg = (S, F, T, D, cp, WC)
    dims = (inner, heads, cols)
    s = lax.axis_index("seq")

    def padc(a, to):
        return jnp.pad(a, [(0, 0)] * (a.ndim - 1) + [(0, to - a.shape[-1])])

    def part(a, start, size, axis):
        return lax.dynamic_slice_in_dim(a, start, size, axis)

    step = padc(part(step_weight, s * (heads // S), heads // S, 1), 128)
    if cols % 128 == 0:
        wsrc = (in_weight, step)
    else:
        wsrc = (
            jnp.concatenate(
                [
                    padc(part(in_weight, s * cols, cols, 1), cp),
                    padc(part(in_weight, inner + s * cols, cols, 1), cp),
                    in_weight[:, 2 * inner :],
                    step,
                ],
                axis=1,
            ),
        )
    if tight(cfg):
        wo = jnp.pad(
            part(out_weight, lax.rem(s, per) * cols, cols, 0), [(0, cp - cols), (0, 0)]
        )
    else:
        wo = out_weight.reshape(per, cols, D)
    vectors = list(conv_kernel) + [
        conv_bias, gate_gain, norm_gain, step_bias, log_decay, skip_gain,
    ]
    flat = jnp.concatenate([padc(a, -(-a.shape[0] // 128) * 128) for a in vectors])[None]
    scratch = {**vars(fwd_scratch(cfg)), **vars(bwd_scratch(cfg))}
    names = list(scratch)
    outs = dict(
        block=jax.ShapeDtypeStruct((T, D), bf16),
        input=jax.ShapeDtypeStruct((T, D), f32),
        gz=jax.ShapeDtypeStruct((S, Dl, cp), bf16),
        gx=jax.ShapeDtypeStruct((S, Dl, cp), bf16),
        gbc=jax.ShapeDtypeStruct((S, bh, 2 * N), bf16),
        go=jax.ShapeDtypeStruct((F, per, cr, D), bf16),
        go_s=jax.ShapeDtypeStruct((S, cr, D), bf16),
        sm=jax.ShapeDtypeStruct((S, 16, D), bf16),
    )
    on = list(outs)
    nw = len(wsrc)

    def kern(tok, cot, wo, flat, *rest):
        O = SimpleNamespace(**dict(zip(on, rest[nw : nw + len(on)])))
        R = SimpleNamespace(**dict(zip(names, rest[nw + len(on) :])))
        if tight(cfg):
            R.bp = R.cot_all
        body_fwd(cfg, dims, tok, cot, rest[:nw], wo, flat, R)
        body_bwd(cfg, dims, tok, cot, R, O)

    v = pl.BlockSpec(memory_space=pltpu.VMEM)
    hbm = pl.BlockSpec(memory_space=pl.ANY)
    res = pl.pallas_call(
        kern,
        out_shape=[outs[n] for n in on],
        in_specs=[v, v, hbm, v] + [hbm] * nw,
        out_specs=[v, v] + [hbm] * (len(on) - 2),
        scratch_shapes=[scratch[n] for n in names],
        compiler_params=pltpu.CompilerParams(
            collective_id=0, has_side_effects=True, vmem_limit_bytes=VMEM_LIMIT
        ),
    )(tokens[0], cotangent[0], wo, flat, *wsrc)
    G = SimpleNamespace(**dict(zip(on, res)))
    pieces = cols // cr
    steps = per * pieces
    rows = Dl // steps
    cl, gl, hl = (inner + 2 * N) // F, inner // F, heads // F

    def whole(*shape):
        return pl.BlockSpec(shape, lambda i: (0,) * len(shape))

    def out(*shape):
        return jax.ShapeDtypeStruct(shape, f32)

    joined = pl.pallas_call(
        lambda *refs: assemble(cfg, dims, *refs),
        grid=(steps,),
        out_shape=[
            out(Dl, 2 * inner + 2 * N), out(Dl, heads), out(4, cl), out(1, cl), out(1, gl),
            out(1, Dl), out(3, hl), out(per * cols, D),
        ],
        in_specs=[
            pl.BlockSpec((S, rows, cp), lambda i: (0, i, 0)),
            pl.BlockSpec((S, rows, cp), lambda i: (0, i, 0)),
            pl.BlockSpec((rows, 2 * N), lambda i: (i, 0)),
            pl.BlockSpec((1, 1, cr, D), lambda i: (lax.rem(i, pieces), i // pieces, 0, 0)),
            whole(S, 16, D),
        ],
        out_specs=[
            pl.BlockSpec((rows, 2 * inner + 2 * N), lambda i: (i, 0)),
            whole(Dl, heads), whole(4, cl), whole(1, cl), whole(1, gl), whole(1, Dl),
            whole(3, hl),
            pl.BlockSpec((cr, D), lambda i: (i, 0)),
        ],
    )(G.gz, G.gx, G.gbc.reshape(Dl, 2 * N), G.go, G.sm)
    win, stepg, conv, bias, gate, norm, hd, wout = joined
    return (
        G.block[None],
        G.input[None],
        win,
        stepg,
        conv,
        bias[0],
        hd[0],
        hd[1],
        hd[2],
        gate[0],
        norm[0],
        wout,
    )


def solution(mesh):
    row = P("fsdp", None)
    tok = P("fsdp", "seq", None)
    one = P("fsdp")
    return jax.shard_map(
        shards,
        mesh=mesh,
        in_specs=(tok, row, row, P(None, "fsdp"), one, one, one, one, one, one, row, tok),
        out_specs=(tok, tok, row, row, P(None, "fsdp"), one, one, one, one, one, one, row),
        check_vma=False,
    )
```

```python
from types import SimpleNamespace

import jax
import jax.numpy as jnp
from jax import lax
from jax.experimental import pallas as pl
from jax.experimental.pallas import tpu as pltpu
from jax.sharding import PartitionSpec as P

N = 128
HEAD = 64
Q = 128
epsilon = 1e-05
bf16 = jnp.bfloat16
f32 = jnp.float32
MESH = pl.DeviceIdType.MESH
HI = lax.Precision.HIGHEST
VMEM_LIMIT = 64 * 1024 * 1024 - 65536


def mm(a, b, da=1, db=0, precision=None):
    return lax.dot_general(
        a, b, (((da,), (db,)), ((), ())), preferred_element_type=f32, precision=precision
    )


def rcopy(src, dst, ss, rs, **dev):
    return pltpu.make_async_remote_copy(
        src_ref=src, dst_ref=dst, send_sem=ss, recv_sem=rs, device_id=dev, device_id_type=MESH
    )


class Axis:
    def __init__(self, name, outer, inner):
        self.name, self.outer, self.inner = name, outer, inner
        self.me = lax.axis_index(name)
        self.o = self.me // inner
        self.i = lax.rem(self.me, inner)

    def near(self, k):
        half = self.outer // 2
        side = self.o // half
        m = self.o + side * (self.outer - 1 - 2 * self.o)
        at = jnp.where(k == 0, m, k - m * ((3 - k) // 2))
        return at + side * (self.outer - 1 - 2 * at)

    def blk(self, k, q):
        return self.near(k) * self.inner + lax.rem(self.i + q, self.inner)

    def to(self, d):
        return {self.name: d}


class Place:
    def __init__(self, S, F):
        self.S, self.F = S, F
        self.seq = Axis("seq", 4, S // 4)
        self.fsdp = Axis("fsdp", F // 2, 2)
        self.Z, self.X = 4, S // 4
        self.s, self.z, self.x = self.seq.me, self.seq.o, self.seq.i
        self.f = self.fsdp.me
        self.blk = self.seq.blk

    def barrier(self):
        bar = pltpu.get_barrier_semaphore()
        n = 0
        for k in range(1, self.S):
            pl.semaphore_signal(
                bar, inc=1, device_id={"seq": lax.rem(self.s + k, self.S)}, device_id_type=MESH
            )
            n += 1
        for k in range(1, self.F):
            pl.semaphore_signal(
                bar, inc=1, device_id={"fsdp": lax.rem(self.f + k, self.F)}, device_id_type=MESH
            )
            n += 1
        pl.semaphore_wait(bar, n)


class Gather:
    def __init__(self, ax, src, buf, sems):
        self.ax, self.src, self.buf = ax, src, buf
        self.ss, self.rs = sems

    def send(self, src, b, sem, dst):
        rcopy(src, self.buf.at[b], self.ss.at[sem], self.rs.at[b], **self.ax.to(dst)).start()

    def start(self):
        ax = self.ax
        for sem, d in ((0, 1), (1, -1)):

            @pl.when(jnp.logical_and(ax.o + d >= 0, ax.o + d < ax.outer))
            def _():
                self.send(self.src, ax.me, sem, ax.me + d * ax.inner)

        self.across(self.src, ax.me, 0)

    def across(self, src, b, k):
        ax = self.ax
        for q in range(1, ax.inner):
            sem = ax.outer + 1 + k * (ax.inner - 1) + q - 1
            self.send(src, b, sem, ax.o * ax.inner + lax.rem(ax.i + q, ax.inner))

    def onward(self, k):
        ax = self.ax
        return ax.o + jnp.where(ax.o > ax.near(k), 1, -1)

    def relay(self, k):
        ax = self.ax
        b = ax.blk(k, 0)
        self.wait(b)
        nxt = self.onward(k)

        @pl.when(jnp.logical_and(nxt >= 0, nxt < ax.outer))
        def _():
            self.send(self.buf.at[b], b, 1 + k, nxt * ax.inner + ax.i)

        self.across(self.buf.at[b], b, k)

    def wait(self, b):
        r = self.buf.at[b]
        rcopy(r, r, self.ss.at[0], self.rs.at[b], **self.ax.to(self.ax.me)).wait_recv()

    def wait_across(self):
        for k in range(self.ax.outer):
            for q in range(1, self.ax.inner):
                self.wait(self.ax.blk(k, q))

    def drain(self):
        ax = self.ax

        def done(sem):
            rcopy(
                self.src, self.src, self.ss.at[sem], self.rs.at[0], **ax.to(ax.me)
            ).wait_send()

        for sem, d in ((0, 1), (1, -1)):

            @pl.when(jnp.logical_and(ax.o + d >= 0, ax.o + d < ax.outer))
            def _():
                done(sem)

        for k in range(1, ax.outer):
            nxt = self.onward(k)

            @pl.when(jnp.logical_and(nxt >= 0, nxt < ax.outer))
            def _():
                done(1 + k)

        for sem in range(ax.outer * (ax.inner - 1)):
            done(ax.outer + 1 + sem)


def gather_sems(outer, inner):
    sem = pltpu.SemaphoreType.DMA
    return sem((outer + 1 + outer * (inner - 1),)), sem((outer * inner,))


def pair(col, p):
    lane = lax.broadcasted_iota(jnp.int32, (col.shape[0], 128), 1)
    return jnp.where(lane < HEAD, col[:, 2 * p : 2 * p + 1], col[:, 2 * p + 1 : 2 * p + 2])


def spread(col, cp):
    return jnp.concatenate([pair(col, p) for p in range(cp // 128)], axis=1)


def sigmoid(v):
    return 1.0 / (1.0 + jnp.exp(-v))


def softplus(v):
    return jnp.maximum(v, 0.0) + jnp.log1p(jnp.exp(-jnp.abs(v)))


def tri(shape, flip=False):
    i = lax.broadcasted_iota(jnp.int32, shape, 0)
    j = lax.broadcasted_iota(jnp.int32, shape, 1)
    return j >= i if flip else i >= j


def split(x2):
    lane = lax.broadcasted_iota(jnp.int32, x2.shape, 1)
    return jnp.concatenate([jnp.where(lane < HEAD, x2, 0), jnp.where(lane >= HEAD, x2, 0)], axis=0)


def chunk_inputs(c, ext, rawb, small, cp):
    r0 = pl.multiple_of(c * Q, Q)
    v = ext[pl.ds(r0, Q + 16), :].astype(f32)
    C = cp + 2 * N
    taps = [pltpu.roll(v, 3 - k, 0)[16:] if k < 3 else v[16:] for k in range(4)]
    summed = small[4:5, :C]
    for k in range(4):
        summed = summed + small[k : k + 1, :C] * taps[k]
    sig = sigmoid(summed)
    raw = rawb[pl.ds(r0, Q), :].astype(f32) + small[7:8, 0:128]
    dt = softplus(raw)
    rate = -jnp.exp(small[7:8, 128:256])
    cum = mm(tri((Q, Q)).astype(f32), dt * rate, precision=HI)
    return taps, summed, sig, raw, dt, rate, cum


def skip_row(small, cp):
    return spread(small[7:8, 256:384], cp)


def tight(cfg):
    S, F, T, D, cp, WC = cfg
    return S * T * D * 2 > 2**22


def lanes_from(row, shift, width, size):
    n = row.shape[1]
    if n < width:
        row = jnp.concatenate([row, jnp.zeros((row.shape[0], width - n), f32)], axis=1)
    row = pltpu.roll(row, lax.rem(shift + width, width), 1)
    return row[:, :size]


def small_rows(cfg, dims, flat, pc):
    S, F, T, D, cp, WC = cfg
    inner, heads, cols = dims
    conv = inner + 2 * N
    cl, gl, nl, hl = conv // F, inner // F, D // F, heads // F
    up = lambda n: -(-n // 128) * 128
    at = 0
    parts = []
    for n in [cl] * 5 + [gl, nl, hl, hl, hl]:
        parts.append(flat[:, at : at + up(n)])
        at += up(n)
    rows = jnp.concatenate(parts[:5] + [jnp.zeros((3, up(cl)), f32)], axis=0)
    lane = lax.broadcasted_iota(jnp.int32, (8, cp), 1)
    xs = lanes_from(rows, cl * pc.f - cols * pc.s, conv, cp)
    bc = lanes_from(rows, cl * pc.f - inner, conv, 2 * N)
    gate = lanes_from(parts[5], gl * pc.f - cols * pc.s, inner, cp)
    if cols < cp:
        xs = jnp.where(lane < cols, xs, 0.0)
        gate = jnp.where(lane[0:1] < cols, gate, 0.0)
    norm = lanes_from(parts[6], nl * pc.f, D, D)
    hg = heads // S
    hv = jnp.concatenate(parts[7:10] + [jnp.zeros((5, 128), f32)], axis=0)
    hv = lanes_from(hv, hl * pc.f - hg * pc.s, 128, 128)
    hv = jnp.where(lane[:, :128] < hg, hv, 0.0)

    def wide(v):
        return jnp.concatenate([v, jnp.zeros((v.shape[0], D - v.shape[1]), f32)], axis=1)

    return jnp.concatenate(
        [
            wide(jnp.concatenate([xs, bc], axis=1)[0:5]),
            wide(gate),
            norm,
            wide(jnp.concatenate([hv[0:1], hv[1:2], hv[2:3]], axis=1)),
        ],
        axis=0,
    )


def body_fwd(cfg, dims, tok, cot, wsrc, wo, flat, R):
    S, F, T, D, cp, WC = cfg
    inner, heads, cols = dims
    L = S * T
    C = cp + 2 * N
    per = S // F
    pc = Place(S, F)
    own = R.w_all.at[pc.f]
    if len(wsrc) == 1:
        parts = [(wsrc[0], own)]
    else:
        win, step = wsrc
        col = pl.multiple_of(pc.s * cols, cols)
        parts = [
            (win.at[:, pl.ds(col, cols)], own.at[:, pl.ds(0, cols)]),
            (win.at[:, pl.ds(inner + col, cols)], own.at[:, pl.ds(cols, cols)]),
            (win.at[:, pl.ds(2 * inner, 2 * N)], own.at[:, pl.ds(2 * cols, 2 * N)]),
            (step, own.at[:, pl.ds(2 * cols + 2 * N, 128)]),
        ]
    parts = [pltpu.make_async_copy(a, b, R.wsem.at[i]) for i, (a, b) in enumerate(parts)]
    for c in parts:
        c.start()
    R.sm_own[...] = small_rows(cfg, dims, flat[...].astype(f32), pc)
    pc.barrier()
    tg = Gather(pc.seq, tok, R.tok_all, (R.ss_t, R.rs_t))
    cg = Gather(pc.seq, cot, R.cot_all, (R.ss_c, R.rs_c))
    wg = Gather(pc.fsdp, own, R.w_all, (R.ss_w, R.rs_w))
    first = lax.rem(pc.s, per)
    owner = pc.s // per
    wogs = []
    if not tight(cfg):
        for p in range(per):
            at = lax.rem(first + p, per)
            wogs.append(
                Gather(pc.fsdp, wo.at[at], R.w_out.at[at], (R.ss_o.at[p], R.rs_o.at[p]))
            )
    sm = R.sm_own
    tg.start()
    for k in range(1, F):
        to = lax.rem(pc.f + k, F)
        rcopy(sm, R.sm_all.at[pc.f], R.ss_m.at[k], R.rs_m.at[pc.f], fsdp=to).start()
    for c in parts:
        c.wait()
    wg.start()
    keep = []
    for p in range(len(wogs)):
        wogs[p].start()
        at = lax.rem(first + p, per)
        keep.append(pltpu.make_async_copy(wo.at[at], R.w_out.at[at, pc.f], R.osem.at[p]))
    if tight(cfg):
        keep.append(pltpu.make_async_copy(wo, R.wo_g, R.osem.at[0]))

        @pl.when(pc.f == owner)
        def _():
            keep[0].start()
            for k in range(1, F):
                to = lax.rem(pc.f + k, F)
                rcopy(wo, R.wo_g, R.ss_o.at[k], R.rs_o.at[0], fsdp=to).start()
    else:
        for c in keep:
            c.start()
    R.tok_all[pc.s] = tok[...]
    R.cot_all[pc.s] = cot[...]
    R.sm_all[pc.f] = sm[...]
    R.ext[0:16, :] = jnp.zeros((16, C), bf16)
    for k in range(1, F):
        o = lax.rem(pc.f + k, F)
        rcopy(sm, R.sm_all.at[o], R.ss_m.at[0], R.rs_m.at[o], fsdp=pc.f).wait_recv()
    total = R.sm_all[0]
    for k in range(1, F):
        total = total + R.sm_all[k]
    R.small[...] = total
    small = R.small
    tg.relay(1)
    tg.relay(2)
    for k in range(1, F // 2):
        wg.relay(k)
    tg.relay(3)
    cg.start()
    wg.wait_across()

    def project(j, carry):
        k, q = j // pc.X, lax.rem(j, pc.X)
        b = pc.blk(k, q)

        @pl.when(q > 0)
        def _():
            tg.wait(b)

        @pl.when(j == S // 2)
        def _():
            cg.relay(1)

        r = R.tok_all[b].astype(f32)
        scale = lax.rsqrt(jnp.mean(r * r, axis=1, keepdims=True) + epsilon)
        h = r * scale * small[6:7, :]
        r0 = pl.multiple_of(b * T, T)
        R.hid_t[:, pl.ds(r0, T)] = h.T.astype(bf16)
        out = mm(h.astype(bf16), R.w_all[...].reshape(D, WC)).astype(bf16)
        R.zb[pl.ds(r0, T), :] = out[:, :cp]
        R.rawb[pl.ds(r0, T), :] = out[:, 2 * cp + 2 * N :]
        R.ext[pl.ds(r0 + 16, T), :] = out[:, cp : 2 * cp + 2 * N]
        return carry

    lax.fori_loop(0, S, project, 0)
    R.state[...] = jnp.zeros((N, cp), f32)
    ones = jnp.ones((8, cp), f32)

    def forward(c, carry):
        @pl.when(jnp.logical_or(c == 0, c == 5))
        def _():
            cg.relay(2 + c // 5)

        r0 = pl.multiple_of(c * Q, Q)
        taps, summed, sig, raw, dt, rate, cum = chunk_inputs(c, R.ext, R.rawb, small, cp)
        act = summed * sig
        x = act[:, :cp]
        bb = act[:, cp : cp + N].astype(bf16)
        cb = act[:, cp + N :].astype(bf16)
        cum_t = cum.T
        dt_t = dt.T
        scores = mm(cb, bb, 1, 1)
        causal = tri((Q, Q))
        parts = []
        for p in range(cp // 128):
            mix = []
            for h in (2 * p, 2 * p + 1):
                gap = jnp.where(causal, cum[:, h : h + 1] - cum_t[h : h + 1, :], -1e30)
                mix.append((jnp.exp(gap) * scores * dt_t[h : h + 1, :]).astype(bf16))
            parts.append(
                mm(jnp.concatenate(mix, axis=1), split(x[:, 128 * p : 128 * p + 128]).astype(bf16))
            )
        state = R.state[...]
        R.states[c] = state
        last = cum[Q - 1 : Q, :]
        y = jnp.concatenate(parts, axis=1) + mm(cb, state.astype(bf16)) * spread(jnp.exp(cum), cp)
        y = y + skip_row(small, cp) * x
        wx = (spread(jnp.exp(last - cum) * dt, cp) * x).astype(bf16)
        R.state[...] = spread(jnp.exp(last), cp) * state + mm(bb, wx, 0, 0)
        R.y[pl.ds(r0, Q), :] = y
        z = R.zb[pl.ds(r0, Q), :].astype(f32)
        gated = (y * (z * sigmoid(z))).astype(bf16)
        R.dpx[pl.ds(r0, Q), :cp] = gated
        g32 = gated.astype(f32)
        R.st[0:1, pl.ds(r0, Q)] = mm(ones, g32 * g32, 1, 1, HI)[0:1]
        return carry

    lax.fori_loop(0, L // Q, forward, 0)

    if tight(cfg):
        group = R.wo_g

        @pl.when(pc.f != owner)
        def _():
            rcopy(wo, R.wo_g, R.ss_o.at[0], R.rs_o.at[0], fsdp=pc.f).wait_recv()

        @pl.when(pc.f == owner)
        def _():
            keep[0].wait()
    else:
        group = R.w_out.at[first, owner]
        for c in keep:
            c.wait()
        for k in range(1, F // 2):
            wogs[0].relay(k)
        wogs[0].wait_across()

    def mixed(j, carry):
        k, q = j // pc.X, lax.rem(j, pc.X)
        b = pc.blk(k, q)

        @pl.when(q > 0)
        def _():
            cg.wait(b)

        r0 = pl.multiple_of(b * T, T)
        mg = mm(R.cot_all[b], group[...], 1, 1)
        R.mg[pl.ds(r0, T), :] = mg
        g = mg * small[5:6, :cp] * R.dpx[pl.ds(r0, T), :cp].astype(f32)
        R.st[1:2, pl.ds(r0, T)] = mm(ones, g, 1, 1, HI)[0:1]
        return carry

    lax.fori_loop(0, S, mixed, 0)
    for k in range(1, S):
        rcopy(
            R.st, R.st_all.at[pc.s], R.ss_s.at[k], R.rs_s.at[pc.s],
            seq=lax.rem(pc.s + k, S),
        ).start()
    R.st_all[pc.s] = R.st[...]
    for k in range(1, S):
        o = lax.rem(pc.s + k, S)
        rcopy(R.st, R.st_all.at[o], R.ss_s.at[0], R.rs_s.at[o], seq=pc.s).wait_recv()
    total = R.st_all[0]
    for k in range(1, S):
        total = total + R.st_all[k]
    R.stats[...] = total

    for g in [tg, cg, wg]:
        g.drain()
    for k in range(1, S):
        rcopy(R.st, R.st, R.ss_s.at[k], R.rs_s.at[0], seq=pc.s).wait_send()
    for k in range(1, F):
        rcopy(sm, sm, R.ss_m.at[k], R.rs_m.at[0], fsdp=pc.f).wait_send()
    if tight(cfg):

        @pl.when(pc.f == owner)
        def _():
            for k in range(1, F):
                rcopy(wo, wo, R.ss_o.at[k], R.rs_o.at[0], fsdp=pc.f).wait_send()

    return wogs


def fwd_scratch(cfg):
    S, F, T, D, cp, WC = cfg
    L = S * T
    Dl = D // F
    C = cp + 2 * N
    V = pltpu.VMEM
    sem = pltpu.SemaphoreType.DMA
    per = S // F
    seq = gather_sems(4, S // 4)
    fsdp = gather_sems(F // 2, 2)
    out = SimpleNamespace(
        tok_all=V((S, T, D), bf16),
        cot_all=V((S, T, D), bf16),
        w_all=V((F, Dl, WC), bf16),
        sm_own=V((8, D), f32),
        sm_all=V((F, 8, D), f32),
        small=V((8, D), f32),
        hid_t=V((D, L), bf16),
        zb=V((L, cp), bf16),
        rawb=V((L, 128), bf16),
        ext=V((16 + L, C), bf16),
        state=V((N, cp), f32),
        states=V((L // Q, N, cp), f32),
        y=V((L, cp), f32),
        mg=V((L, cp), f32),
        st=V((2, L), f32),
        st_all=V((S, 2, L), f32),
        stats=V((2, L), f32),
        ss_t=seq[0],
        rs_t=seq[1],
        ss_c=seq[0],
        rs_c=seq[1],
        ss_w=fsdp[0],
        rs_w=fsdp[1],
        ss_m=sem((F,)),
        rs_m=sem((F,)),
        wsem=sem((4,)),
        osem=sem((per,)),
        ss_s=sem((S,)),
        rs_s=sem((S,)),
    )
    if tight(cfg):
        out.wo_g = V((cp, D), bf16)
        out.ss_o = out.rs_o = sem((F,))
    else:
        out.w_out = V((per, F, cp, D), bf16)
        out.ss_o = sem((per,) + fsdp[0].shape)
        out.rs_o = sem((per,) + fsdp[1].shape)
    return out


class Scatter:
    def __init__(self, pc, part, rx, rz, sems):
        self.pc, self.part, self.rx, self.rz = pc, part, rx, rz
        self.ssx, self.rsx, self.ssz, self.rsz = sems

    def across(self, b):
        pc = self.pc
        zb, xb = b // pc.X, lax.rem(b, pc.X)

        @pl.when(xb != pc.x)
        def _():
            slot = lax.rem(pc.x - xb - 1 + pc.X, pc.X)
            rcopy(
                self.part.at[b], self.rx.at[zb, slot], self.ssx.at[b], self.rsx.at[zb, slot],
                seq=pc.z * pc.X + xb,
            ).start()

    def column(self, zb):
        pc = self.pc
        b = zb * pc.X + pc.x
        total = self.part[b].astype(f32)
        for q in range(pc.X - 1):
            r = self.rx.at[zb, q]
            rcopy(r, r, self.ssx.at[0], self.rsx.at[zb, q], seq=pc.s).wait_recv()
            total = total + self.rx[zb, q].astype(f32)
        self.part[b] = total.astype(bf16)

        @pl.when(zb != pc.z)
        def _():
            slot = lax.rem(pc.z - zb - 1 + pc.Z, pc.Z)
            rcopy(
                self.part.at[b], self.rz.at[slot], self.ssz.at[zb], self.rsz.at[slot], seq=b
            ).start()

    def total(self):
        pc = self.pc
        out = self.part[pc.s].astype(f32)
        for q in range(pc.Z - 1):
            r = self.rz.at[q]
            rcopy(r, r, self.ssz.at[0], self.rsz.at[q], seq=pc.s).wait_recv()
            out = out + self.rz[q].astype(f32)
        return out

    def drain(self):
        pc = self.pc
        r = self.rz.at[0]
        for b in range(pc.S):

            @pl.when(b % pc.X != pc.x)
            def _():
                rcopy(r, r, self.ssx.at[b], self.rsz.at[0], seq=pc.s).wait_send()

        for zb in range(pc.Z):

            @pl.when(zb != pc.z)
            def _():
                rcopy(r, r, self.ssz.at[zb], self.rsz.at[0], seq=pc.s).wait_send()


class Shared:
    def __init__(self, pc, part, recv, ss, rs):
        self.pc, self.part, self.recv, self.ss, self.rs = pc, part, recv, ss, rs

    def send(self, k):
        pc = self.pc
        to = lax.rem(pc.f + k, pc.F)
        rcopy(
            self.part.at[to], self.recv.at[k - 1], self.ss.at[k - 1], self.rs.at[k - 1], fsdp=to
        ).start()

    def total(self):
        pc = self.pc
        out = self.part[pc.f].astype(f32)
        for k in range(1, pc.F):
            r = self.recv.at[k - 1]
            rcopy(r, r, self.ss.at[k - 1], self.rs.at[k - 1], fsdp=pc.f).wait_recv()
            out = out + self.recv[k - 1].astype(f32)
        return out

    def drain(self):
        for k in range(1, self.pc.F):
            r = self.recv.at[k - 1]
            rcopy(r, r, self.ss.at[k - 1], self.rs.at[k - 1], fsdp=self.pc.f).wait_send()


def body_bwd(cfg, dims, tok, cot, wogs, R, O):
    S, F, T, D, cp, WC = cfg
    inner = float(dims[0])
    L = S * T
    C = cp + 2 * N
    Dl = D // F
    nc = L // Q
    cr = cp // F
    per = S // F
    bh = Dl // S
    pc = Place(S, F)
    small = R.small
    if tight(cfg):
        blk = Scatter(pc, R.bp, R.brx, R.brz, (R.bs0, R.bs1, R.bs2, R.bs3))
    hid = Scatter(pc, R.tok_all, R.hrx, R.hrz, (R.hs0, R.hs1, R.hs2, R.hs3))
    zs = Shared(pc, R.zp, R.zr, R.zs0, R.zs1)
    os_ = Shared(pc, R.op, R.orecv, R.os0, R.os1)
    xs = Shared(pc, R.xp, R.xr, R.xs0, R.xs1)
    bs = Shared(pc, R.cp_, R.cr_, R.cs0, R.cs1)
    zg = Gather(pc.seq, R.zred, O.gz, (R.gz0, R.gz1))
    og = Gather(pc.seq, R.ored, O.go_s, (R.go0, R.go1))
    xg = Gather(pc.seq, R.xred, O.gx, (R.gx0, R.gx1))
    sg = Gather(pc.seq, R.asum, O.sm, (R.as2, R.as3))

    def direct(src, dst, ss, rs, to):
        rcopy(src, dst.at[pc.s], ss.at[to], rs.at[pc.s], seq=to).start()

    def arrived(dst, ss, rs):
        for k in range(1, S):
            o = lax.rem(pc.s + k, S)
            r = dst.at[o]
            rcopy(r, r, ss.at[0], rs.at[o], seq=pc.s).wait_recv()

    def sent(src, ss, rs):
        for k in range(1, S):
            rcopy(src, src, ss.at[lax.rem(pc.s + k, S)], rs.at[0], seq=pc.s).wait_send()

    def own(src, dst, i):
        return pltpu.make_async_copy(src, dst, R.lsem.at[i])

    gate = small[5:6, :cp]
    R.acc[...] = jnp.zeros((16, D), f32)
    R.hacc[...] = jnp.zeros((2, 8, 128), f32)
    R.dstate[...] = jnp.zeros((N, cp), f32)
    R.head[...] = jnp.zeros((8, C), f32)

    def first(i, carry):
        c = lax.rem(pc.s + 1 + i, nc)
        r0 = pl.multiple_of(c * Q, Q)
        rows = pl.ds(r0, Q)
        st = jnp.concatenate([R.stats[:, rows], jnp.zeros((6, Q), f32)], axis=0).T
        scale = lax.rsqrt(st[:, 0:1] / inner + epsilon)
        mean = st[:, 1:2] / inner
        gated = R.dpx[rows, :cp].astype(f32)
        mg = R.mg[rows, :]
        ng = gated * scale
        mn = ng * gate
        R.acc[5:6, :cp] += jnp.sum(mg * ng, axis=0, keepdims=True)
        gg = (scale * (mg * gate) - scale * scale * scale * gated * mean).astype(bf16).astype(f32)
        z = R.zb[rows, :].astype(f32)
        sz = sigmoid(z)
        R.zb[rows, :] = (gg * R.y[rows, :] * (sz * (1.0 + z * (1.0 - sz)))).astype(bf16)
        R.mg[rows, :] = gg * (z * sz)
        R.mn_t[:, rows] = mn.T.astype(bf16)
        if tight(cfg):
            R.dpx[rows, :cp] = mn.astype(bf16)
        else:
            R.mn[c] = mn.astype(bf16)

            @pl.when(c != pc.s)
            def _():
                direct(R.mn.at[c], R.mall, R.ms0, R.ms1, c)

        return carry

    def block(i, carry):
        c = nc - 1 - i
        rows = pl.ds(pl.multiple_of(c * Q, Q), Q)
        R.bp[c] = mm(R.dpx[rows, :cp], R.wo_g[...]).astype(bf16)
        blk.across(c)
        return carry

    lax.fori_loop(0, nc, first, 0)

    def zpart(k, carry):
        to = lax.rem(pc.f + k, F)
        rows = pl.ds(pl.multiple_of(to * Dl, Dl), Dl)
        R.zp[to] = mm(R.hid_t[rows, :], R.zb[...]).astype(bf16)

        @pl.when(k < F)
        def _():
            rcopy(
                R.zp.at[to], R.zr.at[k - 1], R.zs0.at[k - 1], R.zs1.at[k - 1], fsdp=to
            ).start()
        return carry

    lax.fori_loop(1, F + 1, zpart, 0)
    W = 384

    def opart(j, carry):
        cols = pl.ds(pl.multiple_of(j * W, W), W)
        a = R.cot_all[:, :, cols].reshape(L, W)
        R.op[:, :, cols] = mm(R.mn_t[...], a).reshape(F, cr, W).astype(bf16)
        return carry

    lax.fori_loop(0, D // W, opart, 0)
    for g in wogs[1:]:
        for k in range(1, F // 2):
            g.relay(k)
    for k in range(1, F):
        os_.send(k)
    if tight(cfg):
        lax.fori_loop(0, nc, block, 0)

    sel = (
        lax.broadcasted_iota(jnp.int32, (8, cp), 1) // HEAD
        == lax.broadcasted_iota(jnp.int32, (8, cp), 0)
    ).astype(f32)
    sub = lax.broadcasted_iota(jnp.int32, (8, Q), 0)

    def scan(i, carry):
        c = nc - 1 - i
        r0 = pl.multiple_of(c * Q, Q)
        rows = pl.ds(r0, Q)

        if tight(cfg):

            @pl.when(i < pc.Z)
            def _():
                blk.column(pc.Z - 1 - i)

        @pl.when(i == 1)
        def _():
            R.zred[...] = zs.total().astype(bf16)
            zg.start()
            own(R.zred, O.gz.at[pc.s], 0).start()

        @pl.when(i == 2)
        def _():
            R.ored[...] = os_.total().astype(bf16)
            og.start()
            own(R.ored, O.go_s.at[pc.s], 5).start()

        @pl.when(jnp.logical_and(i >= 3, i < 3 + pc.Z - 1))
        def _():
            zg.relay(i - 2)

        @pl.when(jnp.logical_and(i >= 4, i < 4 + pc.Z - 1))
        def _():
            og.relay(i - 3)

        taps, summed, sig, raw, dt, rate, cum = chunk_inputs(c, R.ext, R.rawb, small, cp)
        act = summed * sig
        x = act[:, :cp]
        xb = x.astype(bf16)
        bb = act[:, cp : cp + N].astype(bf16)
        cb = act[:, cp + N :].astype(bf16)
        cum_t = cum.T
        dt_t = dt.T
        dy = R.mg[rows, :]
        dyb = dy.astype(bf16)
        last = cum[Q - 1 : Q, :]
        edy = spread(jnp.exp(cum), cp) * dy
        edyb = edy.astype(bf16)
        wdec = jnp.exp(last - cum)
        w = wdec * dt
        state = R.states[c]
        sb = state.astype(bf16)
        ds = R.dstate[...]
        dsb = ds.astype(bf16)
        ws = spread(w, cp)
        v = mm(bb, dsb)
        carr = mm(sel, edy * mm(cb, sb), 1, 1, HI)
        dw = mm(sel, x * v, 1, 1, HI)
        db = mm((ws * x).astype(bf16), dsb, 1, 1)
        dc = mm(edyb, sb, 1, 1)
        dlast = mm(sel, jnp.sum(state * ds, axis=0, keepdims=True), 1, 1, HI)
        R.dstate[...] = spread(jnp.exp(last), cp) * ds + mm(cb, edyb, 0, 0)
        scores = mm(bb, cb, 1, 1)
        seen = tri((Q, Q), True)
        dtb = dt_t[0:8].astype(bf16)
        dsc = jnp.zeros((Q, Q), f32)
        direct = jnp.zeros((8, Q), f32)
        onto = jnp.zeros((8, Q), f32)
        parts = []
        for p in range(cp // 128):
            cols = slice(128 * p, 128 * p + 128)
            g2 = mm(split(x[:, cols]).astype(bf16), dyb[:, cols], 1, 1)
            mix = []
            for h in (2 * p, 2 * p + 1):
                g = g2[:Q] if h % 2 == 0 else g2[Q:]
                decay = jnp.exp(jnp.where(seen, cum_t[h : h + 1, :] - cum[:, h : h + 1], -1e30))
                ls = decay * scores
                mix.append((ls * dt[:, h : h + 1]).astype(bf16))
                e = (g * ls).astype(bf16)
                dsc = dsc + g * decay * dt[:, h : h + 1]
                direct = direct + mm(jnp.where(sub == h, 1.0, 0.0).astype(bf16), e, 1, 1)
                onto = onto + mm(jnp.where(sub == h, dtb.astype(f32), 0.0).astype(bf16), e)
            parts.append(mm(jnp.concatenate(mix, axis=1), split(dy[:, cols]).astype(bf16)))
        dscb = dsc.astype(bf16)
        db = db + mm(dscb, cb)
        dc = dc + mm(dscb, bb, 0, 0)
        dx = skip_row(small, cp) * dy + ws * v + jnp.concatenate(parts, axis=1)
        R.acc[7:8, :cp] += jnp.sum(dy * x, axis=0, keepdims=True)
        dt_r = dt_t[0:8]
        wdec_r = wdec.T[0:8]
        w_r = wdec_r * dt_r
        rate_r = jnp.broadcast_to(rate, (128, 128)).T[0:8, 0:1]
        last_r = jnp.exp(cum_t[0:8, Q - 1 : Q])
        dcum = carr + onto - dtb.astype(f32) * direct - w_r * dw
        end = jnp.sum(w_r * dw, axis=1, keepdims=True) + last_r * dlast
        da = mm(dcum, tri((Q, Q)).astype(f32), precision=HI) + end
        ddt = direct + wdec_r * dw + rate_r * da
        draw = ddt * sigmoid(raw).T[0:8]
        R.hacc[0] += draw
        R.hacc[1] += da * dt_r * rate_r
        dact = jnp.concatenate([dx, db, dc], axis=1)
        dsum = dact * (sig * (1.0 + summed * (1.0 - sig)))
        full = jnp.concatenate([dsum, R.head[...]], axis=0)
        dxbc = jnp.zeros((Q, C), f32)
        for k in range(4):
            R.acc[k : k + 1, :C] += jnp.sum(dsum * taps[k], axis=0, keepdims=True)
            moved = pltpu.roll(full, Q + 8 - (3 - k), 0)[:Q] if k < 3 else dsum
            dxbc = dxbc + small[k : k + 1, :C] * moved
        R.acc[4:5, :C] += jnp.sum(dsum, axis=0, keepdims=True)
        R.head[...] = dsum[:8]
        R.dpx[rows, :C] = dxbc.astype(bf16)
        R.acc[8:16, :] += mm(draw.astype(bf16), R.hid_t[:, rows], 1, 1)
        pad = jnp.concatenate([draw, jnp.zeros((120, Q), f32)], axis=0).T
        R.dpx[rows, C:] = pad.astype(bf16)
        grad = jnp.concatenate([R.zb[rows, :], R.dpx[rows, :]], axis=1)
        hp = mm(grad, R.w_all[...].reshape(D, WC), 1, 1)
        r = R.tok_all[c].astype(f32)
        scale = lax.rsqrt(jnp.mean(r * r, axis=1, keepdims=True) + epsilon)
        R.acc[6:7, :] += jnp.sum(hp * r * scale, axis=0, keepdims=True)
        R.tok_all[c] = hp.astype(bf16)
        hid.across(c)
        return carry

    lax.fori_loop(0, nc, scan, 0)

    def lower(k, carry):
        to = lax.rem(pc.f + k, F)
        rows = pl.ds(pl.multiple_of(to * Dl, Dl), Dl)
        R.cp_[to] = mm(R.hid_t[rows, :], R.dpx[:, cp:C]).astype(bf16)

        @pl.when(k < F)
        def _():
            rcopy(
                R.cp_.at[to], R.cr_.at[k - 1], R.cs0.at[k - 1], R.cs1.at[k - 1], fsdp=to
            ).start()
        return carry

    lax.fori_loop(1, F + 1, lower, 0)

    def xpart(k, carry):
        to = lax.rem(pc.f + k, F)
        rows = pl.ds(pl.multiple_of(to * Dl, Dl), Dl)
        R.xp[to] = mm(R.hid_t[rows, :], R.dpx[:, :cp]).astype(bf16)

        @pl.when(k < F)
        def _():
            rcopy(
                R.xp.at[to], R.xr.at[k - 1], R.xs0.at[k - 1], R.xs1.at[k - 1], fsdp=to
            ).start()
        return carry

    lax.fori_loop(1, F + 1, xpart, 0)
    diag = lax.broadcasted_iota(jnp.int32, (8, 128), 0) == lax.broadcasted_iota(
        jnp.int32, (8, 128), 1
    )

    def along(v):
        return jnp.sum(jnp.where(diag, jnp.sum(v, axis=1, keepdims=True), 0.0), axis=0, keepdims=True)

    dskip = jnp.sum(
        jnp.where(diag, mm(sel, R.acc[7:8, :cp], 1, 1, HI), 0.0), axis=0, keepdims=True
    )
    R.acc[7:8, :] = jnp.concatenate(
        [along(R.hacc[0]), along(R.hacc[1]), dskip, jnp.zeros((1, D - 384), f32)], axis=1
    )
    for k in range(1, F):
        to = lax.rem(pc.f + k, F)
        rcopy(
            R.acc, R.ar.at[k - 1], R.as0.at[k - 1], R.as1.at[k - 1], fsdp=to
        ).start()

    low = bs.total()
    for g in range(S):
        R.cb[g] = low[g * bh : (g + 1) * bh].astype(bf16)
    for k in range(1, S):
        to = lax.rem(pc.s + k, S)
        direct(R.cb.at[to], R.cbr, R.cb0, R.cb1, to)

    def hid_column(i, carry):
        hid.column(pc.Z - 1 - i)
        return carry

    lax.fori_loop(0, pc.Z - 2, hid_column, 0)
    R.xred[...] = xs.total().astype(bf16)
    xg.start()
    own(R.xred, O.gx.at[pc.s], 2).start()
    lax.fori_loop(pc.Z - 2, pc.Z, hid_column, 0)
    total = R.acc[...]
    for k in range(1, F):
        r = R.ar.at[k - 1]
        rcopy(r, r, R.as0.at[k - 1], R.as1.at[k - 1], fsdp=pc.f).wait_recv()
        total = total + R.ar[k - 1]
    R.asum[...] = total.astype(bf16)
    sg.start()
    own(R.asum, O.sm.at[pc.s], 1).start()
    arrived(R.cbr, R.cb0, R.cb1)
    R.cbr[pc.s] = R.cb[pc.s]
    low = R.cbr[0].astype(f32)
    for g in range(1, S):
        low = low + R.cbr[g].astype(f32)
    R.cbd[...] = low.astype(bf16)
    for k in range(1, S):
        direct(R.cbd, O.gbc, R.cd0, R.cd1, lax.rem(pc.s + k, S))
    own(R.cbd, O.gbc.at[pc.s], 4).start()
    own(R.ored, O.go_s.at[pc.s], 5).wait()
    og.wait_across()
    for k in range(1, F):
        to = lax.rem(pc.f + k, F)
        rcopy(
            O.go_s.at[pl.ds(to * per, per)], O.go.at[pc.f], R.gs0.at[k], R.gs1.at[pc.f],
            fsdp=to,
        ).start()
    own(O.go_s.at[pl.ds(pc.f * per, per)], O.go.at[pc.f], 3).start()
    xg.relay(1)
    sg.relay(1)

    mine = tok[...].astype(f32)
    if tight(cfg):
        O.block[...] = (mine + blk.total()).astype(bf16)
    else:
        for g in wogs[1:]:
            g.wait_across()
        arrived(R.mall, R.ms0, R.ms1)
        R.mall[pc.s] = R.mn[pc.s]
        R.total[...] = mine

        def add(g, carry):
            w = R.w_out[lax.rem(g, per), g // per]
            R.total[...] += mm(R.mall[g], w)
            return carry

        lax.fori_loop(0, S, add, 0)
        O.block[...] = R.total[...].astype(bf16)
    xg.relay(2)
    sg.relay(2)
    scale = lax.rsqrt(jnp.mean(mine * mine, axis=1, keepdims=True) + epsilon)
    e = hid.total() * small[6:7, :]
    mean = jnp.mean(e * mine, axis=1, keepdims=True)
    O.input[...] = cot[...].astype(f32) + scale * e - scale * scale * scale * mine * mean
    xg.relay(3)
    sg.relay(3)

    zg.wait_across()
    for k in range(1, F):
        o = lax.rem(pc.f + k, F)
        r = O.go.at[o]
        rcopy(r, r, R.gs0.at[0], R.gs1.at[o], fsdp=pc.f).wait_recv()
    arrived(O.gbc, R.cd0, R.cd1)
    sg.wait_across()
    xg.wait_across()
    own(R.zred, O.gz.at[pc.s], 0).wait()
    own(R.asum, O.sm.at[pc.s], 1).wait()
    own(R.xred, O.gx.at[pc.s], 2).wait()
    own(O.go_s.at[pl.ds(pc.f * per, per)], O.go.at[pc.f], 3).wait()
    own(R.cbd, O.gbc.at[pc.s], 4).wait()
    if tight(cfg):
        blk.drain()
    else:
        sent(R.mn.at[0], R.ms0, R.ms1)
    sent(R.cb.at[0], R.cb0, R.cb1)
    sent(R.cbd, R.cd0, R.cd1)
    for a in [hid, zs, os_, xs, bs, zg, og, xg, sg] + wogs:
        a.drain()
    for k in range(1, F):
        r = R.ar.at[k - 1]
        rcopy(r, r, R.as0.at[k - 1], R.as1.at[0], fsdp=pc.f).wait_send()
        r = O.go.at[0]
        rcopy(r, r, R.gs0.at[k], R.gs1.at[0], fsdp=pc.f).wait_send()


def bwd_scratch(cfg):
    S, F, T, D, cp, WC = cfg
    L = S * T
    Dl = D // F
    C = cp + 2 * N
    Z, X = 4, S // 4
    cr = cp // F
    bh = Dl // S
    V = pltpu.VMEM
    sem = pltpu.SemaphoreType.DMA
    seq = gather_sems(4, S // 4)
    out = SimpleNamespace(
        acc=V((16, D), f32),
        asum=V((16, D), bf16),
        ar=V((F - 1, 16, D), f32),
        hacc=V((2, 8, 128), f32),
        dstate=V((N, cp), f32),
        head=V((8, C), f32),
        mn_t=V((cp, L), bf16),
        dpx=V((L, WC - cp), bf16),
        hrx=V((Z, X - 1, T, D), bf16),
        hrz=V((Z - 1, T, D), bf16),
        zp=V((F, Dl, cp), bf16),
        zr=V((F - 1, Dl, cp), bf16),
        zred=V((Dl, cp), bf16),
        op=V((F, cr, D), bf16),
        orecv=V((F - 1, cr, D), bf16),
        ored=V((cr, D), bf16),
        xp=V((F, Dl, cp), bf16),
        xr=V((F - 1, Dl, cp), bf16),
        xred=V((Dl, cp), bf16),
        cp_=V((F, Dl, 2 * N), bf16),
        cr_=V((F - 1, Dl, 2 * N), bf16),
        cb=V((S, bh, 2 * N), bf16),
        cbr=V((S, bh, 2 * N), bf16),
        cbd=V((bh, 2 * N), bf16),
        lsem=sem((6,)),
        as0=sem((F,)), as1=sem((F,)), as2=seq[0], as3=seq[1],
        gs0=sem((F,)), gs1=sem((F,)), cs0=sem((F,)), cs1=sem((F,)),
        cb0=sem((S,)), cb1=sem((S,)), cd0=sem((S,)), cd1=sem((S,)),
        zs0=sem((F,)), zs1=sem((F,)), gz0=seq[0], gz1=seq[1],
        os0=sem((F,)), os1=sem((F,)), go0=seq[0], go1=seq[1],
        xs0=sem((F,)), xs1=sem((F,)), gx0=seq[0], gx1=seq[1],
        hs0=sem((S,)), hs1=sem((Z, X - 1)), hs2=sem((Z,)), hs3=sem((Z - 1,)),
    )
    if tight(cfg):
        out.brx = V((Z, X - 1, T, D), bf16)
        out.brz = V((Z - 1, T, D), bf16)
        out.bs0, out.bs1, out.bs2, out.bs3 = out.hs0, out.hs1, out.hs2, out.hs3
    else:
        out.mn = V((S, T, cp), bf16)
        out.mall = V((S, T, cp), bf16)
        out.total = V((T, D), f32)
        out.ms0 = out.ms1 = sem((S,))
    return out


def assemble(cfg, dims, gz, gx, gbc, go, sm, win, step, conv, bias, gate, norm, heads, wout):
    S, F, T, D, cp, WC = cfg
    inner, nheads, cols = dims
    for g in range(S):
        win[:, g * cols : (g + 1) * cols] = gz[g, :, :cols].astype(f32)
        win[:, inner + g * cols : inner + (g + 1) * cols] = gx[g, :, :cols].astype(f32)
    wout[...] = go[0, 0].astype(f32)
    C = cp + 2 * N
    hg = nheads // S
    Dl = D // F
    win[:, 2 * inner :] = gbc[...].astype(f32)

    @pl.when(pl.program_id(0) == 0)
    def _():
        f = lax.axis_index("fsdp")

        def mine(v, size):
            n = v.shape[1]
            return pltpu.roll(v, lax.rem(n - size * f, n), 1)[:, :size]

        v = [sm[g].astype(f32) for g in range(S)]
        total = v[0]
        for g in range(1, S):
            total = total + v[g]
        xs = jnp.concatenate([a[0:8, :cols] for a in v] + [total[0:8, cp:C]], axis=1)
        xs = mine(xs, (inner + 2 * N) // F)
        conv[...] = xs[0:4]
        bias[...] = xs[4:5]
        gate[...] = mine(jnp.concatenate([a[0:8, :cols] for a in v], axis=1), inner // F)[5:6]
        norm[...] = mine(total[0:8], Dl)[6:7]
        n = nheads // F
        zero = jnp.zeros((8, 128 - nheads), f32)
        for i in range(3):
            hs = [a[0:8, 128 * i : 128 * i + hg] for a in v]
            heads[i : i + 1, :] = mine(jnp.concatenate(hs + [zero], axis=1), n)[7:8]
        cols_t = [mine(a[8:16], Dl).T[:, :hg] for a in v]
        step[...] = jnp.concatenate(cols_t, axis=1)


def shards(tokens, in_weight, step_weight, conv_kernel, conv_bias, step_bias, log_decay,
           skip_gain, gate_gain, norm_gain, out_weight, cotangent):
    S = lax.axis_size("seq")
    F = lax.axis_size("fsdp")
    _, T, D = tokens.shape
    inner = out_weight.shape[0] * F
    heads = step_weight.shape[1]
    cols = inner // S
    cp = -(-cols // 128) * 128
    WC = 2 * cp + 2 * N + 128
    Dl = D // F
    cr = cp // F
    per = S // F
    bh = Dl // S
    cfg = (S, F, T, D, cp, WC)
    dims = (inner, heads, cols)
    s = lax.axis_index("seq")

    def padc(a, to):
        return jnp.pad(a, [(0, 0)] * (a.ndim - 1) + [(0, to - a.shape[-1])])

    def part(a, start, size, axis):
        return lax.dynamic_slice_in_dim(a, start, size, axis)

    step = padc(part(step_weight, s * (heads // S), heads // S, 1), 128)
    if cols % 128 == 0:
        wsrc = (in_weight, step)
    else:
        wsrc = (
            jnp.concatenate(
                [
                    padc(part(in_weight, s * cols, cols, 1), cp),
                    padc(part(in_weight, inner + s * cols, cols, 1), cp),
                    in_weight[:, 2 * inner :],
                    step,
                ],
                axis=1,
            ),
        )
    if tight(cfg):
        wo = jnp.pad(
            part(out_weight, lax.rem(s, per) * cols, cols, 0), [(0, cp - cols), (0, 0)]
        )
    else:
        wo = out_weight.reshape(per, cols, D)
    vectors = list(conv_kernel) + [
        conv_bias, gate_gain, norm_gain, step_bias, log_decay, skip_gain,
    ]
    flat = jnp.concatenate([padc(a, -(-a.shape[0] // 128) * 128) for a in vectors])[None]
    scratch = {**vars(fwd_scratch(cfg)), **vars(bwd_scratch(cfg))}
    names = list(scratch)
    outs = dict(
        block=jax.ShapeDtypeStruct((T, D), bf16),
        input=jax.ShapeDtypeStruct((T, D), f32),
        gz=jax.ShapeDtypeStruct((S, Dl, cp), bf16),
        gx=jax.ShapeDtypeStruct((S, Dl, cp), bf16),
        gbc=jax.ShapeDtypeStruct((S, bh, 2 * N), bf16),
        go=jax.ShapeDtypeStruct((F, per, cr, D), bf16),
        go_s=jax.ShapeDtypeStruct((S, cr, D), bf16),
        sm=jax.ShapeDtypeStruct((S, 16, D), bf16),
    )
    on = list(outs)
    nw = len(wsrc)

    def kern(tok, cot, wo, flat, *rest):
        O = SimpleNamespace(**dict(zip(on, rest[nw : nw + len(on)])))
        R = SimpleNamespace(**dict(zip(names, rest[nw + len(on) :])))
        if tight(cfg):
            R.bp = R.cot_all
        wogs = body_fwd(cfg, dims, tok, cot, rest[:nw], wo, flat, R)
        body_bwd(cfg, dims, tok, cot, wogs, R, O)

    v = pl.BlockSpec(memory_space=pltpu.VMEM)
    hbm = pl.BlockSpec(memory_space=pl.ANY)
    res = pl.pallas_call(
        kern,
        out_shape=[outs[n] for n in on],
        in_specs=[v, v, hbm, v] + [hbm] * nw,
        out_specs=[v, v] + [hbm] * (len(on) - 2),
        scratch_shapes=[scratch[n] for n in names],
        compiler_params=pltpu.CompilerParams(
            collective_id=0, has_side_effects=True, vmem_limit_bytes=VMEM_LIMIT
        ),
    )(tokens[0], cotangent[0], wo, flat, *wsrc)
    G = SimpleNamespace(**dict(zip(on, res)))
    pieces = cols // cr
    steps = per * pieces
    rows = Dl // steps
    cl, gl, hl = (inner + 2 * N) // F, inner // F, heads // F

    def whole(*shape):
        return pl.BlockSpec(shape, lambda i: (0,) * len(shape))

    def out(*shape):
        return jax.ShapeDtypeStruct(shape, f32)

    joined = pl.pallas_call(
        lambda *refs: assemble(cfg, dims, *refs),
        grid=(steps,),
        out_shape=[
            out(Dl, 2 * inner + 2 * N), out(Dl, heads), out(4, cl), out(1, cl), out(1, gl),
            out(1, Dl), out(3, hl), out(per * cols, D),
        ],
        in_specs=[
            pl.BlockSpec((S, rows, cp), lambda i: (0, i, 0)),
            pl.BlockSpec((S, rows, cp), lambda i: (0, i, 0)),
            pl.BlockSpec((rows, 2 * N), lambda i: (i, 0)),
            pl.BlockSpec((1, 1, cr, D), lambda i: (lax.rem(i, pieces), i // pieces, 0, 0)),
            whole(S, 16, D),
        ],
        out_specs=[
            pl.BlockSpec((rows, 2 * inner + 2 * N), lambda i: (i, 0)),
            whole(Dl, heads), whole(4, cl), whole(1, cl), whole(1, gl), whole(1, Dl),
            whole(3, hl),
            pl.BlockSpec((cr, D), lambda i: (i, 0)),
        ],
    )(G.gz, G.gx, G.gbc.reshape(Dl, 2 * N), G.go, G.sm)
    win, stepg, conv, bias, gate, norm, hd, wout = joined
    return (
        G.block[None],
        G.input[None],
        win,
        stepg,
        conv,
        bias[0],
        hd[0],
        hd[1],
        hd[2],
        gate[0],
        norm[0],
        wout,
    )


def solution(mesh):
    row = P("fsdp", None)
    tok = P("fsdp", "seq", None)
    one = P("fsdp")
    return jax.shard_map(
        shards,
        mesh=mesh,
        in_specs=(tok, row, row, P(None, "fsdp"), one, one, one, one, one, one, row, tok),
        out_specs=(tok, tok, row, row, P(None, "fsdp"), one, one, one, one, one, one, row),
        check_vma=False,
    )
```

```python
from types import SimpleNamespace

import jax
import jax.numpy as jnp
from jax import lax
from jax.experimental import pallas as pl
from jax.experimental.pallas import tpu as pltpu
from jax.sharding import PartitionSpec as P

N = 128
HEAD = 64
Q = 128
epsilon = 1e-05
bf16 = jnp.bfloat16
f32 = jnp.float32
MESH = pl.DeviceIdType.MESH
HI = lax.Precision.HIGHEST
VMEM_LIMIT = 64 * 1024 * 1024 - 65536


def mm(a, b, da=1, db=0, precision=None):
    return lax.dot_general(
        a, b, (((da,), (db,)), ((), ())), preferred_element_type=f32, precision=precision
    )


def rcopy(src, dst, ss, rs, **dev):
    return pltpu.make_async_remote_copy(
        src_ref=src, dst_ref=dst, send_sem=ss, recv_sem=rs, device_id=dev, device_id_type=MESH
    )


class Axis:
    def __init__(self, name, outer, inner):
        self.name, self.outer, self.inner = name, outer, inner
        self.me = lax.axis_index(name)
        self.o = self.me // inner
        self.i = lax.rem(self.me, inner)

    def near(self, k):
        half = self.outer // 2
        side = self.o // half
        m = self.o + side * (self.outer - 1 - 2 * self.o)
        at = jnp.where(k == 0, m, k - m * ((3 - k) // 2))
        return at + side * (self.outer - 1 - 2 * at)

    def blk(self, k, q):
        return self.near(k) * self.inner + lax.rem(self.i + q, self.inner)

    def to(self, d):
        return {self.name: d}


class Place:
    def __init__(self, S, F):
        self.S, self.F = S, F
        self.seq = Axis("seq", 4, S // 4)
        self.fsdp = Axis("fsdp", F // 2, 2)
        self.Z, self.X = 4, S // 4
        self.s, self.z, self.x = self.seq.me, self.seq.o, self.seq.i
        self.f = self.fsdp.me
        self.blk = self.seq.blk

    def barrier(self):
        bar = pltpu.get_barrier_semaphore()
        n = 0
        for k in range(1, self.S):
            pl.semaphore_signal(
                bar, inc=1, device_id={"seq": lax.rem(self.s + k, self.S)}, device_id_type=MESH
            )
            n += 1
        for k in range(1, self.F):
            pl.semaphore_signal(
                bar, inc=1, device_id={"fsdp": lax.rem(self.f + k, self.F)}, device_id_type=MESH
            )
            n += 1
        pl.semaphore_wait(bar, n)


class Gather:
    def __init__(self, ax, src, buf, sems, cut=None):
        self.ax, self.src, self.buf, self.cut = ax, src, buf, cut
        self.ss, self.rs = sems

    def at(self, b):
        return self.buf.at[b] if self.cut is None else self.buf.at[b, self.cut]

    def send(self, src, b, sem, dst):
        rcopy(src, self.at(b), self.ss.at[sem], self.rs.at[b], **self.ax.to(dst)).start()

    def start(self):
        ax = self.ax
        for sem, d in ((0, 1), (1, -1)):

            @pl.when(jnp.logical_and(ax.o + d >= 0, ax.o + d < ax.outer))
            def _():
                self.send(self.src, ax.me, sem, ax.me + d * ax.inner)

        self.across(self.src, ax.me, 0)

    def across(self, src, b, k):
        ax = self.ax
        for q in range(1, ax.inner):
            sem = ax.outer + 1 + k * (ax.inner - 1) + q - 1
            self.send(src, b, sem, ax.o * ax.inner + lax.rem(ax.i + q, ax.inner))

    def onward(self, k):
        ax = self.ax
        return ax.o + jnp.where(ax.o > ax.near(k), 1, -1)

    def relay(self, k):
        ax = self.ax
        b = ax.blk(k, 0)
        self.wait(b)
        nxt = self.onward(k)

        @pl.when(jnp.logical_and(nxt >= 0, nxt < ax.outer))
        def _():
            self.send(self.at(b), b, 1 + k, nxt * ax.inner + ax.i)

        self.across(self.at(b), b, k)

    def wait(self, b):
        r = self.at(b)
        rcopy(r, r, self.ss.at[0], self.rs.at[b], **self.ax.to(self.ax.me)).wait_recv()

    def wait_across(self):
        for k in range(self.ax.outer):
            for q in range(1, self.ax.inner):
                self.wait(self.ax.blk(k, q))

    def drain(self):
        ax = self.ax

        def done(sem):
            rcopy(
                self.src, self.src, self.ss.at[sem], self.rs.at[0], **ax.to(ax.me)
            ).wait_send()

        for sem, d in ((0, 1), (1, -1)):

            @pl.when(jnp.logical_and(ax.o + d >= 0, ax.o + d < ax.outer))
            def _():
                done(sem)

        for k in range(1, ax.outer):
            nxt = self.onward(k)

            @pl.when(jnp.logical_and(nxt >= 0, nxt < ax.outer))
            def _():
                done(1 + k)

        for sem in range(ax.outer * (ax.inner - 1)):
            done(ax.outer + 1 + sem)


class Halves:
    def __init__(self, ax, src, buf, sems):
        n = src.shape[0] // 2
        self.parts = []
        for h in range(2):
            cut = pl.ds(n * h, n)
            self.parts.append(
                Gather(ax, src.at[cut], buf, (sems[0].at[h], sems[1].at[h]), cut)
            )

    def start(self):
        for g in self.parts:
            g.start()

    def relay(self, k, ends=None):
        for g in self.parts:
            if ends is None:
                g.relay(k)
                continue
            last = jnp.logical_or(g.ax.o == 0, g.ax.o == g.ax.outer - 1)

            @pl.when(last if ends else jnp.logical_not(last))
            def _():
                g.relay(k)

    def wait(self, b):
        for g in self.parts:
            g.wait(b)

    def drain(self):
        for g in self.parts:
            g.drain()


def gather_sems(outer, inner):
    sem = pltpu.SemaphoreType.DMA
    return sem((outer + 1 + outer * (inner - 1),)), sem((outer * inner,))


def pair(col, p):
    lane = lax.broadcasted_iota(jnp.int32, (col.shape[0], 128), 1)
    return jnp.where(lane < HEAD, col[:, 2 * p : 2 * p + 1], col[:, 2 * p + 1 : 2 * p + 2])


def spread(col, cp):
    return jnp.concatenate([pair(col, p) for p in range(cp // 128)], axis=1)


def row_sums(v):
    part = v[:, :128]
    for p in range(1, v.shape[1] // 128):
        part = part + v[:, 128 * p : 128 * p + 128]
    return jnp.sum(part.T, axis=0, keepdims=True)


def sigmoid(v):
    return 1.0 / (1.0 + jnp.exp(-v))


def softplus(v):
    return jnp.maximum(v, 0.0) + jnp.log1p(jnp.exp(-jnp.abs(v)))


def tri(shape, flip=False):
    i = lax.broadcasted_iota(jnp.int32, shape, 0)
    j = lax.broadcasted_iota(jnp.int32, shape, 1)
    return j >= i if flip else i >= j


def split(x2):
    lane = lax.broadcasted_iota(jnp.int32, x2.shape, 1)
    return jnp.concatenate([jnp.where(lane < HEAD, x2, 0), jnp.where(lane >= HEAD, x2, 0)], axis=0)


def chunk_inputs(c, ext, rawb, small, cp):
    r0 = pl.multiple_of(c * Q, Q)
    v = ext[pl.ds(r0, Q + 16), :].astype(f32)
    C = cp + 2 * N
    taps = [pltpu.roll(v, 3 - k, 0)[16:] if k < 3 else v[16:] for k in range(4)]
    summed = small[4:5, :C]
    for k in range(4):
        summed = summed + small[k : k + 1, :C] * taps[k]
    sig = sigmoid(summed)
    raw = rawb[pl.ds(r0, Q), :].astype(f32) + small[7:8, 0:128]
    dt = softplus(raw)
    rate = -jnp.exp(small[7:8, 128:256])
    cum = mm(tri((Q, Q)).astype(f32), dt * rate, precision=HI)
    return taps, summed, sig, raw, dt, rate, cum


def skip_row(small, cp):
    return spread(small[7:8, 256:384], cp)


def tight(cfg):
    S, F, T, D, cp, WC = cfg
    return S * T * D * 2 > 2**22


def lanes_from(row, shift, width, size):
    n = row.shape[1]
    if n < width:
        row = jnp.concatenate([row, jnp.zeros((row.shape[0], width - n), f32)], axis=1)
    row = pltpu.roll(row, lax.rem(shift + width, width), 1)
    return row[:, :size]


def small_rows(cfg, dims, flat, pc):
    S, F, T, D, cp, WC = cfg
    inner, heads, cols = dims
    conv = inner + 2 * N
    cl, gl, nl, hl = conv // F, inner // F, D // F, heads // F
    def line(v):
        v = v[...].astype(f32)
        v = v if v.ndim == 2 else v[None]
        n = -v.shape[1] % 128
        return jnp.concatenate([v, jnp.zeros((v.shape[0], n), f32)], axis=1) if n else v

    parts = [line(v) for v in flat]
    rows = jnp.concatenate(parts[:2] + [jnp.zeros((3, parts[0].shape[1]), f32)], axis=0)
    lane = lax.broadcasted_iota(jnp.int32, (8, cp), 1)
    xs = lanes_from(rows, cl * pc.f - cols * pc.s, conv, cp)
    bc = lanes_from(rows, cl * pc.f - inner, conv, 2 * N)
    gate = lanes_from(parts[2], gl * pc.f - cols * pc.s, inner, cp)
    if cols < cp:
        xs = jnp.where(lane < cols, xs, 0.0)
        gate = jnp.where(lane[0:1] < cols, gate, 0.0)
    norm = lanes_from(parts[3], nl * pc.f, D, D)
    hg = heads // S
    hv = jnp.concatenate(parts[4:7] + [jnp.zeros((5, 128), f32)], axis=0)
    hv = lanes_from(hv, hl * pc.f - hg * pc.s, 128, 128)
    hv = jnp.where(lane[:, :128] < hg, hv, 0.0)

    def wide(v):
        return jnp.concatenate([v, jnp.zeros((v.shape[0], D - v.shape[1]), f32)], axis=1)

    return jnp.concatenate(
        [
            wide(jnp.concatenate([xs, bc], axis=1)[0:5]),
            wide(gate),
            norm,
            wide(jnp.concatenate([hv[0:1], hv[1:2], hv[2:3]], axis=1)),
        ],
        axis=0,
    )


def body_fwd(cfg, dims, tok, cot, wsrc, wo, step, flat, R):
    S, F, T, D, cp, WC = cfg
    inner, heads, cols = dims
    L = S * T
    C = cp + 2 * N
    per = S // F
    pc = Place(S, F)
    own = R.w_all.at[pc.f]
    hg = heads // S
    up = -(-heads // 8) * 8
    st = step[...].astype(f32)
    if up > heads:
        st = jnp.concatenate([st, jnp.zeros((up - heads, st.shape[1]), f32)], axis=0)
    st = pltpu.roll(st, lax.rem(up - hg * pc.s, up), 0)[:8].T
    lane = lax.broadcasted_iota(jnp.int32, st.shape, 1)
    st = jnp.where(lane < hg, st, 0.0)
    st = jnp.concatenate([st, jnp.zeros((st.shape[0], 120), f32)], axis=1).astype(bf16)
    R.w_all[pc.f, :, 2 * cp + 2 * N :] = st
    if cols < cp:
        parts = [(wsrc[0], own.at[:, pl.ds(0, 2 * cp + 2 * N)])]
    else:
        (win,) = wsrc
        col = pl.multiple_of(pc.s * cols, cols)
        parts = [
            (win.at[:, pl.ds(col, cols)], own.at[:, pl.ds(0, cols)]),
            (win.at[:, pl.ds(inner + col, cols)], own.at[:, pl.ds(cols, cols)]),
            (win.at[:, pl.ds(2 * inner, 2 * N)], own.at[:, pl.ds(2 * cols, 2 * N)]),
        ]
    parts = [pltpu.make_async_copy(a, b, R.wsem.at[i]) for i, (a, b) in enumerate(parts)]
    for c in parts:
        c.start()
    R.sm_own[...] = small_rows(cfg, dims, flat, pc)
    pc.barrier()
    tg = Halves(pc.seq, tok, R.tok_all, (R.ss_t, R.rs_t))
    cg = Halves(pc.seq, cot, R.cot_all, (R.ss_c, R.rs_c))
    wg = Gather(pc.fsdp, own, R.w_all, (R.ss_w, R.rs_w))
    first = lax.rem(pc.s, per)
    owner = pc.s // per
    wogs = []
    if not tight(cfg):
        for p in range(per):
            at = lax.rem(first + p, per)
            wogs.append(
                Gather(pc.fsdp, wo.at[at], R.w_out.at[at], (R.ss_o.at[p], R.rs_o.at[p]))
            )
    sm = R.sm_own
    tg.start()
    for k in range(1, F):
        to = lax.rem(pc.f + k, F)
        rcopy(sm, R.sm_all.at[pc.f], R.ss_m.at[k], R.rs_m.at[pc.f], fsdp=to).start()
    for c in parts:
        c.wait()
    wg.start()
    keep = []
    for p in range(len(wogs)):
        wogs[p].start()
        at = lax.rem(first + p, per)
        keep.append(pltpu.make_async_copy(wo.at[at], R.w_out.at[at, pc.f], R.osem.at[p]))
    if tight(cfg):
        keep.append(pltpu.make_async_copy(wo, R.wo_g, R.osem.at[0]))

        @pl.when(pc.f == owner)
        def _():
            keep[0].start()
            for k in range(1, F):
                to = lax.rem(pc.f + k, F)
                rcopy(wo, R.wo_g, R.ss_o.at[k], R.rs_o.at[0], fsdp=to).start()
    else:
        for c in keep:
            c.start()
    R.tok_all[pc.s] = tok[...]
    R.cot_all[pc.s] = cot[...]
    R.sm_all[pc.f] = sm[...]
    R.ext[0:16, :] = jnp.zeros((16, C), bf16)
    for k in range(1, F):
        o = lax.rem(pc.f + k, F)
        rcopy(sm, R.sm_all.at[o], R.ss_m.at[0], R.rs_m.at[o], fsdp=pc.f).wait_recv()
    total = R.sm_all[0]
    for k in range(1, F):
        total = total + R.sm_all[k]
    R.small[...] = total
    small = R.small
    tg.relay(1)
    tg.relay(2)
    tg.relay(3, False)
    for k in range(1, F // 2):
        wg.relay(k)
    tg.relay(3, True)
    cg.start()
    wg.wait_across()

    def project(j, carry):
        k, q = j // pc.X, lax.rem(j, pc.X)
        b = pc.blk(k, q)

        @pl.when(q > 0)
        def _():
            tg.wait(b)

        @pl.when(j == S // 2)
        def _():
            cg.relay(1)

        r = R.tok_all[b].astype(f32)
        scale = lax.rsqrt(jnp.mean(r * r, axis=1, keepdims=True) + epsilon)
        h = r * scale * small[6:7, :]
        r0 = pl.multiple_of(b * T, T)
        R.hid_t[:, pl.ds(r0, T)] = h.T.astype(bf16)
        out = mm(h.astype(bf16), R.w_all[...].reshape(D, WC)).astype(bf16)
        R.zb[pl.ds(r0, T), :] = out[:, :cp]
        R.rawb[pl.ds(r0, T), :] = out[:, 2 * cp + 2 * N :]
        R.ext[pl.ds(r0 + 16, T), :] = out[:, cp : 2 * cp + 2 * N]
        return carry

    lax.fori_loop(0, S, project, 0)
    R.state[...] = jnp.zeros((N, cp), f32)

    def forward(c, carry):
        @pl.when(jnp.logical_or(c == 0, c == 5))
        def _():
            cg.relay(2 + c // 5)

        r0 = pl.multiple_of(c * Q, Q)
        taps, summed, sig, raw, dt, rate, cum = chunk_inputs(c, R.ext, R.rawb, small, cp)
        act = summed * sig
        x = act[:, :cp]
        bb = act[:, cp : cp + N].astype(bf16)
        cb = act[:, cp + N :].astype(bf16)
        cum_t = cum.T
        dt_t = dt.T
        scores = mm(cb, bb, 1, 1)
        causal = tri((Q, Q))
        parts = []
        for p in range(cp // 128):
            mix = []
            for h in (2 * p, 2 * p + 1):
                gap = jnp.where(causal, cum[:, h : h + 1] - cum_t[h : h + 1, :], -1e30)
                mix.append((jnp.exp(gap) * scores * dt_t[h : h + 1, :]).astype(bf16))
            parts.append(
                mm(jnp.concatenate(mix, axis=1), split(x[:, 128 * p : 128 * p + 128]).astype(bf16))
            )
        state = R.state[...]
        R.states[c] = state
        last = cum[Q - 1 : Q, :]
        y = jnp.concatenate(parts, axis=1) + mm(cb, state.astype(bf16)) * spread(jnp.exp(cum), cp)
        y = y + skip_row(small, cp) * x
        wx = (spread(jnp.exp(last - cum) * dt, cp) * x).astype(bf16)
        R.state[...] = spread(jnp.exp(last), cp) * state + mm(bb, wx, 0, 0)
        R.y[pl.ds(r0, Q), :] = y
        z = R.zb[pl.ds(r0, Q), :].astype(f32)
        gated = (y * (z * sigmoid(z))).astype(bf16)
        R.dpx[pl.ds(r0, Q), :cp] = gated
        g32 = gated.astype(f32)
        R.st[0:1, pl.ds(r0, Q)] = row_sums(g32 * g32)
        return carry

    lax.fori_loop(0, L // Q, forward, 0)

    if tight(cfg):
        group = R.wo_g

        @pl.when(pc.f != owner)
        def _():
            rcopy(wo, R.wo_g, R.ss_o.at[0], R.rs_o.at[0], fsdp=pc.f).wait_recv()

        @pl.when(pc.f == owner)
        def _():
            keep[0].wait()
    else:
        group = R.w_out.at[first, owner]
        for c in keep:
            c.wait()
        for k in range(1, F // 2):
            wogs[0].relay(k)
        wogs[0].wait_across()

    def mixed(j, carry):
        k, q = j // pc.X, lax.rem(j, pc.X)
        b = pc.blk(k, q)

        @pl.when(q > 0)
        def _():
            cg.wait(b)

        r0 = pl.multiple_of(b * T, T)
        mg = mm(R.cot_all[b], group[...], 1, 1)
        R.mg[pl.ds(r0, T), :] = mg
        g = mg * small[5:6, :cp] * R.dpx[pl.ds(r0, T), :cp].astype(f32)
        R.st[1:2, pl.ds(r0, T)] = row_sums(g)
        return carry

    lax.fori_loop(0, S, mixed, 0)
    for k in range(1, S):
        rcopy(
            R.st, R.st_all.at[pc.s], R.ss_s.at[k], R.rs_s.at[pc.s],
            seq=lax.rem(pc.s + k, S),
        ).start()
    R.st_all[pc.s] = R.st[...]
    for k in range(1, S):
        o = lax.rem(pc.s + k, S)
        rcopy(R.st, R.st_all.at[o], R.ss_s.at[0], R.rs_s.at[o], seq=pc.s).wait_recv()
    total = R.st_all[0]
    for k in range(1, S):
        total = total + R.st_all[k]
    R.stats[...] = total

    for g in [tg, cg, wg]:
        g.drain()
    for k in range(1, S):
        rcopy(R.st, R.st, R.ss_s.at[k], R.rs_s.at[0], seq=pc.s).wait_send()
    for k in range(1, F):
        rcopy(sm, sm, R.ss_m.at[k], R.rs_m.at[0], fsdp=pc.f).wait_send()
    if tight(cfg):

        @pl.when(pc.f == owner)
        def _():
            for k in range(1, F):
                rcopy(wo, wo, R.ss_o.at[k], R.rs_o.at[0], fsdp=pc.f).wait_send()

    return wogs


def fwd_scratch(cfg):
    S, F, T, D, cp, WC = cfg
    L = S * T
    Dl = D // F
    C = cp + 2 * N
    V = pltpu.VMEM
    sem = pltpu.SemaphoreType.DMA
    per = S // F
    seq = gather_sems(4, S // 4)
    fsdp = gather_sems(F // 2, 2)
    out = SimpleNamespace(
        tok_all=V((S, T, D), bf16),
        cot_all=V((S, T, D), bf16),
        w_all=V((F, Dl, WC), bf16),
        sm_own=V((8, D), f32),
        sm_all=V((F, 8, D), f32),
        small=V((8, D), f32),
        hid_t=V((D, L), bf16),
        zb=V((L, cp), bf16),
        rawb=V((L, 128), bf16),
        ext=V((16 + L, C), bf16),
        state=V((N, cp), f32),
        states=V((L // Q, N, cp), f32),
        y=V((L, cp), f32),
        mg=V((L, cp), f32),
        st=V((2, L), f32),
        st_all=V((S, 2, L), f32),
        stats=V((2, L), f32),
        ss_t=sem((2,) + seq[0].shape),
        rs_t=sem((2,) + seq[1].shape),
        ss_c=sem((2,) + seq[0].shape),
        rs_c=sem((2,) + seq[1].shape),
        ss_w=fsdp[0],
        rs_w=fsdp[1],
        ss_m=sem((F,)),
        rs_m=sem((F,)),
        wsem=sem((4,)),
        osem=sem((per,)),
        ss_s=sem((S,)),
        rs_s=sem((S,)),
    )
    if tight(cfg):
        out.wo_g = V((cp, D), bf16)
        out.ss_o = out.rs_o = sem((F,))
    else:
        out.w_out = V((per, F, cp, D), bf16)
        out.ss_o = sem((per,) + fsdp[0].shape)
        out.rs_o = sem((per,) + fsdp[1].shape)
    return out


class Scatter:
    def __init__(self, pc, part, rx, rz, sems):
        self.pc, self.part, self.rx, self.rz = pc, part, rx, rz
        self.ssx, self.rsx, self.ssz, self.rsz = sems

    def across(self, b):
        pc = self.pc
        zb, xb = b // pc.X, lax.rem(b, pc.X)

        @pl.when(xb != pc.x)
        def _():
            slot = lax.rem(pc.x - xb - 1 + pc.X, pc.X)
            rcopy(
                self.part.at[b], self.rx.at[zb, slot], self.ssx.at[b], self.rsx.at[zb, slot],
                seq=pc.z * pc.X + xb,
            ).start()

    def column(self, zb):
        pc = self.pc
        b = zb * pc.X + pc.x
        total = self.part[b].astype(f32)
        for q in range(pc.X - 1):
            r = self.rx.at[zb, q]
            rcopy(r, r, self.ssx.at[0], self.rsx.at[zb, q], seq=pc.s).wait_recv()
            total = total + self.rx[zb, q].astype(f32)
        self.part[b] = total.astype(bf16)

        @pl.when(zb != pc.z)
        def _():
            slot = lax.rem(pc.z - zb - 1 + pc.Z, pc.Z)
            rcopy(
                self.part.at[b], self.rz.at[slot], self.ssz.at[zb], self.rsz.at[slot], seq=b
            ).start()

    def total(self):
        pc = self.pc
        out = self.part[pc.s].astype(f32)
        for q in range(pc.Z - 1):
            r = self.rz.at[q]
            rcopy(r, r, self.ssz.at[0], self.rsz.at[q], seq=pc.s).wait_recv()
            out = out + self.rz[q].astype(f32)
        return out

    def drain(self):
        pc = self.pc
        r = self.rz.at[0]
        for b in range(pc.S):

            @pl.when(b % pc.X != pc.x)
            def _():
                rcopy(r, r, self.ssx.at[b], self.rsz.at[0], seq=pc.s).wait_send()

        for zb in range(pc.Z):

            @pl.when(zb != pc.z)
            def _():
                rcopy(r, r, self.ssz.at[zb], self.rsz.at[0], seq=pc.s).wait_send()


class Shared:
    def __init__(self, pc, part, recv, ss, rs):
        self.pc, self.part, self.recv, self.ss, self.rs = pc, part, recv, ss, rs

    def send(self, k):
        pc = self.pc
        to = lax.rem(pc.f + k, pc.F)
        rcopy(
            self.part.at[to], self.recv.at[k - 1], self.ss.at[k - 1], self.rs.at[k - 1], fsdp=to
        ).start()

    def total(self):
        pc = self.pc
        out = self.part[pc.f].astype(f32)
        for k in range(1, pc.F):
            r = self.recv.at[k - 1]
            rcopy(r, r, self.ss.at[k - 1], self.rs.at[k - 1], fsdp=pc.f).wait_recv()
            out = out + self.recv[k - 1].astype(f32)
        return out

    def drain(self):
        for k in range(1, self.pc.F):
            r = self.recv.at[k - 1]
            rcopy(r, r, self.ss.at[k - 1], self.rs.at[k - 1], fsdp=self.pc.f).wait_send()


def body_bwd(cfg, dims, tok, cot, wogs, R, O):
    S, F, T, D, cp, WC = cfg
    inner = float(dims[0])
    L = S * T
    C = cp + 2 * N
    Dl = D // F
    nc = L // Q
    cr = cp // F
    per = S // F
    bh = Dl // S
    pc = Place(S, F)
    small = R.small
    if tight(cfg):
        blk = Scatter(pc, R.bp, R.brx, R.brz, (R.bs0, R.bs1, R.bs2, R.bs3))
    hid = Scatter(pc, R.tok_all, R.hrx, R.hrz, (R.hs0, R.hs1, R.hs2, R.hs3))
    zs = Shared(pc, R.zp, R.zr, R.zs0, R.zs1)
    os_ = Shared(pc, R.op, R.orecv, R.os0, R.os1)
    nt = cp // 128

    def xs(t):
        return Shared(pc, R.xp.at[t], R.xr.at[t], R.xs0.at[t], R.xs1.at[t])

    def xg(t):
        return Gather(pc.seq, R.xred.at[t], O.gx.at[t], (R.gx0.at[t], R.gx1.at[t]))

    def own_x(t):
        return pltpu.make_async_copy(R.xred.at[t], O.gx.at[t, pc.s], R.xsem.at[t])

    def settle(t):
        R.xred[t] = xs(t).total().astype(bf16)
        xg(t).start()
        own_x(t).start()
    bs = Shared(pc, R.cp_, R.cr_, R.cs0, R.cs1)
    zg = Gather(pc.seq, R.zred, O.gz, (R.gz0, R.gz1))
    og = Gather(pc.seq, R.ored, O.go_s, (R.go0, R.go1))
    sg = Gather(pc.seq, R.asum, O.sm, (R.as2, R.as3))

    def direct(src, dst, ss, rs, to):
        rcopy(src, dst.at[pc.s], ss.at[to], rs.at[pc.s], seq=to).start()

    def arrived(dst, ss, rs):
        for k in range(1, S):
            o = lax.rem(pc.s + k, S)
            r = dst.at[o]
            rcopy(r, r, ss.at[0], rs.at[o], seq=pc.s).wait_recv()

    def sent(src, ss, rs):
        for k in range(1, S):
            rcopy(src, src, ss.at[lax.rem(pc.s + k, S)], rs.at[0], seq=pc.s).wait_send()

    def own(src, dst, i):
        return pltpu.make_async_copy(src, dst, R.lsem.at[i])

    gate = small[5:6, :cp]
    R.acc[...] = jnp.zeros((16, D), f32)
    R.hacc[...] = jnp.zeros((2, 8, 128), f32)
    R.dstate[...] = jnp.zeros((N, cp), f32)
    R.head[...] = jnp.zeros((8, C), f32)

    def first(i, carry):
        c = lax.rem(pc.s + 1 + i, nc)
        r0 = pl.multiple_of(c * Q, Q)
        rows = pl.ds(r0, Q)
        st = jnp.concatenate([R.stats[:, rows], jnp.zeros((6, Q), f32)], axis=0).T
        scale = lax.rsqrt(st[:, 0:1] / inner + epsilon)
        mean = st[:, 1:2] / inner
        gated = R.dpx[rows, :cp].astype(f32)
        mg = R.mg[rows, :]
        ng = gated * scale
        mn = ng * gate
        R.acc[5:6, :cp] += jnp.sum(mg * ng, axis=0, keepdims=True)
        gg = (scale * (mg * gate) - scale * scale * scale * gated * mean).astype(bf16).astype(f32)
        z = R.zb[rows, :].astype(f32)
        sz = sigmoid(z)
        R.zb[rows, :] = (gg * R.y[rows, :] * (sz * (1.0 + z * (1.0 - sz)))).astype(bf16)
        R.mg[rows, :] = gg * (z * sz)
        R.mn_t[:, rows] = mn.T.astype(bf16)
        if tight(cfg):
            R.dpx[rows, :cp] = mn.astype(bf16)
        else:
            R.mn[c] = mn.astype(bf16)

            @pl.when(c != pc.s)
            def _():
                direct(R.mn.at[c], R.mall, R.ms0, R.ms1, c)

        return carry

    def block(i, carry):
        c = nc - 1 - i
        rows = pl.ds(pl.multiple_of(c * Q, Q), Q)
        R.bp[c] = mm(R.dpx[rows, :cp], R.wo_g[...]).astype(bf16)
        blk.across(c)
        return carry

    lax.fori_loop(0, nc, first, 0)

    def zpart(k, carry):
        to = lax.rem(pc.f + k, F)
        rows = pl.ds(pl.multiple_of(to * Dl, Dl), Dl)
        R.zp[to] = mm(R.hid_t[rows, :], R.zb[...]).astype(bf16)

        @pl.when(k < F)
        def _():
            rcopy(
                R.zp.at[to], R.zr.at[k - 1], R.zs0.at[k - 1], R.zs1.at[k - 1], fsdp=to
            ).start()
        return carry

    lax.fori_loop(1, F + 1, zpart, 0)
    W = 384

    def opart(j, carry):
        cols = pl.ds(pl.multiple_of(j * W, W), W)
        a = R.cot_all[:, :, cols].reshape(L, W)
        R.op[:, :, cols] = mm(R.mn_t[...], a).reshape(F, cr, W).astype(bf16)
        return carry

    lax.fori_loop(0, D // W, opart, 0)
    for g in wogs[1:]:
        for k in range(1, F // 2):
            g.relay(k)
    for k in range(1, F):
        os_.send(k)
    if tight(cfg):
        lax.fori_loop(0, nc, block, 0)

    sel = (
        lax.broadcasted_iota(jnp.int32, (8, cp), 1) // HEAD
        == lax.broadcasted_iota(jnp.int32, (8, cp), 0)
    ).astype(f32)
    sub = lax.broadcasted_iota(jnp.int32, (8, Q), 0)

    def scan(i, carry):
        c = nc - 1 - i
        r0 = pl.multiple_of(c * Q, Q)
        rows = pl.ds(r0, Q)

        if tight(cfg):

            @pl.when(i < pc.Z)
            def _():
                blk.column(pc.Z - 1 - i)

        @pl.when(i == 1)
        def _():
            R.zred[...] = zs.total().astype(bf16)
            zg.start()
            own(R.zred, O.gz.at[pc.s], 0).start()

        @pl.when(i == 2)
        def _():
            R.ored[...] = os_.total().astype(bf16)
            og.start()
            own(R.ored, O.go_s.at[pc.s], 5).start()

        @pl.when(jnp.logical_and(i >= 4, i < 4 + pc.Z - 1))
        def _():
            zg.relay(i - 3)

        @pl.when(jnp.logical_and(i >= 6, i < 6 + pc.Z - 2))
        def _():
            og.relay(i - 5)

        taps, summed, sig, raw, dt, rate, cum = chunk_inputs(c, R.ext, R.rawb, small, cp)
        act = summed * sig
        x = act[:, :cp]
        xb = x.astype(bf16)
        bb = act[:, cp : cp + N].astype(bf16)
        cb = act[:, cp + N :].astype(bf16)
        cum_t = cum.T
        dt_t = dt.T
        dy = R.mg[rows, :]
        dyb = dy.astype(bf16)
        last = cum[Q - 1 : Q, :]
        edy = spread(jnp.exp(cum), cp) * dy
        edyb = edy.astype(bf16)
        wdec = jnp.exp(last - cum)
        w = wdec * dt
        state = R.states[c]
        sb = state.astype(bf16)
        ds = R.dstate[...]
        dsb = ds.astype(bf16)
        ws = spread(w, cp)
        v = mm(bb, dsb)
        carr = mm(sel, edy * mm(cb, sb), 1, 1, HI)
        dw = mm(sel, x * v, 1, 1, HI)
        db = mm((ws * x).astype(bf16), dsb, 1, 1)
        dc = mm(edyb, sb, 1, 1)
        dlast = mm(sel, jnp.sum(state * ds, axis=0, keepdims=True), 1, 1, HI)
        R.dstate[...] = spread(jnp.exp(last), cp) * ds + mm(cb, edyb, 0, 0)
        scores = mm(bb, cb, 1, 1)
        seen = tri((Q, Q), True)
        dtb = dt_t[0:8].astype(bf16)
        dsc = jnp.zeros((Q, Q), f32)
        direct = jnp.zeros((8, Q), f32)
        onto = jnp.zeros((8, Q), f32)
        parts = []
        for p in range(cp // 128):
            cols = slice(128 * p, 128 * p + 128)
            g2 = mm(split(x[:, cols]).astype(bf16), dyb[:, cols], 1, 1)
            mix = []
            for h in (2 * p, 2 * p + 1):
                g = g2[:Q] if h % 2 == 0 else g2[Q:]
                decay = jnp.exp(jnp.where(seen, cum_t[h : h + 1, :] - cum[:, h : h + 1], -1e30))
                ls = decay * scores
                mix.append((ls * dt[:, h : h + 1]).astype(bf16))
                e = (g * ls).astype(bf16)
                dsc = dsc + g * decay * dt[:, h : h + 1]
                direct = direct + mm(jnp.where(sub == h, 1.0, 0.0).astype(bf16), e, 1, 1)
                onto = onto + mm(jnp.where(sub == h, dtb.astype(f32), 0.0).astype(bf16), e)
            parts.append(mm(jnp.concatenate(mix, axis=1), split(dy[:, cols]).astype(bf16)))
        dscb = dsc.astype(bf16)
        db = db + mm(dscb, cb)
        dc = dc + mm(dscb, bb, 0, 0)
        dx = skip_row(small, cp) * dy + ws * v + jnp.concatenate(parts, axis=1)
        R.acc[7:8, :cp] += jnp.sum(dy * x, axis=0, keepdims=True)
        dt_r = dt_t[0:8]
        wdec_r = wdec.T[0:8]
        w_r = wdec_r * dt_r
        rate_r = jnp.broadcast_to(rate, (128, 128)).T[0:8, 0:1]
        last_r = jnp.exp(cum_t[0:8, Q - 1 : Q])
        dcum = carr + onto - dtb.astype(f32) * direct - w_r * dw
        end = jnp.sum(w_r * dw, axis=1, keepdims=True) + last_r * dlast
        da = mm(dcum, tri((Q, Q)).astype(f32), precision=HI) + end
        ddt = direct + wdec_r * dw + rate_r * da
        draw = ddt * sigmoid(raw).T[0:8]
        R.hacc[0] += draw
        R.hacc[1] += da * dt_r * rate_r
        dact = jnp.concatenate([dx, db, dc], axis=1)
        dsum = dact * (sig * (1.0 + summed * (1.0 - sig)))
        full = jnp.concatenate([dsum, R.head[...]], axis=0)
        dxbc = jnp.zeros((Q, C), f32)
        for k in range(4):
            R.acc[k : k + 1, :C] += jnp.sum(dsum * taps[k], axis=0, keepdims=True)
            moved = pltpu.roll(full, Q + 8 - (3 - k), 0)[:Q] if k < 3 else dsum
            dxbc = dxbc + small[k : k + 1, :C] * moved
        R.acc[4:5, :C] += jnp.sum(dsum, axis=0, keepdims=True)
        R.head[...] = dsum[:8]
        R.dpx[rows, :C] = dxbc.astype(bf16)
        R.acc[8:16, :] += mm(draw.astype(bf16), R.hid_t[:, rows], 1, 1)
        pad = jnp.concatenate([draw, jnp.zeros((120, Q), f32)], axis=0).T
        R.dpx[rows, C:] = pad.astype(bf16)
        grad = jnp.concatenate([R.zb[rows, :], R.dpx[rows, :]], axis=1)
        hp = mm(grad, R.w_all[...].reshape(D, WC), 1, 1)
        r = R.tok_all[c].astype(f32)
        scale = lax.rsqrt(jnp.mean(r * r, axis=1, keepdims=True) + epsilon)
        R.acc[6:7, :] += jnp.sum(hp * r * scale, axis=0, keepdims=True)
        R.tok_all[c] = hp.astype(bf16)
        hid.across(c)
        return carry

    lax.fori_loop(0, nc, scan, 0)

    diag = lax.broadcasted_iota(jnp.int32, (8, 128), 0) == lax.broadcasted_iota(
        jnp.int32, (8, 128), 1
    )

    def along(v):
        return jnp.sum(jnp.where(diag, jnp.sum(v, axis=1, keepdims=True), 0.0), axis=0, keepdims=True)

    dskip = jnp.sum(
        jnp.where(diag, mm(sel, R.acc[7:8, :cp], 1, 1, HI), 0.0), axis=0, keepdims=True
    )
    R.acc[7:8, :] = jnp.concatenate(
        [along(R.hacc[0]), along(R.hacc[1]), dskip, jnp.zeros((1, D - 384), f32)], axis=1
    )
    R.accb[...] = R.acc[...].astype(bf16)
    for k in range(1, F):
        to = lax.rem(pc.f + k, F)
        rcopy(
            R.accb, R.ar.at[k - 1], R.as0.at[k - 1], R.as1.at[k - 1], fsdp=to
        ).start()

    for t in range(nt):

        def xpart(k, carry):
            to = lax.rem(pc.f + k, F)
            rows = pl.ds(pl.multiple_of(to * Dl, Dl), Dl)
            R.xp[t, to] = mm(R.hid_t[rows, :], R.dpx[:, 128 * t : 128 * t + 128]).astype(bf16)

            @pl.when(k < F)
            def _():
                rcopy(
                    R.xp.at[t, to], R.xr.at[t, k - 1], R.xs0.at[t, k - 1], R.xs1.at[t, k - 1],
                    fsdp=to,
                ).start()
            return carry

        lax.fori_loop(1, F + 1, xpart, 0)

    def lower(k, carry):
        to = lax.rem(pc.f + k, F)
        rows = pl.ds(pl.multiple_of(to * Dl, Dl), Dl)
        R.cp_[to] = mm(R.hid_t[rows, :], R.dpx[:, cp:C]).astype(bf16)

        @pl.when(k < F)
        def _():
            rcopy(
                R.cp_.at[to], R.cr_.at[k - 1], R.cs0.at[k - 1], R.cs1.at[k - 1], fsdp=to
            ).start()
        return carry

    lax.fori_loop(1, F + 1, lower, 0)
    def hid_column(i, carry):
        hid.column(pc.Z - 1 - i)
        return carry

    total = R.acc[...]
    for k in range(1, F):
        r = R.ar.at[k - 1]
        rcopy(r, r, R.as0.at[k - 1], R.as1.at[k - 1], fsdp=pc.f).wait_recv()
        total = total + R.ar[k - 1].astype(f32)
    R.asum[...] = total.astype(bf16)
    sg.start()
    own(R.asum, O.sm.at[pc.s], 1).start()
    og.relay(3)
    settle(0)
    for t in range(1, nt):
        settle(t)
    low = bs.total()
    for g in range(S):
        R.cb[g] = low[g * bh : (g + 1) * bh].astype(bf16)
    for k in range(1, S):
        to = lax.rem(pc.s + k, S)
        direct(R.cb.at[to], R.cbr, R.cb0, R.cb1, to)
    lax.fori_loop(0, 2, hid_column, 0)
    sg.relay(1)
    for t in range(nt):
        xg(t).relay(1)
    sg.relay(2)
    for t in range(nt):
        xg(t).relay(2)
    arrived(R.cbr, R.cb0, R.cb1)
    R.cbr[pc.s] = R.cb[pc.s]
    low = R.cbr[0].astype(f32)
    for g in range(1, S):
        low = low + R.cbr[g].astype(f32)
    R.cbd[...] = low.astype(bf16)
    for k in range(1, S):
        direct(R.cbd, O.gbc, R.cd0, R.cd1, lax.rem(pc.s + k, S))
    own(R.cbd, O.gbc.at[pc.s], 4).start()
    lax.fori_loop(2, pc.Z, hid_column, 0)
    own(R.ored, O.go_s.at[pc.s], 5).wait()
    og.wait_across()
    for k in range(1, F):
        to = lax.rem(pc.f + k, F)
        rcopy(
            O.go_s.at[pl.ds(to * per, per)], O.go.at[pc.f], R.gs0.at[k], R.gs1.at[pc.f],
            fsdp=to,
        ).start()
    own(O.go_s.at[pl.ds(pc.f * per, per)], O.go.at[pc.f], 3).start()
    sg.relay(3)
    for t in range(nt):
        xg(t).relay(3)

    mine = tok[...].astype(f32)
    if tight(cfg):
        O.block[...] = (mine + blk.total()).astype(bf16)
    else:
        for g in wogs[1:]:
            g.wait_across()
        arrived(R.mall, R.ms0, R.ms1)
        R.mall[pc.s] = R.mn[pc.s]
        R.total[...] = mine

        def add(g, carry):
            w = R.w_out[lax.rem(g, per), g // per]
            R.total[...] += mm(R.mall[g], w)
            return carry

        lax.fori_loop(0, S, add, 0)
        O.block[...] = R.total[...].astype(bf16)
    scale = lax.rsqrt(jnp.mean(mine * mine, axis=1, keepdims=True) + epsilon)
    e = hid.total() * small[6:7, :]
    mean = jnp.mean(e * mine, axis=1, keepdims=True)
    O.input[...] = cot[...].astype(f32) + scale * e - scale * scale * scale * mine * mean

    zg.wait_across()
    for k in range(1, F):
        o = lax.rem(pc.f + k, F)
        r = O.go.at[o]
        rcopy(r, r, R.gs0.at[0], R.gs1.at[o], fsdp=pc.f).wait_recv()
    arrived(O.gbc, R.cd0, R.cd1)
    sg.wait_across()
    for t in range(nt):
        xg(t).wait_across()
        own_x(t).wait()
    own(R.zred, O.gz.at[pc.s], 0).wait()
    own(R.asum, O.sm.at[pc.s], 1).wait()
    own(O.go_s.at[pl.ds(pc.f * per, per)], O.go.at[pc.f], 3).wait()
    own(R.cbd, O.gbc.at[pc.s], 4).wait()
    if tight(cfg):
        blk.drain()
    else:
        sent(R.mn.at[0], R.ms0, R.ms1)
    sent(R.cb.at[0], R.cb0, R.cb1)
    sent(R.cbd, R.cd0, R.cd1)
    for a in [hid, zs, os_, bs, zg, og, sg] + wogs:
        a.drain()
    for t in range(nt):
        xs(t).drain()
        xg(t).drain()
    for k in range(1, F):
        r = R.ar.at[k - 1]
        rcopy(r, r, R.as0.at[k - 1], R.as1.at[0], fsdp=pc.f).wait_send()
        r = O.go.at[0]
        rcopy(r, r, R.gs0.at[k], R.gs1.at[0], fsdp=pc.f).wait_send()


def bwd_scratch(cfg):
    S, F, T, D, cp, WC = cfg
    L = S * T
    Dl = D // F
    C = cp + 2 * N
    Z, X = 4, S // 4
    cr = cp // F
    bh = Dl // S
    V = pltpu.VMEM
    sem = pltpu.SemaphoreType.DMA
    seq = gather_sems(4, S // 4)
    nt = cp // 128
    out = SimpleNamespace(
        acc=V((16, D), f32),
        asum=V((16, D), bf16),
        accb=V((16, D), bf16),
        ar=V((F - 1, 16, D), bf16),
        hacc=V((2, 8, 128), f32),
        dstate=V((N, cp), f32),
        head=V((8, C), f32),
        mn_t=V((cp, L), bf16),
        dpx=V((L, WC - cp), bf16),
        hrx=V((Z, X - 1, T, D), bf16),
        hrz=V((Z - 1, T, D), bf16),
        zp=V((F, Dl, cp), bf16),
        zr=V((F - 1, Dl, cp), bf16),
        zred=V((Dl, cp), bf16),
        op=V((F, cr, D), bf16),
        orecv=V((F - 1, cr, D), bf16),
        ored=V((cr, D), bf16),
        xp=V((nt, F, Dl, 128), bf16),
        xr=V((nt, F - 1, Dl, 128), bf16),
        xred=V((nt, Dl, 128), bf16),
        cp_=V((F, Dl, 2 * N), bf16),
        cr_=V((F - 1, Dl, 2 * N), bf16),
        cb=V((S, bh, 2 * N), bf16),
        cbr=V((S, bh, 2 * N), bf16),
        cbd=V((bh, 2 * N), bf16),
        lsem=sem((6,)),
        as0=sem((F,)), as1=sem((F,)), as2=seq[0], as3=seq[1],
        gs0=sem((F,)), gs1=sem((F,)), cs0=sem((F,)), cs1=sem((F,)),
        cb0=sem((S,)), cb1=sem((S,)), cd0=sem((S,)), cd1=sem((S,)),
        zs0=sem((F,)), zs1=sem((F,)), gz0=seq[0], gz1=seq[1],
        os0=sem((F,)), os1=sem((F,)), go0=seq[0], go1=seq[1],
        xs0=sem((nt, F)), xs1=sem((nt, F)), xsem=sem((nt,)),
        gx0=sem((nt,) + seq[0].shape), gx1=sem((nt,) + seq[1].shape),
        hs0=sem((S,)), hs1=sem((Z, X - 1)), hs2=sem((Z,)), hs3=sem((Z - 1,)),
    )
    if tight(cfg):
        out.brx = V((Z, X - 1, T, D), bf16)
        out.brz = V((Z - 1, T, D), bf16)
        out.bs0, out.bs1, out.bs2, out.bs3 = out.hs0, out.hs1, out.hs2, out.hs3
    else:
        out.mn = V((S, T, cp), bf16)
        out.mall = V((S, T, cp), bf16)
        out.total = V((T, D), f32)
        out.ms0 = out.ms1 = sem((S,))
    return out


def assemble(cfg, dims, gz, gx, gbc, go, sm, win, step, conv, bias, gate, norm, h0, h1, h2, wout):
    S, F, T, D, cp, WC = cfg
    inner, nheads, cols = dims
    for g in range(S):
        win[:, g * cols : (g + 1) * cols] = gz[g, :, :cols].astype(f32)
        for t in range(gx.shape[0]):
            n = min(128, cols - 128 * t)
            at = inner + g * cols + 128 * t
            win[:, at : at + n] = gx[t, g, :, :n].astype(f32)
    wout[...] = go[0, 0].astype(f32)
    C = cp + 2 * N
    hg = nheads // S
    Dl = D // F
    win[:, 2 * inner :] = gbc[...].astype(f32)

    @pl.when(pl.program_id(0) == 0)
    def _():
        f = lax.axis_index("fsdp")

        def mine(v, size):
            n = v.shape[1]
            return pltpu.roll(v, lax.rem(n - size * f, n), 1)[:, :size]

        v = [sm[g].astype(f32) for g in range(S)]
        total = v[0]
        for g in range(1, S):
            total = total + v[g]
        xs = jnp.concatenate([a[0:8, :cols] for a in v] + [total[0:8, cp:C]], axis=1)
        xs = mine(xs, (inner + 2 * N) // F)
        conv[...] = xs[0:4]
        bias[...] = xs[4]
        gate[...] = mine(jnp.concatenate([a[0:8, :cols] for a in v], axis=1), inner // F)[5]
        norm[...] = mine(total[0:8], Dl)[6]
        n = nheads // F
        zero = jnp.zeros((8, 128 - nheads), f32)
        for i, ref in enumerate((h0, h1, h2)):
            hs = [a[0:8, 128 * i : 128 * i + hg] for a in v]
            ref[...] = mine(jnp.concatenate(hs + [zero], axis=1), n)[7]
        step[...] = jnp.concatenate([mine(a[8:16], Dl)[:hg] for a in v], axis=0)


def shards(tokens, in_weight, step_weight, conv_kernel, conv_bias, step_bias, log_decay,
           skip_gain, gate_gain, norm_gain, out_weight, cotangent):
    S = lax.axis_size("seq")
    F = lax.axis_size("fsdp")
    _, T, D = tokens.shape
    inner = out_weight.shape[0] * F
    heads = step_weight.shape[1]
    cols = inner // S
    cp = -(-cols // 128) * 128
    WC = 2 * cp + 2 * N + 128
    Dl = D // F
    cr = cp // F
    per = S // F
    bh = Dl // S
    cfg = (S, F, T, D, cp, WC)
    dims = (inner, heads, cols)
    s = lax.axis_index("seq")

    def padc(a, to):
        return jnp.pad(a, [(0, 0)] * (a.ndim - 1) + [(0, to - a.shape[-1])])

    def part(a, start, size, axis):
        return lax.dynamic_slice_in_dim(a, start, size, axis)

    if cols % 128 == 0:
        wsrc = (in_weight,)
    else:
        wsrc = (
            jnp.concatenate(
                [
                    padc(part(in_weight, s * cols, cols, 1), cp),
                    padc(part(in_weight, inner + s * cols, cols, 1), cp),
                    in_weight[:, 2 * inner :],
                ],
                axis=1,
            ),
        )
    if tight(cfg):
        wo = jnp.pad(
            part(out_weight, lax.rem(s, per) * cols, cols, 0), [(0, cp - cols), (0, 0)]
        )
    else:
        wo = out_weight.reshape(per, cols, D)
    flat = (conv_kernel, conv_bias, gate_gain, norm_gain, step_bias, log_decay, skip_gain)
    nt = cp // 128
    scratch = {**vars(fwd_scratch(cfg)), **vars(bwd_scratch(cfg))}
    names = list(scratch)
    outs = dict(
        block=jax.ShapeDtypeStruct((T, D), bf16),
        input=jax.ShapeDtypeStruct((T, D), f32),
        gz=jax.ShapeDtypeStruct((S, Dl, cp), bf16),
        gx=jax.ShapeDtypeStruct((nt, S, Dl, 128), bf16),
        gbc=jax.ShapeDtypeStruct((S, bh, 2 * N), bf16),
        go=jax.ShapeDtypeStruct((F, per, cr, D), bf16),
        go_s=jax.ShapeDtypeStruct((S, cr, D), bf16),
        sm=jax.ShapeDtypeStruct((S, 16, D), bf16),
    )
    on = list(outs)
    nw = 1
    nf = len(flat)

    def kern(tok, cot, wo, step, *rest):
        flat, rest = rest[:nf], rest[nf:]
        O = SimpleNamespace(**dict(zip(on, rest[nw : nw + len(on)])))
        R = SimpleNamespace(**dict(zip(names, rest[nw + len(on) :])))
        if tight(cfg):
            R.bp = R.cot_all
        wogs = body_fwd(cfg, dims, tok, cot, rest[:nw], wo, step, flat, R)
        body_bwd(cfg, dims, tok, cot, wogs, R, O)

    v = pl.BlockSpec(memory_space=pltpu.VMEM)
    hbm = pl.BlockSpec(memory_space=pl.ANY)
    res = pl.pallas_call(
        kern,
        out_shape=[outs[n] for n in on],
        in_specs=[v, v, hbm, v] + [v] * nf + [hbm] * nw,
        out_specs=[v, v] + [hbm] * (len(on) - 2),
        scratch_shapes=[scratch[n] for n in names],
        compiler_params=pltpu.CompilerParams(
            collective_id=0, has_side_effects=True, vmem_limit_bytes=VMEM_LIMIT
        ),
    )(tokens[0], cotangent[0], wo, step_weight.T, *flat, *wsrc)
    G = SimpleNamespace(**dict(zip(on, res)))
    pieces = cols // cr
    steps = per * pieces
    rows = Dl // steps
    cl, gl, hl = (inner + 2 * N) // F, inner // F, heads // F

    def whole(*shape):
        return pl.BlockSpec(shape, lambda i: (0,) * len(shape))

    def out(*shape):
        return jax.ShapeDtypeStruct(shape, f32)

    joined = pl.pallas_call(
        lambda *refs: assemble(cfg, dims, *refs),
        grid=(steps,),
        out_shape=[
            out(Dl, 2 * inner + 2 * N), out(heads, Dl), out(4, cl), out(cl), out(gl),
            out(Dl), out(hl), out(hl), out(hl), out(per * cols, D),
        ],
        in_specs=[
            pl.BlockSpec((S, rows, cp), lambda i: (0, i, 0)),
            pl.BlockSpec((nt, S, rows, 128), lambda i: (0, 0, i, 0)),
            pl.BlockSpec((rows, 2 * N), lambda i: (i, 0)),
            pl.BlockSpec((1, 1, cr, D), lambda i: (lax.rem(i, pieces), i // pieces, 0, 0)),
            whole(S, 16, D),
        ],
        out_specs=[
            pl.BlockSpec((rows, 2 * inner + 2 * N), lambda i: (i, 0)),
            whole(heads, Dl), whole(4, cl), whole(cl), whole(gl), whole(Dl), whole(hl),
            whole(hl), whole(hl),
            pl.BlockSpec((cr, D), lambda i: (i, 0)),
        ],
    )(G.gz, G.gx, G.gbc.reshape(Dl, 2 * N), G.go, G.sm)
    win, stepg, conv, bias, gate, norm, hd0, hd1, hd2, wout = joined
    return (
        G.block[None],
        G.input[None],
        win,
        stepg.T,
        conv,
        bias,
        hd0,
        hd1,
        hd2,
        gate,
        norm,
        wout,
    )


def solution(mesh):
    row = P("fsdp", None)
    tok = P("fsdp", "seq", None)
    one = P("fsdp")
    return jax.shard_map(
        shards,
        mesh=mesh,
        in_specs=(tok, row, row, P(None, "fsdp"), one, one, one, one, one, one, row, tok),
        out_specs=(tok, tok, row, row, P(None, "fsdp"), one, one, one, one, one, one, row),
        check_vma=False,
    )
```

```python
from types import SimpleNamespace

import jax
import jax.numpy as jnp
from jax import lax
from jax.experimental import pallas as pl
from jax.experimental.pallas import tpu as pltpu
from jax.sharding import PartitionSpec as P

N = 128
HEAD = 64
Q = 128
epsilon = 1e-05
bf16 = jnp.bfloat16
f32 = jnp.float32
MESH = pl.DeviceIdType.MESH
HI = lax.Precision.HIGHEST
VMEM_LIMIT = 64 * 1024 * 1024 - 65536


def mm(a, b, da=1, db=0, precision=None):
    return lax.dot_general(
        a, b, (((da,), (db,)), ((), ())), preferred_element_type=f32, precision=precision
    )


def rcopy(src, dst, ss, rs, **dev):
    return pltpu.make_async_remote_copy(
        src_ref=src, dst_ref=dst, send_sem=ss, recv_sem=rs, device_id=dev, device_id_type=MESH
    )


class Axis:
    def __init__(self, name, outer, inner):
        self.name, self.outer, self.inner = name, outer, inner
        self.me = lax.axis_index(name)
        self.o = self.me // inner
        self.i = lax.rem(self.me, inner)

    def near(self, k):
        half = self.outer // 2
        side = self.o // half
        m = self.o + side * (self.outer - 1 - 2 * self.o)
        at = jnp.where(k == 0, m, k - m * ((3 - k) // 2))
        return at + side * (self.outer - 1 - 2 * at)

    def blk(self, k, q):
        return self.near(k) * self.inner + lax.rem(self.i + q, self.inner)

    def to(self, d):
        return {self.name: d}


class Place:
    def __init__(self, S, F):
        self.S, self.F = S, F
        self.seq = Axis("seq", 4, S // 4)
        self.fsdp = Axis("fsdp", F // 2, 2)
        self.Z, self.X = 4, S // 4
        self.s, self.z, self.x = self.seq.me, self.seq.o, self.seq.i
        self.f = self.fsdp.me
        self.blk = self.seq.blk

    def barrier(self):
        bar = pltpu.get_barrier_semaphore()
        n = 0
        for k in range(1, self.S):
            pl.semaphore_signal(
                bar, inc=1, device_id={"seq": lax.rem(self.s + k, self.S)}, device_id_type=MESH
            )
            n += 1
        for k in range(1, self.F):
            pl.semaphore_signal(
                bar, inc=1, device_id={"fsdp": lax.rem(self.f + k, self.F)}, device_id_type=MESH
            )
            n += 1
        pl.semaphore_wait(bar, n)


class Gather:
    def __init__(self, ax, src, buf, sems, cut=None):
        self.ax, self.src, self.buf, self.cut = ax, src, buf, cut
        self.ss, self.rs = sems

    def at(self, b):
        return self.buf.at[b] if self.cut is None else self.buf.at[b, self.cut]

    def send(self, src, b, sem, dst):
        rcopy(src, self.at(b), self.ss.at[sem], self.rs.at[b], **self.ax.to(dst)).start()

    def start(self):
        ax = self.ax
        for sem, d in ((0, 1), (1, -1)):

            @pl.when(jnp.logical_and(ax.o + d >= 0, ax.o + d < ax.outer))
            def _():
                self.send(self.src, ax.me, sem, ax.me + d * ax.inner)

        self.across(self.src, ax.me, 0)

    def across(self, src, b, k):
        ax = self.ax
        for q in range(1, ax.inner):
            sem = ax.outer + 1 + k * (ax.inner - 1) + q - 1
            self.send(src, b, sem, ax.o * ax.inner + lax.rem(ax.i + q, ax.inner))

    def onward(self, k):
        ax = self.ax
        return ax.o + jnp.where(ax.o > ax.near(k), 1, -1)

    def relay(self, k):
        ax = self.ax
        b = ax.blk(k, 0)
        self.wait(b)
        nxt = self.onward(k)

        @pl.when(jnp.logical_and(nxt >= 0, nxt < ax.outer))
        def _():
            self.send(self.at(b), b, 1 + k, nxt * ax.inner + ax.i)

        self.across(self.at(b), b, k)

    def wait(self, b):
        r = self.at(b)
        rcopy(r, r, self.ss.at[0], self.rs.at[b], **self.ax.to(self.ax.me)).wait_recv()

    def wait_across(self):
        for k in range(self.ax.outer):
            for q in range(1, self.ax.inner):
                self.wait(self.ax.blk(k, q))

    def drain(self):
        ax = self.ax

        def done(sem):
            rcopy(
                self.src, self.src, self.ss.at[sem], self.rs.at[0], **ax.to(ax.me)
            ).wait_send()

        for sem, d in ((0, 1), (1, -1)):

            @pl.when(jnp.logical_and(ax.o + d >= 0, ax.o + d < ax.outer))
            def _():
                done(sem)

        for k in range(1, ax.outer):
            nxt = self.onward(k)

            @pl.when(jnp.logical_and(nxt >= 0, nxt < ax.outer))
            def _():
                done(1 + k)

        for sem in range(ax.outer * (ax.inner - 1)):
            done(ax.outer + 1 + sem)


class Halves:
    def __init__(self, ax, src, buf, sems):
        n = src.shape[0] // 2
        self.parts = []
        for h in range(2):
            cut = pl.ds(n * h, n)
            self.parts.append(
                Gather(ax, src.at[cut], buf, (sems[0].at[h], sems[1].at[h]), cut)
            )

    def start(self):
        for g in self.parts:
            g.start()

    def relay(self, k, ends=None):
        for g in self.parts:
            if ends is None:
                g.relay(k)
                continue
            last = jnp.logical_or(g.ax.o == 0, g.ax.o == g.ax.outer - 1)

            @pl.when(last if ends else jnp.logical_not(last))
            def _():
                g.relay(k)

    def wait(self, b):
        for g in self.parts:
            g.wait(b)

    def drain(self):
        for g in self.parts:
            g.drain()


def gather_sems(outer, inner):
    sem = pltpu.SemaphoreType.DMA
    return sem((outer + 1 + outer * (inner - 1),)), sem((outer * inner,))


def pair(col, p):
    lane = lax.broadcasted_iota(jnp.int32, (col.shape[0], 128), 1)
    return jnp.where(lane < HEAD, col[:, 2 * p : 2 * p + 1], col[:, 2 * p + 1 : 2 * p + 2])


def spread(col, cp):
    return jnp.concatenate([pair(col, p) for p in range(cp // 128)], axis=1)


def row_sums(v):
    part = v[:, :128]
    for p in range(1, v.shape[1] // 128):
        part = part + v[:, 128 * p : 128 * p + 128]
    return jnp.sum(part.T, axis=0, keepdims=True)


def sigmoid(v):
    return 1.0 / (1.0 + jnp.exp(-v))


def softplus(v):
    return jnp.maximum(v, 0.0) + jnp.log1p(jnp.exp(-jnp.abs(v)))


def tri(shape, flip=False):
    i = lax.broadcasted_iota(jnp.int32, shape, 0)
    j = lax.broadcasted_iota(jnp.int32, shape, 1)
    return j >= i if flip else i >= j


def split(x2):
    lane = lax.broadcasted_iota(jnp.int32, x2.shape, 1)
    return jnp.concatenate([jnp.where(lane < HEAD, x2, 0), jnp.where(lane >= HEAD, x2, 0)], axis=0)


def chunk_inputs(c, ext, rawb, small, cp):
    r0 = pl.multiple_of(c * Q, Q)
    v = ext[pl.ds(r0, Q + 16), :].astype(f32)
    C = cp + 2 * N
    taps = [pltpu.roll(v, 3 - k, 0)[16:] if k < 3 else v[16:] for k in range(4)]
    summed = small[4:5, :C]
    for k in range(4):
        summed = summed + small[k : k + 1, :C] * taps[k]
    sig = sigmoid(summed)
    raw = rawb[pl.ds(r0, Q), :].astype(f32) + small[7:8, 0:128]
    dt = softplus(raw)
    rate = -jnp.exp(small[7:8, 128:256])
    cum = mm(tri((Q, Q)).astype(f32), dt * rate, precision=HI)
    return taps, summed, sig, raw, dt, rate, cum


def skip_row(small, cp):
    return spread(small[7:8, 256:384], cp)


def tight(cfg):
    S, F, T, D, cp, WC = cfg
    return S * T * D * 2 > 2**22


def lanes_from(row, shift, width, size):
    n = row.shape[1]
    if n < width:
        row = jnp.concatenate([row, jnp.zeros((row.shape[0], width - n), f32)], axis=1)
    row = pltpu.roll(row, lax.rem(shift + width, width), 1)
    return row[:, :size]


def small_rows(cfg, dims, flat, pc):
    S, F, T, D, cp, WC = cfg
    inner, heads, cols = dims
    conv = inner + 2 * N
    cl, gl, nl, hl = conv // F, inner // F, D // F, heads // F
    def line(v):
        v = v[...].astype(f32)
        v = v if v.ndim == 2 else v[None]
        n = -v.shape[1] % 128
        return jnp.concatenate([v, jnp.zeros((v.shape[0], n), f32)], axis=1) if n else v

    parts = [line(v) for v in flat]
    rows = jnp.concatenate(parts[:2] + [jnp.zeros((3, parts[0].shape[1]), f32)], axis=0)
    lane = lax.broadcasted_iota(jnp.int32, (8, cp), 1)
    xs = lanes_from(rows, cl * pc.f - cols * pc.s, conv, cp)
    bc = lanes_from(rows, cl * pc.f - inner, conv, 2 * N)
    gate = lanes_from(parts[2], gl * pc.f - cols * pc.s, inner, cp)
    if cols < cp:
        xs = jnp.where(lane < cols, xs, 0.0)
        gate = jnp.where(lane[0:1] < cols, gate, 0.0)
    norm = lanes_from(parts[3], nl * pc.f, D, D)
    hg = heads // S
    hv = jnp.concatenate(parts[4:7] + [jnp.zeros((5, 128), f32)], axis=0)
    hv = lanes_from(hv, hl * pc.f - hg * pc.s, 128, 128)
    hv = jnp.where(lane[:, :128] < hg, hv, 0.0)

    def wide(v):
        return jnp.concatenate([v, jnp.zeros((v.shape[0], D - v.shape[1]), f32)], axis=1)

    return jnp.concatenate(
        [
            wide(jnp.concatenate([xs, bc], axis=1)[0:5]),
            wide(gate),
            norm,
            wide(jnp.concatenate([hv[0:1], hv[1:2], hv[2:3]], axis=1)),
        ],
        axis=0,
    )


def body_fwd(cfg, dims, tok, cot, wsrc, wo, step, flat, R):
    S, F, T, D, cp, WC = cfg
    inner, heads, cols = dims
    L = S * T
    C = cp + 2 * N
    per = S // F
    pc = Place(S, F)
    own = R.w_all.at[pc.f]
    hg = heads // S
    up = -(-heads // 8) * 8
    st = step[...].astype(f32)
    if up > heads:
        st = jnp.concatenate([st, jnp.zeros((up - heads, st.shape[1]), f32)], axis=0)
    st = pltpu.roll(st, lax.rem(up - hg * pc.s, up), 0)[:8].T
    lane = lax.broadcasted_iota(jnp.int32, st.shape, 1)
    st = jnp.where(lane < hg, st, 0.0)
    st = jnp.concatenate([st, jnp.zeros((st.shape[0], 120), f32)], axis=1).astype(bf16)
    R.w_all[pc.f, :, 2 * cp + 2 * N :] = st
    if cols < cp:
        parts = [(wsrc[0], own.at[:, pl.ds(0, 2 * cp + 2 * N)])]
    else:
        (win,) = wsrc
        col = pl.multiple_of(pc.s * cols, cols)
        parts = [
            (win.at[:, pl.ds(col, cols)], own.at[:, pl.ds(0, cols)]),
            (win.at[:, pl.ds(inner + col, cols)], own.at[:, pl.ds(cols, cols)]),
            (win.at[:, pl.ds(2 * inner, 2 * N)], own.at[:, pl.ds(2 * cols, 2 * N)]),
        ]
    parts = [pltpu.make_async_copy(a, b, R.wsem.at[i]) for i, (a, b) in enumerate(parts)]
    for c in parts:
        c.start()
    R.sm_own[...] = small_rows(cfg, dims, flat, pc)
    pc.barrier()
    tg = Halves(pc.seq, tok, R.tok_all, (R.ss_t, R.rs_t))
    cg = Halves(pc.seq, cot, R.cot_all, (R.ss_c, R.rs_c))
    wg = Gather(pc.fsdp, own, R.w_all, (R.ss_w, R.rs_w))
    first = lax.rem(pc.s, per)
    owner = pc.s // per
    wogs = []
    if not tight(cfg):
        for p in range(per):
            at = lax.rem(first + p, per)
            wogs.append(
                Gather(pc.fsdp, wo.at[at], R.w_out.at[at], (R.ss_o.at[p], R.rs_o.at[p]))
            )
    sm = R.sm_own
    tg.start()
    for k in range(1, F):
        to = lax.rem(pc.f + k, F)
        rcopy(sm, R.sm_all.at[pc.f], R.ss_m.at[k], R.rs_m.at[pc.f], fsdp=to).start()
    for c in parts:
        c.wait()
    wg.start()
    keep = []
    for p in range(len(wogs)):
        wogs[p].start()
        at = lax.rem(first + p, per)
        keep.append(pltpu.make_async_copy(wo.at[at], R.w_out.at[at, pc.f], R.osem.at[p]))
    if tight(cfg):
        keep.append(pltpu.make_async_copy(wo, R.wo_g, R.osem.at[0]))

        @pl.when(pc.f == owner)
        def _():
            keep[0].start()
            for k in range(1, F):
                to = lax.rem(pc.f + k, F)
                rcopy(wo, R.wo_g, R.ss_o.at[k], R.rs_o.at[0], fsdp=to).start()
    else:
        for c in keep:
            c.start()
    R.tok_all[pc.s] = tok[...]
    R.cot_all[pc.s] = cot[...]
    R.sm_all[pc.f] = sm[...]
    R.ext[0:16, :] = jnp.zeros((16, C), bf16)
    for k in range(1, F):
        o = lax.rem(pc.f + k, F)
        rcopy(sm, R.sm_all.at[o], R.ss_m.at[0], R.rs_m.at[o], fsdp=pc.f).wait_recv()
    total = R.sm_all[0]
    for k in range(1, F):
        total = total + R.sm_all[k]
    R.small[...] = total
    small = R.small
    tg.relay(1)
    tg.relay(2)
    tg.relay(3, False)
    for k in range(1, F // 2):
        wg.relay(k)
    tg.relay(3, True)
    cg.start()
    wg.wait_across()

    def project(j, carry):
        k, q = j // pc.X, lax.rem(j, pc.X)
        b = pc.blk(k, q)

        @pl.when(q > 0)
        def _():
            tg.wait(b)

        @pl.when(j == S // 2)
        def _():
            cg.relay(1)

        r = R.tok_all[b].astype(f32)
        scale = lax.rsqrt(jnp.mean(r * r, axis=1, keepdims=True) + epsilon)
        h = r * scale * small[6:7, :]
        r0 = pl.multiple_of(b * T, T)
        R.hid_t[:, pl.ds(r0, T)] = h.T.astype(bf16)
        out = mm(h.astype(bf16), R.w_all[...].reshape(D, WC)).astype(bf16)
        R.zb[pl.ds(r0, T), :] = out[:, :cp]
        R.rawb[pl.ds(r0, T), :] = out[:, 2 * cp + 2 * N :]
        R.ext[pl.ds(r0 + 16, T), :] = out[:, cp : 2 * cp + 2 * N]
        return carry

    lax.fori_loop(0, S, project, 0)
    R.state[...] = jnp.zeros((N, cp), f32)

    def forward(c, carry):
        @pl.when(jnp.logical_or(c == 0, c == 5))
        def _():
            cg.relay(2 + c // 5)

        r0 = pl.multiple_of(c * Q, Q)
        taps, summed, sig, raw, dt, rate, cum = chunk_inputs(c, R.ext, R.rawb, small, cp)
        act = summed * sig
        x = act[:, :cp]
        bb = act[:, cp : cp + N].astype(bf16)
        cb = act[:, cp + N :].astype(bf16)
        cum_t = cum.T
        dt_t = dt.T
        scores = mm(cb, bb, 1, 1)
        causal = tri((Q, Q))
        parts = []
        for p in range(cp // 128):
            mix = []
            for h in (2 * p, 2 * p + 1):
                gap = jnp.where(causal, cum[:, h : h + 1] - cum_t[h : h + 1, :], -1e30)
                mix.append((jnp.exp(gap) * scores * dt_t[h : h + 1, :]).astype(bf16))
            parts.append(
                mm(jnp.concatenate(mix, axis=1), split(x[:, 128 * p : 128 * p + 128]).astype(bf16))
            )
        state = R.state[...]
        R.states[c] = state
        last = cum[Q - 1 : Q, :]
        y = jnp.concatenate(parts, axis=1) + mm(cb, state.astype(bf16)) * spread(jnp.exp(cum), cp)
        y = y + skip_row(small, cp) * x
        wx = (spread(jnp.exp(last - cum) * dt, cp) * x).astype(bf16)
        R.state[...] = spread(jnp.exp(last), cp) * state + mm(bb, wx, 0, 0)
        R.y[pl.ds(r0, Q), :] = y
        z = R.zb[pl.ds(r0, Q), :].astype(f32)
        gated = (y * (z * sigmoid(z))).astype(bf16)
        R.dpx[pl.ds(r0, Q), :cp] = gated
        g32 = gated.astype(f32)
        R.st[0:1, pl.ds(r0, Q)] = row_sums(g32 * g32)
        return carry

    lax.fori_loop(0, L // Q, forward, 0)

    if tight(cfg):
        group = R.wo_g

        @pl.when(pc.f != owner)
        def _():
            rcopy(wo, R.wo_g, R.ss_o.at[0], R.rs_o.at[0], fsdp=pc.f).wait_recv()

        @pl.when(pc.f == owner)
        def _():
            keep[0].wait()
    else:
        group = R.w_out.at[first, owner]
        for c in keep:
            c.wait()
        for k in range(1, F // 2):
            wogs[0].relay(k)
        wogs[0].wait_across()

    def mixed(j, carry):
        k, q = j // pc.X, lax.rem(j, pc.X)
        b = pc.blk(k, q)

        @pl.when(q > 0)
        def _():
            cg.wait(b)

        r0 = pl.multiple_of(b * T, T)
        mg = mm(R.cot_all[b], group[...], 1, 1)
        R.mg[pl.ds(r0, T), :] = mg
        g = mg * small[5:6, :cp] * R.dpx[pl.ds(r0, T), :cp].astype(f32)
        R.st[1:2, pl.ds(r0, T)] = row_sums(g)
        return carry

    lax.fori_loop(0, S, mixed, 0)
    for k in range(1, S):
        rcopy(
            R.st, R.st_all.at[pc.s], R.ss_s.at[k], R.rs_s.at[pc.s],
            seq=lax.rem(pc.s + k, S),
        ).start()
    R.st_all[pc.s] = R.st[...]
    for k in range(1, S):
        o = lax.rem(pc.s + k, S)
        rcopy(R.st, R.st_all.at[o], R.ss_s.at[0], R.rs_s.at[o], seq=pc.s).wait_recv()
    total = R.st_all[0]
    for k in range(1, S):
        total = total + R.st_all[k]
    R.stats[...] = total

    for g in [tg, cg, wg]:
        g.drain()
    for k in range(1, S):
        rcopy(R.st, R.st, R.ss_s.at[k], R.rs_s.at[0], seq=pc.s).wait_send()
    for k in range(1, F):
        rcopy(sm, sm, R.ss_m.at[k], R.rs_m.at[0], fsdp=pc.f).wait_send()
    if tight(cfg):

        @pl.when(pc.f == owner)
        def _():
            for k in range(1, F):
                rcopy(wo, wo, R.ss_o.at[k], R.rs_o.at[0], fsdp=pc.f).wait_send()

    return wogs


def fwd_scratch(cfg):
    S, F, T, D, cp, WC = cfg
    L = S * T
    Dl = D // F
    C = cp + 2 * N
    V = pltpu.VMEM
    sem = pltpu.SemaphoreType.DMA
    per = S // F
    seq = gather_sems(4, S // 4)
    fsdp = gather_sems(F // 2, 2)
    out = SimpleNamespace(
        tok_all=V((S, T, D), bf16),
        cot_all=V((S, T, D), bf16),
        w_all=V((F, Dl, WC), bf16),
        sm_own=V((8, D), f32),
        sm_all=V((F, 8, D), f32),
        small=V((8, D), f32),
        hid_t=V((D, L), bf16),
        zb=V((L, cp), bf16),
        rawb=V((L, 128), bf16),
        ext=V((16 + L, C), bf16),
        state=V((N, cp), f32),
        states=V((L // Q, N, cp), f32),
        y=V((L, cp), f32),
        mg=V((L, cp), f32),
        st=V((2, L), f32),
        st_all=V((S, 2, L), f32),
        stats=V((2, L), f32),
        ss_t=sem((2,) + seq[0].shape),
        rs_t=sem((2,) + seq[1].shape),
        ss_c=sem((2,) + seq[0].shape),
        rs_c=sem((2,) + seq[1].shape),
        ss_w=fsdp[0],
        rs_w=fsdp[1],
        ss_m=sem((F,)),
        rs_m=sem((F,)),
        wsem=sem((4,)),
        osem=sem((per,)),
        ss_s=sem((S,)),
        rs_s=sem((S,)),
    )
    if tight(cfg):
        out.wo_g = V((cp, D), bf16)
        out.ss_o = out.rs_o = sem((F,))
    else:
        out.w_out = V((per, F, cp, D), bf16)
        out.ss_o = sem((per,) + fsdp[0].shape)
        out.rs_o = sem((per,) + fsdp[1].shape)
    return out


class Scatter:
    def __init__(self, pc, part, rx, rz, rn, sems):
        self.pc, self.part, self.rx, self.rz, self.rn = pc, part, rx, rz, rn
        self.ssx, self.rsx, self.ssz, self.rsz, self.rsn = sems
        self.near = jnp.logical_or(pc.z == 1, pc.z == 2)

    @staticmethod
    def sems(S):
        sem = pltpu.SemaphoreType.DMA
        return sem((S,)), sem((4, S // 4 - 1)), sem((4,)), sem((2,)), sem((2,))

    def got(self, ref, sem):
        rcopy(ref, ref, sem, sem, seq=self.pc.s).wait_recv()

    def across(self, b):
        pc = self.pc
        zb, xb = b // pc.X, lax.rem(b, pc.X)

        @pl.when(xb != pc.x)
        def _():
            slot = lax.rem(pc.x - xb - 1 + pc.X, pc.X)
            rcopy(
                self.part.at[b], self.rx.at[zb, slot], self.ssx.at[b], self.rsx.at[zb, slot],
                seq=pc.z * pc.X + xb,
            ).start()

    def other(self, zb):
        return zb // 2 != self.pc.z // 2

    def column(self, zb):
        pc = self.pc
        b = zb * pc.X + pc.x
        total = self.part[b].astype(f32)
        for q in range(pc.X - 1):
            self.got(self.rx.at[zb, q], self.rsx.at[zb, q])
            total = total + self.rx[zb, q].astype(f32)
        self.part[b] = total.astype(bf16)

        @pl.when(jnp.logical_and(zb != pc.z, jnp.logical_not(self.other(zb))))
        def _():
            rcopy(
                self.part.at[b], self.rz.at[0], self.ssz.at[zb], self.rsz.at[0], seq=b
            ).start()

        @pl.when(jnp.logical_and(self.other(zb), jnp.logical_not(self.near)))
        def _():
            slot = lax.rem(zb, 2)
            rcopy(
                self.part.at[b], self.rn.at[slot], self.ssz.at[zb], self.rsn.at[slot],
                seq=(pc.z + 1 - 2 * lax.rem(pc.z, 2)) * pc.X + pc.x,
            ).start()

    def merge(self, zb):
        pc = self.pc

        @pl.when(jnp.logical_and(self.other(zb), self.near))
        def _():
            b = zb * pc.X + pc.x
            slot = lax.rem(zb, 2)
            self.got(self.rn.at[slot], self.rsn.at[slot])
            total = self.part[b].astype(f32) + self.rn[slot].astype(f32)
            self.part[b] = total.astype(bf16)
            rcopy(
                self.part.at[b], self.rz.at[1], self.ssz.at[zb], self.rsz.at[1], seq=b
            ).start()

    def total(self):
        out = self.part[self.pc.s].astype(f32)
        for q in range(2):
            self.got(self.rz.at[q], self.rsz.at[q])
            out = out + self.rz[q].astype(f32)
        return out

    def drain(self):
        pc = self.pc
        r = self.rz.at[0]
        for b in range(pc.S):

            @pl.when(b % pc.X != pc.x)
            def _():
                rcopy(r, r, self.ssx.at[b], self.rsz.at[0], seq=pc.s).wait_send()

        for zb in range(pc.Z):

            @pl.when(zb != pc.z)
            def _():
                rcopy(r, r, self.ssz.at[zb], self.rsz.at[0], seq=pc.s).wait_send()


class Shared:
    def __init__(self, pc, part, recv, ss, rs):
        self.pc, self.part, self.recv, self.ss, self.rs = pc, part, recv, ss, rs

    def send(self, k):
        pc = self.pc
        to = lax.rem(pc.f + k, pc.F)
        rcopy(
            self.part.at[to], self.recv.at[k - 1], self.ss.at[k - 1], self.rs.at[k - 1], fsdp=to
        ).start()

    def total(self):
        pc = self.pc
        out = self.part[pc.f].astype(f32)
        for k in range(1, pc.F):
            r = self.recv.at[k - 1]
            rcopy(r, r, self.ss.at[k - 1], self.rs.at[k - 1], fsdp=pc.f).wait_recv()
            out = out + self.recv[k - 1].astype(f32)
        return out

    def drain(self):
        for k in range(1, self.pc.F):
            r = self.recv.at[k - 1]
            rcopy(r, r, self.ss.at[k - 1], self.rs.at[k - 1], fsdp=self.pc.f).wait_send()


def body_bwd(cfg, dims, tok, cot, wogs, R, O):
    S, F, T, D, cp, WC = cfg
    inner = float(dims[0])
    L = S * T
    C = cp + 2 * N
    Dl = D // F
    nc = L // Q
    cr = cp // F
    per = S // F
    bh = Dl // S
    pc = Place(S, F)
    small = R.small
    if tight(cfg):
        blk = Scatter(pc, R.bp, R.brx, R.brz, R.brn, (R.bs0, R.bs1, R.bs2, R.bs3, R.bs4))
    hid = Scatter(pc, R.tok_all, R.hrx, R.hrz, R.hrn, (R.hs0, R.hs1, R.hs2, R.hs3, R.hs4))
    zs = Shared(pc, R.zp, R.zr, R.zs0, R.zs1)
    os_ = Shared(pc, R.op, R.orecv, R.os0, R.os1)
    nt = cp // 128

    def xs(t):
        return Shared(pc, R.xp.at[t], R.xr.at[t], R.xs0.at[t], R.xs1.at[t])

    def xg(t):
        return Gather(pc.seq, R.xred.at[t], O.gx.at[t], (R.gx0.at[t], R.gx1.at[t]))

    def own_x(t):
        return pltpu.make_async_copy(R.xred.at[t], O.gx.at[t, pc.s], R.xsem.at[t])

    def settle(t):
        R.xred[t] = xs(t).total().astype(bf16)
        xg(t).start()
        own_x(t).start()
    bs = Shared(pc, R.cp_, R.cr_, R.cs0, R.cs1)
    zg = Gather(pc.seq, R.zred, O.gz, (R.gz0, R.gz1))
    og = Gather(pc.seq, R.ored, O.go_s, (R.go0, R.go1))
    sg = Gather(pc.seq, R.asum, O.sm, (R.as2, R.as3))

    def direct(src, dst, ss, rs, to):
        rcopy(src, dst.at[pc.s], ss.at[to], rs.at[pc.s], seq=to).start()

    def arrived(dst, ss, rs):
        for k in range(1, S):
            o = lax.rem(pc.s + k, S)
            r = dst.at[o]
            rcopy(r, r, ss.at[0], rs.at[o], seq=pc.s).wait_recv()

    def sent(src, ss, rs):
        for k in range(1, S):
            rcopy(src, src, ss.at[lax.rem(pc.s + k, S)], rs.at[0], seq=pc.s).wait_send()

    def own(src, dst, i):
        return pltpu.make_async_copy(src, dst, R.lsem.at[i])

    gate = small[5:6, :cp]
    R.acc[...] = jnp.zeros((16, D), f32)
    R.hacc[...] = jnp.zeros((2, 8, 128), f32)
    R.dstate[...] = jnp.zeros((N, cp), f32)
    R.head[...] = jnp.zeros((8, C), f32)

    def first(i, carry):
        c = lax.rem(pc.s + 1 + i, nc)
        r0 = pl.multiple_of(c * Q, Q)
        rows = pl.ds(r0, Q)
        st = jnp.concatenate([R.stats[:, rows], jnp.zeros((6, Q), f32)], axis=0).T
        scale = lax.rsqrt(st[:, 0:1] / inner + epsilon)
        mean = st[:, 1:2] / inner
        gated = R.dpx[rows, :cp].astype(f32)
        mg = R.mg[rows, :]
        ng = gated * scale
        mn = ng * gate
        R.acc[5:6, :cp] += jnp.sum(mg * ng, axis=0, keepdims=True)
        gg = (scale * (mg * gate) - scale * scale * scale * gated * mean).astype(bf16).astype(f32)
        z = R.zb[rows, :].astype(f32)
        sz = sigmoid(z)
        R.zb[rows, :] = (gg * R.y[rows, :] * (sz * (1.0 + z * (1.0 - sz)))).astype(bf16)
        R.mg[rows, :] = gg * (z * sz)
        R.mn_t[:, rows] = mn.T.astype(bf16)
        if tight(cfg):
            R.dpx[rows, :cp] = mn.astype(bf16)
        else:
            R.mn[c] = mn.astype(bf16)

            @pl.when(c != pc.s)
            def _():
                direct(R.mn.at[c], R.mall, R.ms0, R.ms1, c)

        return carry

    def block(i, carry):
        c = nc - 1 - i
        rows = pl.ds(pl.multiple_of(c * Q, Q), Q)
        R.bp[c] = mm(R.dpx[rows, :cp], R.wo_g[...]).astype(bf16)
        blk.across(c)
        return carry

    lax.fori_loop(0, nc, first, 0)

    def zpart(k, carry):
        to = lax.rem(pc.f + k, F)
        rows = pl.ds(pl.multiple_of(to * Dl, Dl), Dl)
        R.zp[to] = mm(R.hid_t[rows, :], R.zb[...]).astype(bf16)

        @pl.when(k < F)
        def _():
            rcopy(
                R.zp.at[to], R.zr.at[k - 1], R.zs0.at[k - 1], R.zs1.at[k - 1], fsdp=to
            ).start()
        return carry

    lax.fori_loop(1, F + 1, zpart, 0)
    W = 384

    def opart(j, carry):
        cols = pl.ds(pl.multiple_of(j * W, W), W)
        a = R.cot_all[:, :, cols].reshape(L, W)
        R.op[:, :, cols] = mm(R.mn_t[...], a).reshape(F, cr, W).astype(bf16)
        return carry

    lax.fori_loop(0, D // W, opart, 0)
    for g in wogs[1:]:
        for k in range(1, F // 2):
            g.relay(k)
    for k in range(1, F):
        os_.send(k)
    if tight(cfg):
        lax.fori_loop(0, nc, block, 0)

    sel = (
        lax.broadcasted_iota(jnp.int32, (8, cp), 1) // HEAD
        == lax.broadcasted_iota(jnp.int32, (8, cp), 0)
    ).astype(f32)
    sub = lax.broadcasted_iota(jnp.int32, (8, Q), 0)

    def scan(i, carry):
        c = nc - 1 - i
        r0 = pl.multiple_of(c * Q, Q)
        rows = pl.ds(r0, Q)

        if tight(cfg):

            @pl.when(i < pc.Z)
            def _():
                blk.column(pc.Z - 1 - i)

            @pl.when(jnp.logical_and(i >= pc.Z, i < 2 * pc.Z))
            def _():
                blk.merge(2 * pc.Z - 1 - i)

        @pl.when(i == 1)
        def _():
            R.zred[...] = zs.total().astype(bf16)
            zg.start()
            own(R.zred, O.gz.at[pc.s], 0).start()

        @pl.when(i == 4)
        def _():
            R.ored[...] = os_.total().astype(bf16)
            og.start()
            own(R.ored, O.go_s.at[pc.s], 5).start()

        @pl.when(jnp.logical_and(i >= 4, i < 4 + pc.Z - 1))
        def _():
            zg.relay(i - 3)

        @pl.when(i == 7)
        def _():
            og.relay(1)

        taps, summed, sig, raw, dt, rate, cum = chunk_inputs(c, R.ext, R.rawb, small, cp)
        act = summed * sig
        x = act[:, :cp]
        xb = x.astype(bf16)
        bb = act[:, cp : cp + N].astype(bf16)
        cb = act[:, cp + N :].astype(bf16)
        cum_t = cum.T
        dt_t = dt.T
        dy = R.mg[rows, :]
        dyb = dy.astype(bf16)
        last = cum[Q - 1 : Q, :]
        edy = spread(jnp.exp(cum), cp) * dy
        edyb = edy.astype(bf16)
        wdec = jnp.exp(last - cum)
        w = wdec * dt
        state = R.states[c]
        sb = state.astype(bf16)
        ds = R.dstate[...]
        dsb = ds.astype(bf16)
        ws = spread(w, cp)
        v = mm(bb, dsb)
        carr = mm(sel, edy * mm(cb, sb), 1, 1, HI)
        dw = mm(sel, x * v, 1, 1, HI)
        db = mm((ws * x).astype(bf16), dsb, 1, 1)
        dc = mm(edyb, sb, 1, 1)
        dlast = mm(sel, jnp.sum(state * ds, axis=0, keepdims=True), 1, 1, HI)
        R.dstate[...] = spread(jnp.exp(last), cp) * ds + mm(cb, edyb, 0, 0)
        scores = mm(bb, cb, 1, 1)
        seen = tri((Q, Q), True)
        dtb = dt_t[0:8].astype(bf16)
        dsc = jnp.zeros((Q, Q), f32)
        direct = jnp.zeros((8, Q), f32)
        onto = jnp.zeros((8, Q), f32)
        parts = []
        for p in range(cp // 128):
            cols = slice(128 * p, 128 * p + 128)
            g2 = mm(split(x[:, cols]).astype(bf16), dyb[:, cols], 1, 1)
            mix = []
            for h in (2 * p, 2 * p + 1):
                g = g2[:Q] if h % 2 == 0 else g2[Q:]
                decay = jnp.exp(jnp.where(seen, cum_t[h : h + 1, :] - cum[:, h : h + 1], -1e30))
                ls = decay * scores
                mix.append((ls * dt[:, h : h + 1]).astype(bf16))
                e = (g * ls).astype(bf16)
                dsc = dsc + g * decay * dt[:, h : h + 1]
                direct = direct + mm(jnp.where(sub == h, 1.0, 0.0).astype(bf16), e, 1, 1)
                onto = onto + mm(jnp.where(sub == h, dtb.astype(f32), 0.0).astype(bf16), e)
            parts.append(mm(jnp.concatenate(mix, axis=1), split(dy[:, cols]).astype(bf16)))
        dscb = dsc.astype(bf16)
        db = db + mm(dscb, cb)
        dc = dc + mm(dscb, bb, 0, 0)
        dx = skip_row(small, cp) * dy + ws * v + jnp.concatenate(parts, axis=1)
        R.acc[7:8, :cp] += jnp.sum(dy * x, axis=0, keepdims=True)
        dt_r = dt_t[0:8]
        wdec_r = wdec.T[0:8]
        w_r = wdec_r * dt_r
        rate_r = jnp.broadcast_to(rate, (128, 128)).T[0:8, 0:1]
        last_r = jnp.exp(cum_t[0:8, Q - 1 : Q])
        dcum = carr + onto - dtb.astype(f32) * direct - w_r * dw
        end = jnp.sum(w_r * dw, axis=1, keepdims=True) + last_r * dlast
        da = mm(dcum, tri((Q, Q)).astype(f32), precision=HI) + end
        ddt = direct + wdec_r * dw + rate_r * da
        draw = ddt * sigmoid(raw).T[0:8]
        R.hacc[0] += draw
        R.hacc[1] += da * dt_r * rate_r
        dact = jnp.concatenate([dx, db, dc], axis=1)
        dsum = dact * (sig * (1.0 + summed * (1.0 - sig)))
        full = jnp.concatenate([dsum, R.head[...]], axis=0)
        dxbc = jnp.zeros((Q, C), f32)
        for k in range(4):
            R.acc[k : k + 1, :C] += jnp.sum(dsum * taps[k], axis=0, keepdims=True)
            moved = pltpu.roll(full, Q + 8 - (3 - k), 0)[:Q] if k < 3 else dsum
            dxbc = dxbc + small[k : k + 1, :C] * moved
        R.acc[4:5, :C] += jnp.sum(dsum, axis=0, keepdims=True)
        R.head[...] = dsum[:8]
        R.dpx[rows, :C] = dxbc.astype(bf16)
        R.acc[8:16, :] += mm(draw.astype(bf16), R.hid_t[:, rows], 1, 1)
        pad = jnp.concatenate([draw, jnp.zeros((120, Q), f32)], axis=0).T
        R.dpx[rows, C:] = pad.astype(bf16)
        grad = jnp.concatenate([R.zb[rows, :], R.dpx[rows, :]], axis=1)
        hp = mm(grad, R.w_all[...].reshape(D, WC), 1, 1)
        r = R.tok_all[c].astype(f32)
        scale = lax.rsqrt(jnp.mean(r * r, axis=1, keepdims=True) + epsilon)
        R.acc[6:7, :] += jnp.sum(hp * r * scale, axis=0, keepdims=True)
        R.tok_all[c] = hp.astype(bf16)
        hid.across(c)
        return carry

    lax.fori_loop(0, nc, scan, 0)

    diag = lax.broadcasted_iota(jnp.int32, (8, 128), 0) == lax.broadcasted_iota(
        jnp.int32, (8, 128), 1
    )

    def along(v):
        return jnp.sum(jnp.where(diag, jnp.sum(v, axis=1, keepdims=True), 0.0), axis=0, keepdims=True)

    dskip = jnp.sum(
        jnp.where(diag, mm(sel, R.acc[7:8, :cp], 1, 1, HI), 0.0), axis=0, keepdims=True
    )
    R.acc[7:8, :] = jnp.concatenate(
        [along(R.hacc[0]), along(R.hacc[1]), dskip, jnp.zeros((1, D - 384), f32)], axis=1
    )
    R.accb[...] = R.acc[...].astype(bf16)
    for k in range(1, F):
        to = lax.rem(pc.f + k, F)
        rcopy(
            R.accb, R.ar.at[k - 1], R.as0.at[k - 1], R.as1.at[k - 1], fsdp=to
        ).start()

    for t in range(nt):

        def xpart(k, carry):
            to = lax.rem(pc.f + k, F)
            rows = pl.ds(pl.multiple_of(to * Dl, Dl), Dl)
            R.xp[t, to] = mm(R.hid_t[rows, :], R.dpx[:, 128 * t : 128 * t + 128]).astype(bf16)

            @pl.when(k < F)
            def _():
                rcopy(
                    R.xp.at[t, to], R.xr.at[t, k - 1], R.xs0.at[t, k - 1], R.xs1.at[t, k - 1],
                    fsdp=to,
                ).start()
            return carry

        lax.fori_loop(1, F + 1, xpart, 0)

    def lower(k, carry):
        to = lax.rem(pc.f + k, F)
        rows = pl.ds(pl.multiple_of(to * Dl, Dl), Dl)
        R.cp_[to] = mm(R.hid_t[rows, :], R.dpx[:, cp:C]).astype(bf16)

        @pl.when(k < F)
        def _():
            rcopy(
                R.cp_.at[to], R.cr_.at[k - 1], R.cs0.at[k - 1], R.cs1.at[k - 1], fsdp=to
            ).start()
        return carry

    lax.fori_loop(1, F + 1, lower, 0)
    def hid_column(i, carry):
        hid.column(pc.Z - 1 - i)
        return carry

    total = R.acc[...]
    for k in range(1, F):
        r = R.ar.at[k - 1]
        rcopy(r, r, R.as0.at[k - 1], R.as1.at[k - 1], fsdp=pc.f).wait_recv()
        total = total + R.ar[k - 1].astype(f32)
    R.asum[...] = total.astype(bf16)
    sg.start()
    own(R.asum, O.sm.at[pc.s], 1).start()
    og.relay(2)
    settle(0)
    og.relay(3)
    for t in range(1, nt):
        settle(t)
    low = bs.total()
    for g in range(S):
        R.cb[g] = low[g * bh : (g + 1) * bh].astype(bf16)
    for k in range(1, S):
        to = lax.rem(pc.s + k, S)
        direct(R.cb.at[to], R.cbr, R.cb0, R.cb1, to)
    lax.fori_loop(0, 2, hid_column, 0)
    sg.relay(1)
    for t in range(nt):
        xg(t).relay(1)
    lax.fori_loop(2, pc.Z, hid_column, 0)
    for zb in (3, 2):
        hid.merge(zb)
    sg.relay(2)
    for t in range(nt):
        xg(t).relay(2)
    arrived(R.cbr, R.cb0, R.cb1)
    R.cbr[pc.s] = R.cb[pc.s]
    low = R.cbr[0].astype(f32)
    for g in range(1, S):
        low = low + R.cbr[g].astype(f32)
    R.cbd[...] = low.astype(bf16)
    for k in range(1, S):
        direct(R.cbd, O.gbc, R.cd0, R.cd1, lax.rem(pc.s + k, S))
    own(R.cbd, O.gbc.at[pc.s], 4).start()
    own(R.ored, O.go_s.at[pc.s], 5).wait()
    og.wait_across()
    for k in range(1, F):
        to = lax.rem(pc.f + k, F)
        rcopy(
            O.go_s.at[pl.ds(to * per, per)], O.go.at[pc.f], R.gs0.at[k], R.gs1.at[pc.f],
            fsdp=to,
        ).start()
    own(O.go_s.at[pl.ds(pc.f * per, per)], O.go.at[pc.f], 3).start()
    sg.relay(3)
    for t in range(nt):
        xg(t).relay(3)
    for zb in (1, 0):
        hid.merge(zb)

    mine = tok[...].astype(f32)
    if tight(cfg):
        O.block[...] = (mine + blk.total()).astype(bf16)
    else:
        for g in wogs[1:]:
            g.wait_across()
        arrived(R.mall, R.ms0, R.ms1)
        R.mall[pc.s] = R.mn[pc.s]
        R.total[...] = mine

        def add(g, carry):
            w = R.w_out[lax.rem(g, per), g // per]
            R.total[...] += mm(R.mall[g], w)
            return carry

        lax.fori_loop(0, S, add, 0)
        O.block[...] = R.total[...].astype(bf16)
    scale = lax.rsqrt(jnp.mean(mine * mine, axis=1, keepdims=True) + epsilon)
    e = hid.total() * small[6:7, :]
    mean = jnp.mean(e * mine, axis=1, keepdims=True)
    O.input[...] = cot[...].astype(f32) + scale * e - scale * scale * scale * mine * mean

    zg.wait_across()
    for k in range(1, F):
        o = lax.rem(pc.f + k, F)
        r = O.go.at[o]
        rcopy(r, r, R.gs0.at[0], R.gs1.at[o], fsdp=pc.f).wait_recv()
    arrived(O.gbc, R.cd0, R.cd1)
    sg.wait_across()
    for t in range(nt):
        xg(t).wait_across()
        own_x(t).wait()
    own(R.zred, O.gz.at[pc.s], 0).wait()
    own(R.asum, O.sm.at[pc.s], 1).wait()
    own(O.go_s.at[pl.ds(pc.f * per, per)], O.go.at[pc.f], 3).wait()
    own(R.cbd, O.gbc.at[pc.s], 4).wait()
    if tight(cfg):
        blk.drain()
    else:
        sent(R.mn.at[0], R.ms0, R.ms1)
    sent(R.cb.at[0], R.cb0, R.cb1)
    sent(R.cbd, R.cd0, R.cd1)
    for a in [hid, zs, os_, bs, zg, og, sg] + wogs:
        a.drain()
    for t in range(nt):
        xs(t).drain()
        xg(t).drain()
    for k in range(1, F):
        r = R.ar.at[k - 1]
        rcopy(r, r, R.as0.at[k - 1], R.as1.at[0], fsdp=pc.f).wait_send()
        r = O.go.at[0]
        rcopy(r, r, R.gs0.at[k], R.gs1.at[0], fsdp=pc.f).wait_send()


def bwd_scratch(cfg):
    S, F, T, D, cp, WC = cfg
    L = S * T
    Dl = D // F
    C = cp + 2 * N
    Z, X = 4, S // 4
    cr = cp // F
    bh = Dl // S
    V = pltpu.VMEM
    sem = pltpu.SemaphoreType.DMA
    seq = gather_sems(4, S // 4)
    nt = cp // 128
    out = SimpleNamespace(
        acc=V((16, D), f32),
        asum=V((16, D), bf16),
        accb=V((16, D), bf16),
        ar=V((F - 1, 16, D), bf16),
        hacc=V((2, 8, 128), f32),
        dstate=V((N, cp), f32),
        head=V((8, C), f32),
        mn_t=V((cp, L), bf16),
        dpx=V((L, WC - cp), bf16),
        hrx=V((Z, X - 1, T, D), bf16),
        hrz=V((2, T, D), bf16),
        hrn=V((2, T, D), bf16),
        zp=V((F, Dl, cp), bf16),
        zr=V((F - 1, Dl, cp), bf16),
        zred=V((Dl, cp), bf16),
        op=V((F, cr, D), bf16),
        orecv=V((F - 1, cr, D), bf16),
        ored=V((cr, D), bf16),
        xp=V((nt, F, Dl, 128), bf16),
        xr=V((nt, F - 1, Dl, 128), bf16),
        xred=V((nt, Dl, 128), bf16),
        cp_=V((F, Dl, 2 * N), bf16),
        cr_=V((F - 1, Dl, 2 * N), bf16),
        cb=V((S, bh, 2 * N), bf16),
        cbr=V((S, bh, 2 * N), bf16),
        cbd=V((bh, 2 * N), bf16),
        lsem=sem((6,)),
        as0=sem((F,)), as1=sem((F,)), as2=seq[0], as3=seq[1],
        gs0=sem((F,)), gs1=sem((F,)), cs0=sem((F,)), cs1=sem((F,)),
        cb0=sem((S,)), cb1=sem((S,)), cd0=sem((S,)), cd1=sem((S,)),
        zs0=sem((F,)), zs1=sem((F,)), gz0=seq[0], gz1=seq[1],
        os0=sem((F,)), os1=sem((F,)), go0=seq[0], go1=seq[1],
        xs0=sem((nt, F)), xs1=sem((nt, F)), xsem=sem((nt,)),
        gx0=sem((nt,) + seq[0].shape), gx1=sem((nt,) + seq[1].shape),
    )
    out.hs0, out.hs1, out.hs2, out.hs3, out.hs4 = Scatter.sems(S)
    if tight(cfg):
        out.brx = V((Z, X - 1, T, D), bf16)
        out.brz = V((2, T, D), bf16)
        out.brn = V((2, T, D), bf16)
        out.bs0, out.bs1, out.bs2, out.bs3, out.bs4 = Scatter.sems(S)
    else:
        out.mn = V((S, T, cp), bf16)
        out.mall = V((S, T, cp), bf16)
        out.total = V((T, D), f32)
        out.ms0 = out.ms1 = sem((S,))
    return out


def assemble(cfg, dims, gz, gx, gbc, go, sm, win, step, conv, bias, gate, norm, h0, h1, h2, wout):
    S, F, T, D, cp, WC = cfg
    inner, nheads, cols = dims
    for g in range(S):
        win[:, g * cols : (g + 1) * cols] = gz[g, :, :cols].astype(f32)
        for t in range(gx.shape[0]):
            n = min(128, cols - 128 * t)
            at = inner + g * cols + 128 * t
            win[:, at : at + n] = gx[t, g, :, :n].astype(f32)
    wout[...] = go[0, 0].astype(f32)
    C = cp + 2 * N
    hg = nheads // S
    Dl = D // F
    win[:, 2 * inner :] = gbc[...].astype(f32)

    @pl.when(pl.program_id(0) == 0)
    def _():
        f = lax.axis_index("fsdp")

        def mine(v, size):
            n = v.shape[1]
            return pltpu.roll(v, lax.rem(n - size * f, n), 1)[:, :size]

        v = [sm[g].astype(f32) for g in range(S)]
        total = v[0]
        for g in range(1, S):
            total = total + v[g]
        xs = jnp.concatenate([a[0:8, :cols] for a in v] + [total[0:8, cp:C]], axis=1)
        xs = mine(xs, (inner + 2 * N) // F)
        conv[...] = xs[0:4]
        bias[...] = xs[4]
        gate[...] = mine(jnp.concatenate([a[0:8, :cols] for a in v], axis=1), inner // F)[5]
        norm[...] = mine(total[0:8], Dl)[6]
        n = nheads // F
        zero = jnp.zeros((8, 128 - nheads), f32)
        for i, ref in enumerate((h0, h1, h2)):
            hs = [a[0:8, 128 * i : 128 * i + hg] for a in v]
            ref[...] = mine(jnp.concatenate(hs + [zero], axis=1), n)[7]
        step[...] = jnp.concatenate([mine(a[8:16], Dl)[:hg] for a in v], axis=0)


def shards(tokens, in_weight, step_weight, conv_kernel, conv_bias, step_bias, log_decay,
           skip_gain, gate_gain, norm_gain, out_weight, cotangent):
    S = lax.axis_size("seq")
    F = lax.axis_size("fsdp")
    _, T, D = tokens.shape
    inner = out_weight.shape[0] * F
    heads = step_weight.shape[1]
    cols = inner // S
    cp = -(-cols // 128) * 128
    WC = 2 * cp + 2 * N + 128
    Dl = D // F
    cr = cp // F
    per = S // F
    bh = Dl // S
    cfg = (S, F, T, D, cp, WC)
    dims = (inner, heads, cols)
    s = lax.axis_index("seq")

    def padc(a, to):
        return jnp.pad(a, [(0, 0)] * (a.ndim - 1) + [(0, to - a.shape[-1])])

    def part(a, start, size, axis):
        return lax.dynamic_slice_in_dim(a, start, size, axis)

    if cols % 128 == 0:
        wsrc = (in_weight,)
    else:
        wsrc = (
            jnp.concatenate(
                [
                    padc(part(in_weight, s * cols, cols, 1), cp),
                    padc(part(in_weight, inner + s * cols, cols, 1), cp),
                    in_weight[:, 2 * inner :],
                ],
                axis=1,
            ),
        )
    if tight(cfg):
        wo = jnp.pad(
            part(out_weight, lax.rem(s, per) * cols, cols, 0), [(0, cp - cols), (0, 0)]
        )
    else:
        wo = out_weight.reshape(per, cols, D)
    flat = (conv_kernel, conv_bias, gate_gain, norm_gain, step_bias, log_decay, skip_gain)
    nt = cp // 128
    scratch = {**vars(fwd_scratch(cfg)), **vars(bwd_scratch(cfg))}
    names = list(scratch)
    outs = dict(
        block=jax.ShapeDtypeStruct((T, D), bf16),
        input=jax.ShapeDtypeStruct((T, D), f32),
        gz=jax.ShapeDtypeStruct((S, Dl, cp), bf16),
        gx=jax.ShapeDtypeStruct((nt, S, Dl, 128), bf16),
        gbc=jax.ShapeDtypeStruct((S, bh, 2 * N), bf16),
        go=jax.ShapeDtypeStruct((F, per, cr, D), bf16),
        go_s=jax.ShapeDtypeStruct((S, cr, D), bf16),
        sm=jax.ShapeDtypeStruct((S, 16, D), bf16),
    )
    on = list(outs)
    nw = 1
    nf = len(flat)

    def kern(tok, cot, wo, step, *rest):
        flat, rest = rest[:nf], rest[nf:]
        O = SimpleNamespace(**dict(zip(on, rest[nw : nw + len(on)])))
        R = SimpleNamespace(**dict(zip(names, rest[nw + len(on) :])))
        if tight(cfg):
            R.bp = R.cot_all
        wogs = body_fwd(cfg, dims, tok, cot, rest[:nw], wo, step, flat, R)
        body_bwd(cfg, dims, tok, cot, wogs, R, O)

    v = pl.BlockSpec(memory_space=pltpu.VMEM)
    hbm = pl.BlockSpec(memory_space=pl.ANY)
    res = pl.pallas_call(
        kern,
        out_shape=[outs[n] for n in on],
        in_specs=[v, v, hbm, v] + [v] * nf + [hbm] * nw,
        out_specs=[v, v] + [hbm] * (len(on) - 2),
        scratch_shapes=[scratch[n] for n in names],
        compiler_params=pltpu.CompilerParams(
            collective_id=0, has_side_effects=True, vmem_limit_bytes=VMEM_LIMIT
        ),
    )(tokens[0], cotangent[0], wo, step_weight.T, *flat, *wsrc)
    G = SimpleNamespace(**dict(zip(on, res)))
    pieces = cols // cr
    steps = per * pieces
    rows = Dl // steps
    cl, gl, hl = (inner + 2 * N) // F, inner // F, heads // F

    def whole(*shape):
        return pl.BlockSpec(shape, lambda i: (0,) * len(shape))

    def out(*shape):
        return jax.ShapeDtypeStruct(shape, f32)

    joined = pl.pallas_call(
        lambda *refs: assemble(cfg, dims, *refs),
        grid=(steps,),
        out_shape=[
            out(Dl, 2 * inner + 2 * N), out(heads, Dl), out(4, cl), out(cl), out(gl),
            out(Dl), out(hl), out(hl), out(hl), out(per * cols, D),
        ],
        in_specs=[
            pl.BlockSpec((S, rows, cp), lambda i: (0, i, 0)),
            pl.BlockSpec((nt, S, rows, 128), lambda i: (0, 0, i, 0)),
            pl.BlockSpec((rows, 2 * N), lambda i: (i, 0)),
            pl.BlockSpec((1, 1, cr, D), lambda i: (lax.rem(i, pieces), i // pieces, 0, 0)),
            whole(S, 16, D),
        ],
        out_specs=[
            pl.BlockSpec((rows, 2 * inner + 2 * N), lambda i: (i, 0)),
            whole(heads, Dl), whole(4, cl), whole(cl), whole(gl), whole(Dl), whole(hl),
            whole(hl), whole(hl),
            pl.BlockSpec((cr, D), lambda i: (i, 0)),
        ],
    )(G.gz, G.gx, G.gbc.reshape(Dl, 2 * N), G.go, G.sm)
    win, stepg, conv, bias, gate, norm, hd0, hd1, hd2, wout = joined
    return (
        G.block[None],
        G.input[None],
        win,
        stepg.T,
        conv,
        bias,
        hd0,
        hd1,
        hd2,
        gate,
        norm,
        wout,
    )


def solution(mesh):
    row = P("fsdp", None)
    tok = P("fsdp", "seq", None)
    one = P("fsdp")
    return jax.shard_map(
        shards,
        mesh=mesh,
        in_specs=(tok, row, row, P(None, "fsdp"), one, one, one, one, one, one, row, tok),
        out_specs=(tok, tok, row, row, P(None, "fsdp"), one, one, one, one, one, one, row),
        check_vma=False,
    )
```

```python
from types import SimpleNamespace

import jax
import jax.numpy as jnp
from jax import lax
from jax.experimental import pallas as pl
from jax.experimental.pallas import tpu as pltpu
from jax.sharding import PartitionSpec as P

N = 128
HEAD = 64
Q = 128
epsilon = 1e-05
bf16 = jnp.bfloat16
f32 = jnp.float32
MESH = pl.DeviceIdType.MESH
HI = lax.Precision.HIGHEST
VMEM_LIMIT = 64 * 1024 * 1024 - 65536


def mm(a, b, da=1, db=0, precision=None):
    return lax.dot_general(
        a, b, (((da,), (db,)), ((), ())), preferred_element_type=f32, precision=precision
    )


def rcopy(src, dst, ss, rs, **dev):
    return pltpu.make_async_remote_copy(
        src_ref=src, dst_ref=dst, send_sem=ss, recv_sem=rs, device_id=dev, device_id_type=MESH
    )


class Axis:
    def __init__(self, name, outer, inner):
        self.name, self.outer, self.inner = name, outer, inner
        self.me = lax.axis_index(name)
        self.o = self.me // inner
        self.i = lax.rem(self.me, inner)

    def near(self, k):
        half = self.outer // 2
        side = self.o // half
        m = self.o + side * (self.outer - 1 - 2 * self.o)
        at = jnp.where(k == 0, m, k - m * ((3 - k) // 2))
        return at + side * (self.outer - 1 - 2 * at)

    def blk(self, k, q):
        return self.near(k) * self.inner + lax.rem(self.i + q, self.inner)

    def to(self, d):
        return {self.name: d}


class Place:
    def __init__(self, S, F):
        self.S, self.F = S, F
        self.seq = Axis("seq", 4, S // 4)
        self.fsdp = Axis("fsdp", F // 2, 2)
        self.Z, self.X = 4, S // 4
        self.s, self.z, self.x = self.seq.me, self.seq.o, self.seq.i
        self.f = self.fsdp.me
        self.blk = self.seq.blk

    def barrier(self):
        bar = pltpu.get_barrier_semaphore()
        n = 0
        for k in range(1, self.S):
            pl.semaphore_signal(
                bar, inc=1, device_id={"seq": lax.rem(self.s + k, self.S)}, device_id_type=MESH
            )
            n += 1
        for k in range(1, self.F):
            pl.semaphore_signal(
                bar, inc=1, device_id={"fsdp": lax.rem(self.f + k, self.F)}, device_id_type=MESH
            )
            n += 1
        pl.semaphore_wait(bar, n)


class Gather:
    def __init__(self, ax, src, buf, sems, cut=None):
        self.ax, self.src, self.buf, self.cut = ax, src, buf, cut
        self.ss, self.rs = sems

    def at(self, b):
        return self.buf.at[b] if self.cut is None else self.buf.at[b, self.cut]

    def send(self, src, b, sem, dst):
        rcopy(src, self.at(b), self.ss.at[sem], self.rs.at[b], **self.ax.to(dst)).start()

    def start(self):
        ax = self.ax
        for sem, d in ((0, 1), (1, -1)):

            @pl.when(jnp.logical_and(ax.o + d >= 0, ax.o + d < ax.outer))
            def _():
                self.send(self.src, ax.me, sem, ax.me + d * ax.inner)

        self.across(self.src, ax.me, 0)

    def across(self, src, b, k):
        ax = self.ax
        for q in range(1, ax.inner):
            sem = ax.outer + 1 + k * (ax.inner - 1) + q - 1
            self.send(src, b, sem, ax.o * ax.inner + lax.rem(ax.i + q, ax.inner))

    def onward(self, k):
        ax = self.ax
        return ax.o + jnp.where(ax.o > ax.near(k), 1, -1)

    def relay(self, k):
        ax = self.ax
        b = ax.blk(k, 0)
        self.wait(b)
        nxt = self.onward(k)

        @pl.when(jnp.logical_and(nxt >= 0, nxt < ax.outer))
        def _():
            self.send(self.at(b), b, 1 + k, nxt * ax.inner + ax.i)

        self.across(self.at(b), b, k)

    def wait(self, b):
        r = self.at(b)
        rcopy(r, r, self.ss.at[0], self.rs.at[b], **self.ax.to(self.ax.me)).wait_recv()

    def wait_across(self):
        for k in range(self.ax.outer):
            for q in range(1, self.ax.inner):
                self.wait(self.ax.blk(k, q))

    def drain(self):
        ax = self.ax

        def done(sem):
            rcopy(
                self.src, self.src, self.ss.at[sem], self.rs.at[0], **ax.to(ax.me)
            ).wait_send()

        for sem, d in ((0, 1), (1, -1)):

            @pl.when(jnp.logical_and(ax.o + d >= 0, ax.o + d < ax.outer))
            def _():
                done(sem)

        for k in range(1, ax.outer):
            nxt = self.onward(k)

            @pl.when(jnp.logical_and(nxt >= 0, nxt < ax.outer))
            def _():
                done(1 + k)

        for sem in range(ax.outer * (ax.inner - 1)):
            done(ax.outer + 1 + sem)


class Halves:
    def __init__(self, ax, src, buf, sems):
        n = src.shape[0] // 2
        self.parts = []
        for h in range(2):
            cut = pl.ds(n * h, n)
            self.parts.append(
                Gather(ax, src.at[cut], buf, (sems[0].at[h], sems[1].at[h]), cut)
            )

    def start(self):
        for g in self.parts:
            g.start()

    def relay(self, k, ends=None):
        for g in self.parts:
            if ends is None:
                g.relay(k)
                continue
            last = jnp.logical_or(g.ax.o == 0, g.ax.o == g.ax.outer - 1)

            @pl.when(last if ends else jnp.logical_not(last))
            def _():
                g.relay(k)

    def wait(self, b):
        for g in self.parts:
            g.wait(b)

    def drain(self):
        for g in self.parts:
            g.drain()


def gather_sems(outer, inner):
    sem = pltpu.SemaphoreType.DMA
    return sem((outer + 1 + outer * (inner - 1),)), sem((outer * inner,))


def pair(col, p):
    lane = lax.broadcasted_iota(jnp.int32, (col.shape[0], 128), 1)
    return jnp.where(lane < HEAD, col[:, 2 * p : 2 * p + 1], col[:, 2 * p + 1 : 2 * p + 2])


def spread(col, cp):
    return jnp.concatenate([pair(col, p) for p in range(cp // 128)], axis=1)


def row_sums(v):
    part = v[:, :128]
    for p in range(1, v.shape[1] // 128):
        part = part + v[:, 128 * p : 128 * p + 128]
    return jnp.sum(part.T, axis=0, keepdims=True)


def sigmoid(v):
    return 1.0 / (1.0 + jnp.exp(-v))


def softplus(v):
    return jnp.maximum(v, 0.0) + jnp.log1p(jnp.exp(-jnp.abs(v)))


def tri(shape, flip=False):
    i = lax.broadcasted_iota(jnp.int32, shape, 0)
    j = lax.broadcasted_iota(jnp.int32, shape, 1)
    return j >= i if flip else i >= j


def split(x2):
    lane = lax.broadcasted_iota(jnp.int32, x2.shape, 1)
    return jnp.concatenate([jnp.where(lane < HEAD, x2, 0), jnp.where(lane >= HEAD, x2, 0)], axis=0)


def chunk_inputs(c, ext, rawb, small, cp):
    r0 = pl.multiple_of(c * Q, Q)
    v = ext[pl.ds(r0, Q + 16), :].astype(f32)
    C = cp + 2 * N
    taps = [pltpu.roll(v, 3 - k, 0)[16:] if k < 3 else v[16:] for k in range(4)]
    summed = small[4:5, :C]
    for k in range(4):
        summed = summed + small[k : k + 1, :C] * taps[k]
    sig = sigmoid(summed)
    raw = rawb[pl.ds(r0, Q), :].astype(f32) + small[7:8, 0:128]
    dt = softplus(raw)
    rate = -jnp.exp(small[7:8, 128:256])
    cum = mm(tri((Q, Q)).astype(f32), dt * rate, precision=HI)
    return taps, summed, sig, raw, dt, rate, cum


def skip_row(small, cp):
    return spread(small[7:8, 256:384], cp)


def tight(cfg):
    S, F, T, D, cp, WC = cfg
    return S * T * D * 2 > 2**22


def lanes_from(row, shift, width, size):
    n = row.shape[1]
    if n < width:
        row = jnp.concatenate([row, jnp.zeros((row.shape[0], width - n), f32)], axis=1)
    row = pltpu.roll(row, lax.rem(shift + width, width), 1)
    return row[:, :size]


def small_rows(cfg, dims, flat, pc):
    S, F, T, D, cp, WC = cfg
    inner, heads, cols = dims
    conv = inner + 2 * N
    cl, gl, nl, hl = conv // F, inner // F, D // F, heads // F
    def line(v):
        v = v[...].astype(f32)
        v = v if v.ndim == 2 else v[None]
        n = -v.shape[1] % 128
        return jnp.concatenate([v, jnp.zeros((v.shape[0], n), f32)], axis=1) if n else v

    parts = [line(v) for v in flat]
    rows = jnp.concatenate(parts[:2] + [jnp.zeros((3, parts[0].shape[1]), f32)], axis=0)
    lane = lax.broadcasted_iota(jnp.int32, (8, cp), 1)
    xs = lanes_from(rows, cl * pc.f - cols * pc.s, conv, cp)
    bc = lanes_from(rows, cl * pc.f - inner, conv, 2 * N)
    gate = lanes_from(parts[2], gl * pc.f - cols * pc.s, inner, cp)
    if cols < cp:
        xs = jnp.where(lane < cols, xs, 0.0)
        gate = jnp.where(lane[0:1] < cols, gate, 0.0)
    norm = lanes_from(parts[3], nl * pc.f, D, D)
    hg = heads // S
    hv = jnp.concatenate(parts[4:7] + [jnp.zeros((5, 128), f32)], axis=0)
    hv = lanes_from(hv, hl * pc.f - hg * pc.s, 128, 128)
    hv = jnp.where(lane[:, :128] < hg, hv, 0.0)

    def wide(v):
        return jnp.concatenate([v, jnp.zeros((v.shape[0], D - v.shape[1]), f32)], axis=1)

    return jnp.concatenate(
        [
            wide(jnp.concatenate([xs, bc], axis=1)[0:5]),
            wide(gate),
            norm,
            wide(jnp.concatenate([hv[0:1], hv[1:2], hv[2:3]], axis=1)),
        ],
        axis=0,
    )


def body_fwd(cfg, dims, tok, cot, wsrc, wo, step, flat, R):
    S, F, T, D, cp, WC = cfg
    inner, heads, cols = dims
    L = S * T
    C = cp + 2 * N
    per = S // F
    pc = Place(S, F)
    own = R.w_all.at[pc.f]
    hg = heads // S
    up = -(-heads // 8) * 8
    st = step[...].astype(f32)
    if up > heads:
        st = jnp.concatenate([st, jnp.zeros((up - heads, st.shape[1]), f32)], axis=0)
    st = pltpu.roll(st, lax.rem(up - hg * pc.s, up), 0)[:8].T
    lane = lax.broadcasted_iota(jnp.int32, st.shape, 1)
    st = jnp.where(lane < hg, st, 0.0)
    st = jnp.concatenate([st, jnp.zeros((st.shape[0], 120), f32)], axis=1).astype(bf16)
    R.w_all[pc.f, :, 2 * cp + 2 * N :] = st
    if cols < cp:
        parts = [(wsrc[0], own.at[:, pl.ds(0, 2 * cp + 2 * N)])]
    else:
        (win,) = wsrc
        col = pl.multiple_of(pc.s * cols, cols)
        parts = [
            (win.at[:, pl.ds(col, cols)], own.at[:, pl.ds(0, cols)]),
            (win.at[:, pl.ds(inner + col, cols)], own.at[:, pl.ds(cols, cols)]),
            (win.at[:, pl.ds(2 * inner, 2 * N)], own.at[:, pl.ds(2 * cols, 2 * N)]),
        ]
    parts = [pltpu.make_async_copy(a, b, R.wsem.at[i]) for i, (a, b) in enumerate(parts)]
    for c in parts:
        c.start()
    R.sm_own[...] = small_rows(cfg, dims, flat, pc)
    pc.barrier()
    tg = Halves(pc.seq, tok, R.tok_all, (R.ss_t, R.rs_t))
    cg = Halves(pc.seq, cot, R.cot_all, (R.ss_c, R.rs_c))
    wg = Gather(pc.fsdp, own, R.w_all, (R.ss_w, R.rs_w))
    first = lax.rem(pc.s, per)
    owner = pc.s // per
    wogs = []
    if not tight(cfg):
        for p in range(per):
            at = lax.rem(first + p, per)
            wogs.append(
                Gather(pc.fsdp, wo.at[at], R.w_out.at[at], (R.ss_o.at[p], R.rs_o.at[p]))
            )
    sm = R.sm_own
    tg.start()
    for k in range(1, F):
        to = lax.rem(pc.f + k, F)
        rcopy(sm, R.sm_all.at[pc.f], R.ss_m.at[k], R.rs_m.at[pc.f], fsdp=to).start()
    for c in parts:
        c.wait()
    wg.start()
    keep = []
    for p in range(len(wogs)):
        wogs[p].start()
        at = lax.rem(first + p, per)
        keep.append(pltpu.make_async_copy(wo.at[at], R.w_out.at[at, pc.f], R.osem.at[p]))
    if tight(cfg):
        keep.append(pltpu.make_async_copy(wo, R.wo_g, R.osem.at[0]))

        @pl.when(pc.f == owner)
        def _():
            keep[0].start()
            for k in range(1, F):
                to = lax.rem(pc.f + k, F)
                rcopy(wo, R.wo_g, R.ss_o.at[k], R.rs_o.at[0], fsdp=to).start()
    else:
        for c in keep:
            c.start()
    R.tok_all[pc.s] = tok[...]
    R.cot_all[pc.s] = cot[...]
    R.sm_all[pc.f] = sm[...]
    R.ext[0:16, :] = jnp.zeros((16, C), bf16)
    for k in range(1, F):
        o = lax.rem(pc.f + k, F)
        rcopy(sm, R.sm_all.at[o], R.ss_m.at[0], R.rs_m.at[o], fsdp=pc.f).wait_recv()
    total = R.sm_all[0]
    for k in range(1, F):
        total = total + R.sm_all[k]
    R.small[...] = total
    small = R.small
    tg.relay(1)
    tg.relay(2)
    tg.relay(3, False)
    for k in range(1, F // 2):
        wg.relay(k)
    tg.relay(3, True)
    cg.start()
    wg.wait_across()

    def project(j, carry):
        k, q = j // pc.X, lax.rem(j, pc.X)
        b = pc.blk(k, q)

        @pl.when(q > 0)
        def _():
            tg.wait(b)

        @pl.when(j == S // 2)
        def _():
            cg.relay(1)

        r = R.tok_all[b].astype(f32)
        scale = lax.rsqrt(jnp.mean(r * r, axis=1, keepdims=True) + epsilon)
        h = r * scale * small[6:7, :]
        r0 = pl.multiple_of(b * T, T)
        R.hid_t[:, pl.ds(r0, T)] = h.T.astype(bf16)
        out = mm(h.astype(bf16), R.w_all[...].reshape(D, WC)).astype(bf16)
        R.zb[pl.ds(r0, T), :] = out[:, :cp]
        R.rawb[pl.ds(r0, T), :] = out[:, 2 * cp + 2 * N :]
        R.ext[pl.ds(r0 + 16, T), :] = out[:, cp : 2 * cp + 2 * N]
        return carry

    lax.fori_loop(0, S, project, 0)
    R.state[...] = jnp.zeros((N, cp), f32)

    def forward(c, carry):
        @pl.when(jnp.logical_or(c == 0, c == 5))
        def _():
            cg.relay(2 + c // 5)

        r0 = pl.multiple_of(c * Q, Q)
        taps, summed, sig, raw, dt, rate, cum = chunk_inputs(c, R.ext, R.rawb, small, cp)
        act = summed * sig
        x = act[:, :cp]
        bb = act[:, cp : cp + N].astype(bf16)
        cb = act[:, cp + N :].astype(bf16)
        cum_t = cum.T
        dt_t = dt.T
        scores = mm(cb, bb, 1, 1)
        causal = tri((Q, Q))
        parts = []
        for p in range(cp // 128):
            mix = []
            for h in (2 * p, 2 * p + 1):
                gap = jnp.where(causal, cum[:, h : h + 1] - cum_t[h : h + 1, :], -1e30)
                mix.append((jnp.exp(gap) * scores * dt_t[h : h + 1, :]).astype(bf16))
            parts.append(
                mm(jnp.concatenate(mix, axis=1), split(x[:, 128 * p : 128 * p + 128]).astype(bf16))
            )
        state = R.state[...]
        R.states[c] = state
        last = cum[Q - 1 : Q, :]
        y = jnp.concatenate(parts, axis=1) + mm(cb, state.astype(bf16)) * spread(jnp.exp(cum), cp)
        y = y + skip_row(small, cp) * x
        wx = (spread(jnp.exp(last - cum) * dt, cp) * x).astype(bf16)
        R.state[...] = spread(jnp.exp(last), cp) * state + mm(bb, wx, 0, 0)
        R.y[pl.ds(r0, Q), :] = y
        z = R.zb[pl.ds(r0, Q), :].astype(f32)
        gated = (y * (z * sigmoid(z))).astype(bf16)
        R.dpx[pl.ds(r0, Q), :cp] = gated
        g32 = gated.astype(f32)
        R.st[0:1, pl.ds(r0, Q)] = row_sums(g32 * g32)
        return carry

    lax.fori_loop(0, L // Q, forward, 0)

    if tight(cfg):
        group = R.wo_g

        @pl.when(pc.f != owner)
        def _():
            rcopy(wo, R.wo_g, R.ss_o.at[0], R.rs_o.at[0], fsdp=pc.f).wait_recv()

        @pl.when(pc.f == owner)
        def _():
            keep[0].wait()
    else:
        group = R.w_out.at[first, owner]
        for c in keep:
            c.wait()
        for k in range(1, F // 2):
            wogs[0].relay(k)
        wogs[0].wait_across()

    def mixed(j, carry):
        k, q = j // pc.X, lax.rem(j, pc.X)
        b = pc.blk(k, q)

        @pl.when(q > 0)
        def _():
            cg.wait(b)

        r0 = pl.multiple_of(b * T, T)
        mg = mm(R.cot_all[b], group[...], 1, 1)
        R.mg[pl.ds(r0, T), :] = mg
        g = mg * small[5:6, :cp] * R.dpx[pl.ds(r0, T), :cp].astype(f32)
        R.st[1:2, pl.ds(r0, T)] = row_sums(g)
        return carry

    lax.fori_loop(0, S, mixed, 0)
    for k in range(1, S):
        rcopy(
            R.st, R.st_all.at[pc.s], R.ss_s.at[k], R.rs_s.at[pc.s],
            seq=lax.rem(pc.s + k, S),
        ).start()
    R.st_all[pc.s] = R.st[...]
    for k in range(1, S):
        o = lax.rem(pc.s + k, S)
        rcopy(R.st, R.st_all.at[o], R.ss_s.at[0], R.rs_s.at[o], seq=pc.s).wait_recv()
    total = R.st_all[0]
    for k in range(1, S):
        total = total + R.st_all[k]
    R.stats[...] = total

    for g in [tg, cg, wg]:
        g.drain()
    for k in range(1, S):
        rcopy(R.st, R.st, R.ss_s.at[k], R.rs_s.at[0], seq=pc.s).wait_send()
    for k in range(1, F):
        rcopy(sm, sm, R.ss_m.at[k], R.rs_m.at[0], fsdp=pc.f).wait_send()
    if tight(cfg):

        @pl.when(pc.f == owner)
        def _():
            for k in range(1, F):
                rcopy(wo, wo, R.ss_o.at[k], R.rs_o.at[0], fsdp=pc.f).wait_send()

    return wogs


def fwd_scratch(cfg):
    S, F, T, D, cp, WC = cfg
    L = S * T
    Dl = D // F
    C = cp + 2 * N
    V = pltpu.VMEM
    sem = pltpu.SemaphoreType.DMA
    per = S // F
    seq = gather_sems(4, S // 4)
    fsdp = gather_sems(F // 2, 2)
    out = SimpleNamespace(
        tok_all=V((S, T, D), bf16),
        cot_all=V((S, T, D), bf16),
        w_all=V((F, Dl, WC), bf16),
        sm_own=V((8, D), f32),
        sm_all=V((F, 8, D), f32),
        small=V((8, D), f32),
        hid_t=V((D, L), bf16),
        zb=V((L, cp), bf16),
        rawb=V((L, 128), bf16),
        ext=V((16 + L, C), bf16),
        state=V((N, cp), f32),
        states=V((L // Q, N, cp), f32),
        y=V((L, cp), f32),
        mg=V((L, cp), f32),
        st=V((2, L), f32),
        st_all=V((S, 2, L), f32),
        stats=V((2, L), f32),
        ss_t=sem((2,) + seq[0].shape),
        rs_t=sem((2,) + seq[1].shape),
        ss_c=sem((2,) + seq[0].shape),
        rs_c=sem((2,) + seq[1].shape),
        ss_w=fsdp[0],
        rs_w=fsdp[1],
        ss_m=sem((F,)),
        rs_m=sem((F,)),
        wsem=sem((4,)),
        osem=sem((per,)),
        ss_s=sem((S,)),
        rs_s=sem((S,)),
    )
    if tight(cfg):
        out.wo_g = V((cp, D), bf16)
        out.ss_o = out.rs_o = sem((F,))
    else:
        out.w_out = V((per, F, cp, D), bf16)
        out.ss_o = sem((per,) + fsdp[0].shape)
        out.rs_o = sem((per,) + fsdp[1].shape)
    return out


class Scatter:
    def __init__(self, pc, part, rx, rz, rn, sems):
        self.pc, self.part, self.rx, self.rz, self.rn = pc, part, rx, rz, rn
        self.ssx, self.rsx, self.ssz, self.rsz, self.rsn = sems
        self.near = jnp.logical_or(pc.z == 1, pc.z == 2)

    @staticmethod
    def sems(S):
        sem = pltpu.SemaphoreType.DMA
        return sem((S,)), sem((4, S // 4 - 1)), sem((4,)), sem((2,)), sem((2,))

    def got(self, ref, sem):
        rcopy(ref, ref, sem, sem, seq=self.pc.s).wait_recv()

    def across(self, b):
        pc = self.pc
        zb, xb = b // pc.X, lax.rem(b, pc.X)

        @pl.when(xb != pc.x)
        def _():
            slot = lax.rem(pc.x - xb - 1 + pc.X, pc.X)
            rcopy(
                self.part.at[b], self.rx.at[zb, slot], self.ssx.at[b], self.rsx.at[zb, slot],
                seq=pc.z * pc.X + xb,
            ).start()

    def other(self, zb):
        return zb // 2 != self.pc.z // 2

    def column(self, zb):
        pc = self.pc
        b = zb * pc.X + pc.x
        total = self.part[b].astype(f32)
        for q in range(pc.X - 1):
            self.got(self.rx.at[zb, q], self.rsx.at[zb, q])
            total = total + self.rx[zb, q].astype(f32)
        self.part[b] = total.astype(bf16)

        @pl.when(jnp.logical_and(zb != pc.z, jnp.logical_not(self.other(zb))))
        def _():
            rcopy(
                self.part.at[b], self.rz.at[0], self.ssz.at[zb], self.rsz.at[0], seq=b
            ).start()

        @pl.when(jnp.logical_and(self.other(zb), jnp.logical_not(self.near)))
        def _():
            slot = lax.rem(zb, 2)
            rcopy(
                self.part.at[b], self.rn.at[slot], self.ssz.at[zb], self.rsn.at[slot],
                seq=(pc.z + 1 - 2 * lax.rem(pc.z, 2)) * pc.X + pc.x,
            ).start()

    def merge(self, zb):
        pc = self.pc

        @pl.when(jnp.logical_and(self.other(zb), self.near))
        def _():
            b = zb * pc.X + pc.x
            slot = lax.rem(zb, 2)
            self.got(self.rn.at[slot], self.rsn.at[slot])
            total = self.part[b].astype(f32) + self.rn[slot].astype(f32)
            self.part[b] = total.astype(bf16)
            rcopy(
                self.part.at[b], self.rz.at[1], self.ssz.at[zb], self.rsz.at[1], seq=b
            ).start()

    def total(self):
        out = self.part[self.pc.s].astype(f32)
        for q in range(2):
            self.got(self.rz.at[q], self.rsz.at[q])
            out = out + self.rz[q].astype(f32)
        return out

    def drain(self):
        pc = self.pc
        r = self.rz.at[0]
        for b in range(pc.S):

            @pl.when(b % pc.X != pc.x)
            def _():
                rcopy(r, r, self.ssx.at[b], self.rsz.at[0], seq=pc.s).wait_send()

        for zb in range(pc.Z):

            @pl.when(zb != pc.z)
            def _():
                rcopy(r, r, self.ssz.at[zb], self.rsz.at[0], seq=pc.s).wait_send()


class Shared:
    def __init__(self, pc, part, recv, ss, rs):
        self.pc, self.part, self.recv, self.ss, self.rs = pc, part, recv, ss, rs

    def send(self, k):
        pc = self.pc
        to = lax.rem(pc.f + k, pc.F)
        rcopy(
            self.part.at[to], self.recv.at[k - 1], self.ss.at[k - 1], self.rs.at[k - 1], fsdp=to
        ).start()

    def total(self):
        pc = self.pc
        out = self.part[pc.f].astype(f32)
        for k in range(1, pc.F):
            r = self.recv.at[k - 1]
            rcopy(r, r, self.ss.at[k - 1], self.rs.at[k - 1], fsdp=pc.f).wait_recv()
            out = out + self.recv[k - 1].astype(f32)
        return out

    def drain(self):
        for k in range(1, self.pc.F):
            r = self.recv.at[k - 1]
            rcopy(r, r, self.ss.at[k - 1], self.rs.at[k - 1], fsdp=self.pc.f).wait_send()


def body_bwd(cfg, dims, tok, cot, wogs, R, O):
    S, F, T, D, cp, WC = cfg
    inner = float(dims[0])
    L = S * T
    C = cp + 2 * N
    Dl = D // F
    nc = L // Q
    cr = cp // F
    per = S // F
    bh = Dl // S
    pc = Place(S, F)
    small = R.small
    if tight(cfg):
        blk = Scatter(pc, R.bp, R.brx, R.brz, R.brn, (R.bs0, R.bs1, R.bs2, R.bs3, R.bs4))
    hid = Scatter(pc, R.tok_all, R.hrx, R.hrz, R.hrn, (R.hs0, R.hs1, R.hs2, R.hs3, R.hs4))
    zs = Shared(pc, R.zp, R.zr, R.zs0, R.zs1)
    os_ = Shared(pc, R.op, R.orecv, R.os0, R.os1)
    nt = cp // 128

    def xs(t):
        return Shared(pc, R.xp.at[t], R.xr.at[t], R.xs0.at[t], R.xs1.at[t])

    def xg(t):
        return Gather(pc.seq, R.xred.at[t], O.gx.at[t], (R.gx0.at[t], R.gx1.at[t]))

    def own_x(t):
        return pltpu.make_async_copy(R.xred.at[t], O.gx.at[t, pc.s], R.xsem.at[t])

    def settle(t):
        R.xred[t] = xs(t).total().astype(bf16)
        xg(t).start()
        own_x(t).start()
    bs = Shared(pc, R.cp_, R.cr_, R.cs0, R.cs1)
    zg = Gather(pc.seq, R.zred, O.gz, (R.gz0, R.gz1))
    og = Gather(pc.seq, R.ored, O.go_s, (R.go0, R.go1))
    sg = Gather(pc.seq, R.asum, O.sm, (R.as2, R.as3))

    def direct(src, dst, ss, rs, to):
        rcopy(src, dst.at[pc.s], ss.at[to], rs.at[pc.s], seq=to).start()

    def arrived(dst, ss, rs):
        for k in range(1, S):
            o = lax.rem(pc.s + k, S)
            r = dst.at[o]
            rcopy(r, r, ss.at[0], rs.at[o], seq=pc.s).wait_recv()

    def sent(src, ss, rs):
        for k in range(1, S):
            rcopy(src, src, ss.at[lax.rem(pc.s + k, S)], rs.at[0], seq=pc.s).wait_send()

    def own(src, dst, i):
        return pltpu.make_async_copy(src, dst, R.lsem.at[i])

    gate = small[5:6, :cp]
    R.acc[...] = jnp.zeros((16, D), f32)
    R.hacc[...] = jnp.zeros((2, 8, 128), f32)
    R.dstate[...] = jnp.zeros((N, cp), f32)
    R.head[...] = jnp.zeros((8, C), f32)

    def first(i, carry):
        c = lax.rem(pc.s + 1 + i, nc)
        r0 = pl.multiple_of(c * Q, Q)
        rows = pl.ds(r0, Q)
        st = jnp.concatenate([R.stats[:, rows], jnp.zeros((6, Q), f32)], axis=0).T
        scale = lax.rsqrt(st[:, 0:1] / inner + epsilon)
        mean = st[:, 1:2] / inner
        gated = R.dpx[rows, :cp].astype(f32)
        mg = R.mg[rows, :]
        ng = gated * scale
        mn = ng * gate
        R.acc[5:6, :cp] += jnp.sum(mg * ng, axis=0, keepdims=True)
        gg = (scale * (mg * gate) - scale * scale * scale * gated * mean).astype(bf16).astype(f32)
        z = R.zb[rows, :].astype(f32)
        sz = sigmoid(z)
        R.zb[rows, :] = (gg * R.y[rows, :] * (sz * (1.0 + z * (1.0 - sz)))).astype(bf16)
        R.mg[rows, :] = gg * (z * sz)
        R.mn_t[:, rows] = mn.T.astype(bf16)
        if tight(cfg):
            R.dpx[rows, :cp] = mn.astype(bf16)
        else:
            R.mn[c] = mn.astype(bf16)

            @pl.when(c != pc.s)
            def _():
                direct(R.mn.at[c], R.mall, R.ms0, R.ms1, c)

        return carry

    def block(i, carry):
        c = nc - 1 - i
        rows = pl.ds(pl.multiple_of(c * Q, Q), Q)
        R.bp[c] = mm(R.dpx[rows, :cp], R.wo_g[...]).astype(bf16)
        blk.across(c)
        return carry

    lax.fori_loop(0, nc, first, 0)

    def zpart(k, carry):
        to = lax.rem(pc.f + k, F)
        rows = pl.ds(pl.multiple_of(to * Dl, Dl), Dl)
        R.zp[to] = mm(R.hid_t[rows, :], R.zb[...]).astype(bf16)

        @pl.when(k < F)
        def _():
            rcopy(
                R.zp.at[to], R.zr.at[k - 1], R.zs0.at[k - 1], R.zs1.at[k - 1], fsdp=to
            ).start()
        return carry

    lax.fori_loop(1, F + 1, zpart, 0)
    W = 384

    def opart(j, carry):
        cols = pl.ds(pl.multiple_of(j * W, W), W)
        a = R.cot_all[:, :, cols].reshape(L, W)
        R.op[:, :, cols] = mm(R.mn_t[...], a).reshape(F, cr, W).astype(bf16)
        return carry

    lax.fori_loop(0, D // W, opart, 0)
    for g in wogs[1:]:
        for k in range(1, F // 2):
            g.relay(k)
    for k in range(1, F):
        os_.send(k)
    if tight(cfg):
        lax.fori_loop(0, nc, block, 0)

    sel = (
        lax.broadcasted_iota(jnp.int32, (8, cp), 1) // HEAD
        == lax.broadcasted_iota(jnp.int32, (8, cp), 0)
    ).astype(f32)
    sub = lax.broadcasted_iota(jnp.int32, (8, Q), 0)

    def scan(i, carry):
        c = nc - 1 - i
        r0 = pl.multiple_of(c * Q, Q)
        rows = pl.ds(r0, Q)

        if tight(cfg):

            @pl.when(i < pc.Z)
            def _():
                blk.column(pc.Z - 1 - i)

            @pl.when(jnp.logical_and(i >= pc.Z, i < 2 * pc.Z))
            def _():
                blk.merge(2 * pc.Z - 1 - i)

        @pl.when(i == 1)
        def _():
            R.zred[...] = zs.total().astype(bf16)
            zg.start()
            own(R.zred, O.gz.at[pc.s], 0).start()

        @pl.when(i == 4)
        def _():
            R.ored[...] = os_.total().astype(bf16)
            og.start()
            own(R.ored, O.go_s.at[pc.s], 5).start()

        @pl.when(jnp.logical_and(i >= 4, i < 4 + pc.Z - 1))
        def _():
            zg.relay(i - 3)

        @pl.when(i == 7)
        def _():
            og.relay(1)

        taps, summed, sig, raw, dt, rate, cum = chunk_inputs(c, R.ext, R.rawb, small, cp)
        act = summed * sig
        x = act[:, :cp]
        xb = x.astype(bf16)
        bb = act[:, cp : cp + N].astype(bf16)
        cb = act[:, cp + N :].astype(bf16)
        cum_t = cum.T
        dt_t = dt.T
        dy = R.mg[rows, :]
        dyb = dy.astype(bf16)
        last = cum[Q - 1 : Q, :]
        edy = spread(jnp.exp(cum), cp) * dy
        edyb = edy.astype(bf16)
        wdec = jnp.exp(last - cum)
        w = wdec * dt
        state = R.states[c]
        sb = state.astype(bf16)
        ds = R.dstate[...]
        dsb = ds.astype(bf16)
        ws = spread(w, cp)
        v = mm(bb, dsb)
        carr = mm(sel, edy * mm(cb, sb), 1, 1, HI)
        dw = mm(sel, x * v, 1, 1, HI)
        db = mm((ws * x).astype(bf16), dsb, 1, 1)
        dc = mm(edyb, sb, 1, 1)
        dlast = mm(sel, jnp.sum(state * ds, axis=0, keepdims=True), 1, 1, HI)
        R.dstate[...] = spread(jnp.exp(last), cp) * ds + mm(cb, edyb, 0, 0)
        scores = mm(bb, cb, 1, 1)
        seen = tri((Q, Q), True)
        dtb = dt_t[0:8].astype(bf16)
        dsc = jnp.zeros((Q, Q), f32)
        direct = jnp.zeros((8, Q), f32)
        onto = jnp.zeros((8, Q), f32)
        parts = []
        for p in range(cp // 128):
            cols = slice(128 * p, 128 * p + 128)
            g2 = mm(split(x[:, cols]).astype(bf16), dyb[:, cols], 1, 1)
            mix = []
            for h in (2 * p, 2 * p + 1):
                g = g2[:Q] if h % 2 == 0 else g2[Q:]
                decay = jnp.exp(jnp.where(seen, cum_t[h : h + 1, :] - cum[:, h : h + 1], -1e30))
                ls = decay * scores
                mix.append((ls * dt[:, h : h + 1]).astype(bf16))
                e = (g * ls).astype(bf16)
                dsc = dsc + g * decay * dt[:, h : h + 1]
                direct = direct + mm(jnp.where(sub == h, 1.0, 0.0).astype(bf16), e, 1, 1)
                onto = onto + mm(jnp.where(sub == h, dtb.astype(f32), 0.0).astype(bf16), e)
            parts.append(mm(jnp.concatenate(mix, axis=1), split(dy[:, cols]).astype(bf16)))
        dscb = dsc.astype(bf16)
        db = db + mm(dscb, cb)
        dc = dc + mm(dscb, bb, 0, 0)
        dx = skip_row(small, cp) * dy + ws * v + jnp.concatenate(parts, axis=1)
        R.acc[7:8, :cp] += jnp.sum(dy * x, axis=0, keepdims=True)
        dt_r = dt_t[0:8]
        wdec_r = wdec.T[0:8]
        w_r = wdec_r * dt_r
        rate_r = jnp.broadcast_to(rate, (128, 128)).T[0:8, 0:1]
        last_r = jnp.exp(cum_t[0:8, Q - 1 : Q])
        dcum = carr + onto - dtb.astype(f32) * direct - w_r * dw
        end = jnp.sum(w_r * dw, axis=1, keepdims=True) + last_r * dlast
        da = mm(dcum, tri((Q, Q)).astype(f32), precision=HI) + end
        ddt = direct + wdec_r * dw + rate_r * da
        draw = ddt * sigmoid(raw).T[0:8]
        R.hacc[0] += draw
        R.hacc[1] += da * dt_r * rate_r
        dact = jnp.concatenate([dx, db, dc], axis=1)
        dsum = dact * (sig * (1.0 + summed * (1.0 - sig)))
        full = jnp.concatenate([dsum, R.head[...]], axis=0)
        dxbc = jnp.zeros((Q, C), f32)
        for k in range(4):
            R.acc[k : k + 1, :C] += jnp.sum(dsum * taps[k], axis=0, keepdims=True)
            moved = pltpu.roll(full, Q + 8 - (3 - k), 0)[:Q] if k < 3 else dsum
            dxbc = dxbc + small[k : k + 1, :C] * moved
        R.acc[4:5, :C] += jnp.sum(dsum, axis=0, keepdims=True)
        R.head[...] = dsum[:8]
        R.dpx[rows, :C] = dxbc.astype(bf16)
        R.acc[8:16, :] += mm(draw.astype(bf16), R.hid_t[:, rows], 1, 1)
        pad = jnp.concatenate([draw, jnp.zeros((120, Q), f32)], axis=0).T
        R.dpx[rows, C:] = pad.astype(bf16)
        grad = jnp.concatenate([R.zb[rows, :], R.dpx[rows, :]], axis=1)
        hp = mm(grad, R.w_all[...].reshape(D, WC), 1, 1)
        r = R.tok_all[c].astype(f32)
        scale = lax.rsqrt(jnp.mean(r * r, axis=1, keepdims=True) + epsilon)
        R.acc[6:7, :] += jnp.sum(hp * r * scale, axis=0, keepdims=True)
        R.tok_all[c] = hp.astype(bf16)
        hid.across(c)
        return carry

    lax.fori_loop(0, nc, scan, 0)

    diag = lax.broadcasted_iota(jnp.int32, (8, 128), 0) == lax.broadcasted_iota(
        jnp.int32, (8, 128), 1
    )

    def along(v):
        return jnp.sum(jnp.where(diag, jnp.sum(v, axis=1, keepdims=True), 0.0), axis=0, keepdims=True)

    dskip = jnp.sum(
        jnp.where(diag, mm(sel, R.acc[7:8, :cp], 1, 1, HI), 0.0), axis=0, keepdims=True
    )
    R.acc[7:8, :] = jnp.concatenate(
        [along(R.hacc[0]), along(R.hacc[1]), dskip, jnp.zeros((1, D - 384), f32)], axis=1
    )
    R.accb[...] = R.acc[...].astype(bf16)
    for k in range(1, F):
        to = lax.rem(pc.f + k, F)
        rcopy(
            R.accb, R.ar.at[k - 1], R.as0.at[k - 1], R.as1.at[k - 1], fsdp=to
        ).start()

    for t in range(nt):

        def xpart(k, carry):
            to = lax.rem(pc.f + k, F)
            rows = pl.ds(pl.multiple_of(to * Dl, Dl), Dl)
            R.xp[t, to] = mm(R.hid_t[rows, :], R.dpx[:, 128 * t : 128 * t + 128]).astype(bf16)

            @pl.when(k < F)
            def _():
                rcopy(
                    R.xp.at[t, to], R.xr.at[t, k - 1], R.xs0.at[t, k - 1], R.xs1.at[t, k - 1],
                    fsdp=to,
                ).start()
            return carry

        lax.fori_loop(1, F + 1, xpart, 0)

    def lower(k, carry):
        to = lax.rem(pc.f + k, F)
        rows = pl.ds(pl.multiple_of(to * Dl, Dl), Dl)
        R.cp_[to] = mm(R.hid_t[rows, :], R.dpx[:, cp:C]).astype(bf16)

        @pl.when(k < F)
        def _():
            rcopy(
                R.cp_.at[to], R.cr_.at[k - 1], R.cs0.at[k - 1], R.cs1.at[k - 1], fsdp=to
            ).start()
        return carry

    lax.fori_loop(1, F + 1, lower, 0)
    def hid_column(i, carry):
        hid.column(pc.Z - 1 - i)
        return carry

    total = R.acc[...]
    for k in range(1, F):
        r = R.ar.at[k - 1]
        rcopy(r, r, R.as0.at[k - 1], R.as1.at[k - 1], fsdp=pc.f).wait_recv()
        total = total + R.ar[k - 1].astype(f32)
    R.asum[...] = total.astype(bf16)
    sg.start()
    own(R.asum, O.sm.at[pc.s], 1).start()
    og.relay(2)
    settle(0)
    og.relay(3)
    for t in range(1, nt):
        settle(t)
    low = bs.total()
    for g in range(S):
        R.cb[g] = low[g * bh : (g + 1) * bh].astype(bf16)
    for k in range(1, S):
        to = lax.rem(pc.s + k, S)
        direct(R.cb.at[to], R.cbr, R.cb0, R.cb1, to)
    lax.fori_loop(0, 2, hid_column, 0)
    sg.relay(1)
    for t in range(nt):
        xg(t).relay(1)
    mine = tok[...].astype(f32)
    if tight(cfg):
        O.block[...] = (mine + blk.total()).astype(bf16)
    else:
        for g in wogs[1:]:
            g.wait_across()
        arrived(R.mall, R.ms0, R.ms1)
        R.mall[pc.s] = R.mn[pc.s]
        R.total[...] = mine

        def add(g, carry):
            w = R.w_out[lax.rem(g, per), g // per]
            R.total[...] += mm(R.mall[g], w)
            return carry

        lax.fori_loop(0, S, add, 0)
        O.block[...] = R.total[...].astype(bf16)
    lax.fori_loop(2, pc.Z, hid_column, 0)
    for zb in (3, 2):
        hid.merge(zb)
    sg.relay(2)
    for t in range(nt):
        xg(t).relay(2)
    arrived(R.cbr, R.cb0, R.cb1)
    R.cbr[pc.s] = R.cb[pc.s]
    low = R.cbr[0].astype(f32)
    for g in range(1, S):
        low = low + R.cbr[g].astype(f32)
    R.cbd[...] = low.astype(bf16)
    for k in range(1, S):
        direct(R.cbd, O.gbc, R.cd0, R.cd1, lax.rem(pc.s + k, S))
    own(R.cbd, O.gbc.at[pc.s], 4).start()
    own(R.ored, O.go_s.at[pc.s], 5).wait()
    og.wait_across()
    for k in range(1, F):
        to = lax.rem(pc.f + k, F)
        rcopy(
            O.go_s.at[pl.ds(to * per, per)], O.go.at[pc.f], R.gs0.at[k], R.gs1.at[pc.f],
            fsdp=to,
        ).start()
    own(O.go_s.at[pl.ds(pc.f * per, per)], O.go.at[pc.f], 3).start()
    sg.relay(3)
    for t in range(nt):
        xg(t).relay(3)
    for zb in (1, 0):
        hid.merge(zb)

    scale = lax.rsqrt(jnp.mean(mine * mine, axis=1, keepdims=True) + epsilon)
    e = hid.total() * small[6:7, :]
    mean = jnp.mean(e * mine, axis=1, keepdims=True)
    O.input[...] = cot[...].astype(f32) + scale * e - scale * scale * scale * mine * mean

    zg.wait_across()
    for k in range(1, F):
        o = lax.rem(pc.f + k, F)
        r = O.go.at[o]
        rcopy(r, r, R.gs0.at[0], R.gs1.at[o], fsdp=pc.f).wait_recv()
    arrived(O.gbc, R.cd0, R.cd1)
    sg.wait_across()
    for t in range(nt):
        xg(t).wait_across()
        own_x(t).wait()
    own(R.zred, O.gz.at[pc.s], 0).wait()
    own(R.asum, O.sm.at[pc.s], 1).wait()
    own(O.go_s.at[pl.ds(pc.f * per, per)], O.go.at[pc.f], 3).wait()
    own(R.cbd, O.gbc.at[pc.s], 4).wait()
    if tight(cfg):
        blk.drain()
    else:
        sent(R.mn.at[0], R.ms0, R.ms1)
    sent(R.cb.at[0], R.cb0, R.cb1)
    sent(R.cbd, R.cd0, R.cd1)
    for a in [hid, zs, os_, bs, zg, og, sg] + wogs:
        a.drain()
    for t in range(nt):
        xs(t).drain()
        xg(t).drain()
    for k in range(1, F):
        r = R.ar.at[k - 1]
        rcopy(r, r, R.as0.at[k - 1], R.as1.at[0], fsdp=pc.f).wait_send()
        r = O.go.at[0]
        rcopy(r, r, R.gs0.at[k], R.gs1.at[0], fsdp=pc.f).wait_send()


def bwd_scratch(cfg):
    S, F, T, D, cp, WC = cfg
    L = S * T
    Dl = D // F
    C = cp + 2 * N
    Z, X = 4, S // 4
    cr = cp // F
    bh = Dl // S
    V = pltpu.VMEM
    sem = pltpu.SemaphoreType.DMA
    seq = gather_sems(4, S // 4)
    nt = cp // 128
    out = SimpleNamespace(
        acc=V((16, D), f32),
        asum=V((16, D), bf16),
        accb=V((16, D), bf16),
        ar=V((F - 1, 16, D), bf16),
        hacc=V((2, 8, 128), f32),
        dstate=V((N, cp), f32),
        head=V((8, C), f32),
        mn_t=V((cp, L), bf16),
        dpx=V((L, WC - cp), bf16),
        hrx=V((Z, X - 1, T, D), bf16),
        hrz=V((2, T, D), bf16),
        hrn=V((2, T, D), bf16),
        zp=V((F, Dl, cp), bf16),
        zr=V((F - 1, Dl, cp), bf16),
        zred=V((Dl, cp), bf16),
        op=V((F, cr, D), bf16),
        orecv=V((F - 1, cr, D), bf16),
        ored=V((cr, D), bf16),
        xp=V((nt, F, Dl, 128), bf16),
        xr=V((nt, F - 1, Dl, 128), bf16),
        xred=V((nt, Dl, 128), bf16),
        cp_=V((F, Dl, 2 * N), bf16),
        cr_=V((F - 1, Dl, 2 * N), bf16),
        cb=V((S, bh, 2 * N), bf16),
        cbr=V((S, bh, 2 * N), bf16),
        cbd=V((bh, 2 * N), bf16),
        lsem=sem((6,)),
        as0=sem((F,)), as1=sem((F,)), as2=seq[0], as3=seq[1],
        gs0=sem((F,)), gs1=sem((F,)), cs0=sem((F,)), cs1=sem((F,)),
        cb0=sem((S,)), cb1=sem((S,)), cd0=sem((S,)), cd1=sem((S,)),
        zs0=sem((F,)), zs1=sem((F,)), gz0=seq[0], gz1=seq[1],
        os0=sem((F,)), os1=sem((F,)), go0=seq[0], go1=seq[1],
        xs0=sem((nt, F)), xs1=sem((nt, F)), xsem=sem((nt,)),
        gx0=sem((nt,) + seq[0].shape), gx1=sem((nt,) + seq[1].shape),
    )
    out.hs0, out.hs1, out.hs2, out.hs3, out.hs4 = Scatter.sems(S)
    if tight(cfg):
        out.brx = V((Z, X - 1, T, D), bf16)
        out.brz = V((2, T, D), bf16)
        out.brn = V((2, T, D), bf16)
        out.bs0, out.bs1, out.bs2, out.bs3, out.bs4 = Scatter.sems(S)
    else:
        out.mn = V((S, T, cp), bf16)
        out.mall = V((S, T, cp), bf16)
        out.total = V((T, D), f32)
        out.ms0 = out.ms1 = sem((S,))
    return out


def assemble(cfg, dims, gz, gx, gbc, go, sm, *refs):
    S, F, T, D, cp, WC = cfg
    n = (len(refs) - 10) // 2
    for a, b in zip(refs[:n], refs[n + 10 :]):
        b[...] = a[...]
    win, step, conv, bias, gate, norm, h0, h1, h2, wout = refs[n : n + 10]
    inner, nheads, cols = dims
    for g in range(S):
        win[:, g * cols : (g + 1) * cols] = gz[g, :, :cols].astype(f32)
        for t in range(gx.shape[0]):
            n = min(128, cols - 128 * t)
            at = inner + g * cols + 128 * t
            win[:, at : at + n] = gx[t, g, :, :n].astype(f32)
    wout[...] = go[0, 0].astype(f32)
    C = cp + 2 * N
    hg = nheads // S
    Dl = D // F
    win[:, 2 * inner :] = gbc[...].astype(f32)

    @pl.when(pl.program_id(0) == 0)
    def _():
        f = lax.axis_index("fsdp")

        def mine(v, size):
            n = v.shape[1]
            return pltpu.roll(v, lax.rem(n - size * f, n), 1)[:, :size]

        v = [sm[g].astype(f32) for g in range(S)]
        total = v[0]
        for g in range(1, S):
            total = total + v[g]
        xs = jnp.concatenate([a[0:8, :cols] for a in v] + [total[0:8, cp:C]], axis=1)
        xs = mine(xs, (inner + 2 * N) // F)
        conv[...] = xs[0:4]
        bias[...] = xs[4]
        gate[...] = mine(jnp.concatenate([a[0:8, :cols] for a in v], axis=1), inner // F)[5]
        norm[...] = mine(total[0:8], Dl)[6]
        n = nheads // F
        zero = jnp.zeros((8, 128 - nheads), f32)
        for i, ref in enumerate((h0, h1, h2)):
            hs = [a[0:8, 128 * i : 128 * i + hg] for a in v]
            ref[...] = mine(jnp.concatenate(hs + [zero], axis=1), n)[7]
        step[...] = jnp.concatenate([mine(a[8:16], Dl)[:hg] for a in v], axis=0)


def shards(tokens, in_weight, step_weight, conv_kernel, conv_bias, step_bias, log_decay,
           skip_gain, gate_gain, norm_gain, out_weight, cotangent):
    S = lax.axis_size("seq")
    F = lax.axis_size("fsdp")
    _, T, D = tokens.shape
    inner = out_weight.shape[0] * F
    heads = step_weight.shape[1]
    cols = inner // S
    cp = -(-cols // 128) * 128
    WC = 2 * cp + 2 * N + 128
    Dl = D // F
    cr = cp // F
    per = S // F
    bh = Dl // S
    cfg = (S, F, T, D, cp, WC)
    dims = (inner, heads, cols)
    s = lax.axis_index("seq")

    def padc(a, to):
        return jnp.pad(a, [(0, 0)] * (a.ndim - 1) + [(0, to - a.shape[-1])])

    def part(a, start, size, axis):
        return lax.dynamic_slice_in_dim(a, start, size, axis)

    if cols % 128 == 0:
        wsrc = (in_weight,)
    else:
        wsrc = (
            jnp.concatenate(
                [
                    padc(part(in_weight, s * cols, cols, 1), cp),
                    padc(part(in_weight, inner + s * cols, cols, 1), cp),
                    in_weight[:, 2 * inner :],
                ],
                axis=1,
            ),
        )
    if tight(cfg):
        wo = jnp.pad(
            part(out_weight, lax.rem(s, per) * cols, cols, 0), [(0, cp - cols), (0, 0)]
        )
    else:
        wo = out_weight.reshape(per, cols, D)
    flat = (conv_kernel, conv_bias, gate_gain, norm_gain, step_bias, log_decay, skip_gain)
    nt = cp // 128
    scratch = {**vars(fwd_scratch(cfg)), **vars(bwd_scratch(cfg))}
    names = list(scratch)
    outs = dict(
        block=jax.ShapeDtypeStruct((T, D), bf16),
        input=jax.ShapeDtypeStruct((T, D), f32),
        gz=jax.ShapeDtypeStruct((S, Dl, cp), bf16),
        gx=jax.ShapeDtypeStruct((nt, S, Dl, 128), bf16),
        gbc=jax.ShapeDtypeStruct((S, bh, 2 * N), bf16),
        go=jax.ShapeDtypeStruct((F, per, cr, D), bf16),
        go_s=jax.ShapeDtypeStruct((S, cr, D), bf16),
        sm=jax.ShapeDtypeStruct((S, 16, D), bf16),
    )
    on = list(outs)
    nw = 1
    nf = len(flat)

    def kern(tok, cot, wo, step, *rest):
        flat, rest = rest[:nf], rest[nf:]
        O = SimpleNamespace(**dict(zip(on, rest[nw : nw + len(on)])))
        R = SimpleNamespace(**dict(zip(names, rest[nw + len(on) :])))
        if tight(cfg):
            R.bp = R.cot_all
        wogs = body_fwd(cfg, dims, tok, cot, rest[:nw], wo, step, flat, R)
        body_bwd(cfg, dims, tok, cot, wogs, R, O)

    v = pl.BlockSpec(memory_space=pltpu.VMEM)
    hbm = pl.BlockSpec(memory_space=pl.ANY)
    res = pl.pallas_call(
        kern,
        out_shape=[outs[n] for n in on],
        in_specs=[v, v, hbm, v] + [v] * nf + [hbm] * nw,
        out_specs=[v, v] + [hbm] * (len(on) - 2),
        scratch_shapes=[scratch[n] for n in names],
        compiler_params=pltpu.CompilerParams(
            collective_id=0, has_side_effects=True, vmem_limit_bytes=VMEM_LIMIT
        ),
    )(tokens[0], cotangent[0], wo, step_weight.T, *flat, *wsrc)
    G = SimpleNamespace(**dict(zip(on, res)))
    pieces = cols // cr
    steps = per * pieces
    rows = Dl // steps
    cl, gl, hl = (inner + 2 * N) // F, inner // F, heads // F

    def whole(*shape):
        return pl.BlockSpec(shape, lambda i: (0,) * len(shape))

    def out(*shape):
        return jax.ShapeDtypeStruct(shape, f32)

    through = [G.block, G.input] if T % (16 * steps) == 0 else []
    tok_rows = [pl.BlockSpec((T // steps, D), lambda i: (i, 0)) for _ in through]
    joined = pl.pallas_call(
        lambda *refs: assemble(cfg, dims, *refs),
        grid=(steps,),
        out_shape=[
            out(Dl, 2 * inner + 2 * N), out(heads, Dl), out(4, cl), out(cl), out(gl),
            out(Dl), out(hl), out(hl), out(hl), out(per * cols, D),
        ]
        + [jax.ShapeDtypeStruct(a.shape, a.dtype) for a in through],
        in_specs=[
            pl.BlockSpec((S, rows, cp), lambda i: (0, i, 0)),
            pl.BlockSpec((nt, S, rows, 128), lambda i: (0, 0, i, 0)),
            pl.BlockSpec((rows, 2 * N), lambda i: (i, 0)),
            pl.BlockSpec((1, 1, cr, D), lambda i: (lax.rem(i, pieces), i // pieces, 0, 0)),
            whole(S, 16, D),
        ]
        + tok_rows,
        out_specs=[
            pl.BlockSpec((rows, 2 * inner + 2 * N), lambda i: (i, 0)),
            whole(heads, Dl), whole(4, cl), whole(cl), whole(gl), whole(Dl), whole(hl),
            whole(hl), whole(hl),
            pl.BlockSpec((cr, D), lambda i: (i, 0)),
        ]
        + tok_rows,
    )(G.gz, G.gx, G.gbc.reshape(Dl, 2 * N), G.go, G.sm, *through)
    win, stepg, conv, bias, gate, norm, hd0, hd1, hd2, wout = joined[:10]
    block, grad = joined[10:] if through else (G.block, G.input)
    return (
        block[None],
        grad[None],
        win,
        stepg.T,
        conv,
        bias,
        hd0,
        hd1,
        hd2,
        gate,
        norm,
        wout,
    )


def solution(mesh):
    row = P("fsdp", None)
    tok = P("fsdp", "seq", None)
    one = P("fsdp")
    return jax.shard_map(
        shards,
        mesh=mesh,
        in_specs=(tok, row, row, P(None, "fsdp"), one, one, one, one, one, one, row, tok),
        out_specs=(tok, tok, row, row, P(None, "fsdp"), one, one, one, one, one, one, row),
        check_vma=False,
    )
```

```python
from types import SimpleNamespace

import jax
import jax.numpy as jnp
from jax import lax
from jax.experimental import pallas as pl
from jax.experimental.pallas import tpu as pltpu
from jax.sharding import PartitionSpec as P

N = 128
HEAD = 64
Q = 128
epsilon = 1e-05
bf16 = jnp.bfloat16
f32 = jnp.float32
MESH = pl.DeviceIdType.MESH
HI = lax.Precision.HIGHEST
VMEM_LIMIT = 64 * 1024 * 1024 - 65536


def mm(a, b, da=1, db=0, precision=None):
    return lax.dot_general(
        a, b, (((da,), (db,)), ((), ())), preferred_element_type=f32, precision=precision
    )


def rcopy(src, dst, ss, rs, **dev):
    return pltpu.make_async_remote_copy(
        src_ref=src, dst_ref=dst, send_sem=ss, recv_sem=rs, device_id=dev, device_id_type=MESH
    )


class Axis:
    def __init__(self, name, outer, inner):
        self.name, self.outer, self.inner = name, outer, inner
        self.me = lax.axis_index(name)
        self.o = self.me // inner
        self.i = lax.rem(self.me, inner)

    def near(self, k):
        half = self.outer // 2
        side = self.o // half
        m = self.o + side * (self.outer - 1 - 2 * self.o)
        at = jnp.where(k == 0, m, k - m * ((3 - k) // 2))
        return at + side * (self.outer - 1 - 2 * at)

    def blk(self, k, q):
        return self.near(k) * self.inner + lax.rem(self.i + q, self.inner)

    def to(self, d):
        return {self.name: d}


class Place:
    def __init__(self, S, F):
        self.S, self.F = S, F
        self.seq = Axis("seq", 4, S // 4)
        self.fsdp = Axis("fsdp", F // 2, 2)
        self.Z, self.X = 4, S // 4
        self.s, self.z, self.x = self.seq.me, self.seq.o, self.seq.i
        self.f = self.fsdp.me
        self.blk = self.seq.blk

    def barrier(self):
        bar = pltpu.get_barrier_semaphore()
        n = 0
        for k in range(1, self.S):
            pl.semaphore_signal(
                bar, inc=1, device_id={"seq": lax.rem(self.s + k, self.S)}, device_id_type=MESH
            )
            n += 1
        for k in range(1, self.F):
            pl.semaphore_signal(
                bar, inc=1, device_id={"fsdp": lax.rem(self.f + k, self.F)}, device_id_type=MESH
            )
            n += 1
        pl.semaphore_wait(bar, n)


class Gather:
    def __init__(self, ax, src, buf, sems, cut=None):
        self.ax, self.src, self.buf, self.cut = ax, src, buf, cut
        self.ss, self.rs = sems

    def at(self, b):
        return self.buf.at[b] if self.cut is None else self.buf.at[b, self.cut]

    def send(self, src, b, sem, dst):
        rcopy(src, self.at(b), self.ss.at[sem], self.rs.at[b], **self.ax.to(dst)).start()

    def start(self):
        ax = self.ax
        for sem, d in ((0, 1), (1, -1)):

            @pl.when(jnp.logical_and(ax.o + d >= 0, ax.o + d < ax.outer))
            def _():
                self.send(self.src, ax.me, sem, ax.me + d * ax.inner)

        self.across(self.src, ax.me, 0)

    def across(self, src, b, k):
        ax = self.ax
        for q in range(1, ax.inner):
            sem = ax.outer + 1 + k * (ax.inner - 1) + q - 1
            self.send(src, b, sem, ax.o * ax.inner + lax.rem(ax.i + q, ax.inner))

    def onward(self, k):
        ax = self.ax
        return ax.o + jnp.where(ax.o > ax.near(k), 1, -1)

    def relay(self, k):
        ax = self.ax
        b = ax.blk(k, 0)
        self.wait(b)
        nxt = self.onward(k)

        @pl.when(jnp.logical_and(nxt >= 0, nxt < ax.outer))
        def _():
            self.send(self.at(b), b, 1 + k, nxt * ax.inner + ax.i)

        self.across(self.at(b), b, k)

    def wait(self, b):
        r = self.at(b)
        rcopy(r, r, self.ss.at[0], self.rs.at[b], **self.ax.to(self.ax.me)).wait_recv()

    def wait_across(self):
        for k in range(self.ax.outer):
            for q in range(1, self.ax.inner):
                self.wait(self.ax.blk(k, q))

    def drain(self):
        ax = self.ax

        def done(sem):
            rcopy(
                self.src, self.src, self.ss.at[sem], self.rs.at[0], **ax.to(ax.me)
            ).wait_send()

        for sem, d in ((0, 1), (1, -1)):

            @pl.when(jnp.logical_and(ax.o + d >= 0, ax.o + d < ax.outer))
            def _():
                done(sem)

        for k in range(1, ax.outer):
            nxt = self.onward(k)

            @pl.when(jnp.logical_and(nxt >= 0, nxt < ax.outer))
            def _():
                done(1 + k)

        for sem in range(ax.outer * (ax.inner - 1)):
            done(ax.outer + 1 + sem)


class Halves:
    def __init__(self, ax, src, buf, sems):
        n = src.shape[0] // 2
        self.parts = []
        for h in range(2):
            cut = pl.ds(n * h, n)
            self.parts.append(
                Gather(ax, src.at[cut], buf, (sems[0].at[h], sems[1].at[h]), cut)
            )

    def start(self):
        for g in self.parts:
            g.start()

    def relay(self, k, ends=None):
        for g in self.parts:
            if ends is None:
                g.relay(k)
                continue
            last = jnp.logical_or(g.ax.o == 0, g.ax.o == g.ax.outer - 1)

            @pl.when(last if ends else jnp.logical_not(last))
            def _():
                g.relay(k)

    def wait(self, b):
        for g in self.parts:
            g.wait(b)

    def drain(self):
        for g in self.parts:
            g.drain()


def gather_sems(outer, inner):
    sem = pltpu.SemaphoreType.DMA
    return sem((outer + 1 + outer * (inner - 1),)), sem((outer * inner,))


def pair(col, p):
    lane = lax.broadcasted_iota(jnp.int32, (col.shape[0], 128), 1)
    return jnp.where(lane < HEAD, col[:, 2 * p : 2 * p + 1], col[:, 2 * p + 1 : 2 * p + 2])


def spread(col, cp):
    return jnp.concatenate([pair(col, p) for p in range(cp // 128)], axis=1)


def row_sums(v):
    part = v[:, :128]
    for p in range(1, v.shape[1] // 128):
        part = part + v[:, 128 * p : 128 * p + 128]
    return jnp.sum(part.T, axis=0, keepdims=True)


def sigmoid(v):
    return 1.0 / (1.0 + jnp.exp(-v))


def softplus(v):
    return jnp.maximum(v, 0.0) + jnp.log1p(jnp.exp(-jnp.abs(v)))


def tri(shape, flip=False):
    i = lax.broadcasted_iota(jnp.int32, shape, 0)
    j = lax.broadcasted_iota(jnp.int32, shape, 1)
    return j >= i if flip else i >= j


def split(x2):
    lane = lax.broadcasted_iota(jnp.int32, x2.shape, 1)
    return jnp.concatenate([jnp.where(lane < HEAD, x2, 0), jnp.where(lane >= HEAD, x2, 0)], axis=0)


def chunk_inputs(c, ext, rawb, small, cp):
    r0 = pl.multiple_of(c * Q, Q)
    v = ext[pl.ds(r0, Q + 16), :].astype(f32)
    C = cp + 2 * N
    taps = [pltpu.roll(v, 3 - k, 0)[16:] if k < 3 else v[16:] for k in range(4)]
    summed = small[4:5, :C]
    for k in range(4):
        summed = summed + small[k : k + 1, :C] * taps[k]
    sig = sigmoid(summed)
    raw = rawb[pl.ds(r0, Q), :].astype(f32) + small[7:8, 0:128]
    dt = softplus(raw)
    rate = -jnp.exp(small[7:8, 128:256])
    cum = mm(tri((Q, Q)).astype(f32), dt * rate, precision=HI)
    return taps, summed, sig, raw, dt, rate, cum


def skip_row(small, cp):
    return spread(small[7:8, 256:384], cp)


def tight(cfg):
    S, F, T, D, cp, WC = cfg
    return S * T * D * 2 > 2**22


def lanes_from(row, shift, width, size):
    n = row.shape[1]
    if n < width:
        row = jnp.concatenate([row, jnp.zeros((row.shape[0], width - n), f32)], axis=1)
    row = pltpu.roll(row, lax.rem(shift + width, width), 1)
    return row[:, :size]


def small_rows(cfg, dims, flat, pc):
    S, F, T, D, cp, WC = cfg
    inner, heads, cols = dims
    conv = inner + 2 * N
    cl, gl, nl, hl = conv // F, inner // F, D // F, heads // F
    def line(v):
        v = v[...].astype(f32)
        v = v if v.ndim == 2 else v[None]
        n = -v.shape[1] % 128
        return jnp.concatenate([v, jnp.zeros((v.shape[0], n), f32)], axis=1) if n else v

    parts = [line(v) for v in flat]
    rows = jnp.concatenate(parts[:2] + [jnp.zeros((3, parts[0].shape[1]), f32)], axis=0)
    lane = lax.broadcasted_iota(jnp.int32, (8, cp), 1)
    xs = lanes_from(rows, cl * pc.f - cols * pc.s, conv, cp)
    bc = lanes_from(rows, cl * pc.f - inner, conv, 2 * N)
    gate = lanes_from(parts[2], gl * pc.f - cols * pc.s, inner, cp)
    if cols < cp:
        xs = jnp.where(lane < cols, xs, 0.0)
        gate = jnp.where(lane[0:1] < cols, gate, 0.0)
    norm = lanes_from(parts[3], nl * pc.f, D, D)
    hg = heads // S
    hv = jnp.concatenate(parts[4:7] + [jnp.zeros((5, 128), f32)], axis=0)
    hv = lanes_from(hv, hl * pc.f - hg * pc.s, 128, 128)
    hv = jnp.where(lane[:, :128] < hg, hv, 0.0)

    def wide(v):
        return jnp.concatenate([v, jnp.zeros((v.shape[0], D - v.shape[1]), f32)], axis=1)

    return jnp.concatenate(
        [
            wide(jnp.concatenate([xs, bc], axis=1)[0:5]),
            wide(gate),
            norm,
            wide(jnp.concatenate([hv[0:1], hv[1:2], hv[2:3]], axis=1)),
        ],
        axis=0,
    )


def body_fwd(cfg, dims, tok, cot, wsrc, wo, step, flat, R):
    S, F, T, D, cp, WC = cfg
    inner, heads, cols = dims
    L = S * T
    C = cp + 2 * N
    per = S // F
    pc = Place(S, F)
    own = R.w_all.at[pc.f]
    hg = heads // S
    up = -(-heads // 8) * 8
    st = step[...].astype(f32)
    if up > heads:
        st = jnp.concatenate([st, jnp.zeros((up - heads, st.shape[1]), f32)], axis=0)
    st = pltpu.roll(st, lax.rem(up - hg * pc.s, up), 0)[:8].T
    lane = lax.broadcasted_iota(jnp.int32, st.shape, 1)
    st = jnp.where(lane < hg, st, 0.0)
    st = jnp.concatenate([st, jnp.zeros((st.shape[0], 120), f32)], axis=1).astype(bf16)
    R.w_all[pc.f, :, 2 * cp + 2 * N :] = st
    if cols < cp:
        parts = [(wsrc[0], own.at[:, pl.ds(0, 2 * cp + 2 * N)])]
    else:
        (win,) = wsrc
        col = pl.multiple_of(pc.s * cols, cols)
        parts = [
            (win.at[:, pl.ds(col, cols)], own.at[:, pl.ds(0, cols)]),
            (win.at[:, pl.ds(inner + col, cols)], own.at[:, pl.ds(cols, cols)]),
            (win.at[:, pl.ds(2 * inner, 2 * N)], own.at[:, pl.ds(2 * cols, 2 * N)]),
        ]
    parts = [pltpu.make_async_copy(a, b, R.wsem.at[i]) for i, (a, b) in enumerate(parts)]
    for c in parts:
        c.start()
    R.sm_own[...] = small_rows(cfg, dims, flat, pc)
    pc.barrier()
    tg = Halves(pc.seq, tok, R.tok_all, (R.ss_t, R.rs_t))
    cg = Halves(pc.seq, cot, R.cot_all, (R.ss_c, R.rs_c))
    wg = Gather(pc.fsdp, own, R.w_all, (R.ss_w, R.rs_w))
    first = lax.rem(pc.s, per)
    owner = pc.s // per
    wogs = []
    if not tight(cfg):
        for p in range(per):
            at = lax.rem(first + p, per)
            wogs.append(
                Gather(pc.fsdp, wo.at[at], R.w_out.at[at], (R.ss_o.at[p], R.rs_o.at[p]))
            )
    sm = R.sm_own
    tg.start()
    for k in range(1, F):
        to = lax.rem(pc.f + k, F)
        rcopy(sm, R.sm_all.at[pc.f], R.ss_m.at[k], R.rs_m.at[pc.f], fsdp=to).start()
    for c in parts:
        c.wait()
    wg.start()
    keep = []
    for p in range(len(wogs)):
        wogs[p].start()
        at = lax.rem(first + p, per)
        keep.append(pltpu.make_async_copy(wo.at[at], R.w_out.at[at, pc.f], R.osem.at[p]))
    if tight(cfg):
        keep.append(pltpu.make_async_copy(wo, R.wo_g, R.osem.at[0]))

        @pl.when(pc.f == owner)
        def _():
            keep[0].start()
            for k in range(1, F):
                to = lax.rem(pc.f + k, F)
                rcopy(wo, R.wo_g, R.ss_o.at[k], R.rs_o.at[0], fsdp=to).start()
    else:
        for c in keep:
            c.start()
    R.tok_all[pc.s] = tok[...]
    R.cot_all[pc.s] = cot[...]
    R.sm_all[pc.f] = sm[...]
    R.ext[0:16, :] = jnp.zeros((16, C), bf16)
    for k in range(1, F):
        o = lax.rem(pc.f + k, F)
        rcopy(sm, R.sm_all.at[o], R.ss_m.at[0], R.rs_m.at[o], fsdp=pc.f).wait_recv()
    total = R.sm_all[0]
    for k in range(1, F):
        total = total + R.sm_all[k]
    R.small[...] = total
    small = R.small
    tg.relay(1)
    tg.relay(2)
    tg.relay(3, False)
    for k in range(1, F // 2):
        wg.relay(k)
    tg.relay(3, True)
    cg.start()
    wg.wait_across()

    def project(j, carry):
        k, q = j // pc.X, lax.rem(j, pc.X)
        b = pc.blk(k, q)

        @pl.when(q > 0)
        def _():
            tg.wait(b)

        @pl.when(j == S // 2)
        def _():
            cg.relay(1)

        r = R.tok_all[b].astype(f32)
        scale = lax.rsqrt(jnp.mean(r * r, axis=1, keepdims=True) + epsilon)
        h = r * scale * small[6:7, :]
        r0 = pl.multiple_of(b * T, T)
        R.hid_t[:, pl.ds(r0, T)] = h.T.astype(bf16)
        out = mm(h.astype(bf16), R.w_all[...].reshape(D, WC)).astype(bf16)
        R.zb[pl.ds(r0, T), :] = out[:, :cp]
        R.rawb[pl.ds(r0, T), :] = out[:, 2 * cp + 2 * N :]
        R.ext[pl.ds(r0 + 16, T), :] = out[:, cp : 2 * cp + 2 * N]
        return carry

    lax.fori_loop(0, S, project, 0)
    R.state[...] = jnp.zeros((N, cp), f32)

    def forward(c, carry):
        @pl.when(jnp.logical_or(c == 0, c == 5))
        def _():
            cg.relay(2 + c // 5)

        r0 = pl.multiple_of(c * Q, Q)
        taps, summed, sig, raw, dt, rate, cum = chunk_inputs(c, R.ext, R.rawb, small, cp)
        act = summed * sig
        x = act[:, :cp]
        bb = act[:, cp : cp + N].astype(bf16)
        cb = act[:, cp + N :].astype(bf16)
        cum_t = cum.T
        dt_t = dt.T
        scores = mm(cb, bb, 1, 1)
        causal = tri((Q, Q))
        parts = []
        for p in range(cp // 128):
            mix = []
            for h in (2 * p, 2 * p + 1):
                gap = jnp.where(causal, cum[:, h : h + 1] - cum_t[h : h + 1, :], -1e30)
                mix.append((jnp.exp(gap) * scores * dt_t[h : h + 1, :]).astype(bf16))
            parts.append(
                mm(jnp.concatenate(mix, axis=1), split(x[:, 128 * p : 128 * p + 128]).astype(bf16))
            )
        state = R.state[...]
        R.states[c] = state
        last = cum[Q - 1 : Q, :]
        y = jnp.concatenate(parts, axis=1) + mm(cb, state.astype(bf16)) * spread(jnp.exp(cum), cp)
        y = y + skip_row(small, cp) * x
        wx = (spread(jnp.exp(last - cum) * dt, cp) * x).astype(bf16)
        R.state[...] = spread(jnp.exp(last), cp) * state + mm(bb, wx, 0, 0)
        R.y[pl.ds(r0, Q), :] = y
        z = R.zb[pl.ds(r0, Q), :].astype(f32)
        gated = (y * (z * sigmoid(z))).astype(bf16)
        R.dpx[pl.ds(r0, Q), :cp] = gated
        g32 = gated.astype(f32)
        R.st[0:1, pl.ds(r0, Q)] = row_sums(g32 * g32)
        return carry

    lax.fori_loop(0, L // Q, forward, 0)

    if tight(cfg):
        group = R.wo_g

        @pl.when(pc.f != owner)
        def _():
            rcopy(wo, R.wo_g, R.ss_o.at[0], R.rs_o.at[0], fsdp=pc.f).wait_recv()

        @pl.when(pc.f == owner)
        def _():
            keep[0].wait()
    else:
        group = R.w_out.at[first, owner]
        for c in keep:
            c.wait()
        for k in range(1, F // 2):
            wogs[0].relay(k)
        wogs[0].wait_across()

    def mixed(j, carry):
        k, q = j // pc.X, lax.rem(j, pc.X)
        b = pc.blk(k, q)

        @pl.when(q > 0)
        def _():
            cg.wait(b)

        r0 = pl.multiple_of(b * T, T)
        mg = mm(R.cot_all[b], group[...], 1, 1)
        R.mg[pl.ds(r0, T), :] = mg
        g = mg * small[5:6, :cp] * R.dpx[pl.ds(r0, T), :cp].astype(f32)
        R.st[1:2, pl.ds(r0, T)] = row_sums(g)
        return carry

    lax.fori_loop(0, S, mixed, 0)
    for k in range(1, S):
        rcopy(
            R.st, R.st_all.at[pc.s], R.ss_s.at[k], R.rs_s.at[pc.s],
            seq=lax.rem(pc.s + k, S),
        ).start()
    R.st_all[pc.s] = R.st[...]
    for k in range(1, S):
        o = lax.rem(pc.s + k, S)
        rcopy(R.st, R.st_all.at[o], R.ss_s.at[0], R.rs_s.at[o], seq=pc.s).wait_recv()
    total = R.st_all[0]
    for k in range(1, S):
        total = total + R.st_all[k]
    R.stats[...] = total

    for g in [tg, cg, wg]:
        g.drain()
    for k in range(1, S):
        rcopy(R.st, R.st, R.ss_s.at[k], R.rs_s.at[0], seq=pc.s).wait_send()
    for k in range(1, F):
        rcopy(sm, sm, R.ss_m.at[k], R.rs_m.at[0], fsdp=pc.f).wait_send()
    if tight(cfg):

        @pl.when(pc.f == owner)
        def _():
            for k in range(1, F):
                rcopy(wo, wo, R.ss_o.at[k], R.rs_o.at[0], fsdp=pc.f).wait_send()

    return wogs


def fwd_scratch(cfg):
    S, F, T, D, cp, WC = cfg
    L = S * T
    Dl = D // F
    C = cp + 2 * N
    V = pltpu.VMEM
    sem = pltpu.SemaphoreType.DMA
    per = S // F
    seq = gather_sems(4, S // 4)
    fsdp = gather_sems(F // 2, 2)
    out = SimpleNamespace(
        tok_all=V((S, T, D), bf16),
        cot_all=V((S, T, D), bf16),
        w_all=V((F, Dl, WC), bf16),
        sm_own=V((8, D), f32),
        sm_all=V((F, 8, D), f32),
        small=V((8, D), f32),
        hid_t=V((D, L), bf16),
        zb=V((L, cp), bf16),
        rawb=V((L, 128), bf16),
        ext=V((16 + L, C), bf16),
        state=V((N, cp), f32),
        states=V((L // Q, N, cp), f32),
        y=V((L, cp), f32),
        mg=V((L, cp), f32),
        st=V((2, L), f32),
        st_all=V((S, 2, L), f32),
        stats=V((2, L), f32),
        ss_t=sem((2,) + seq[0].shape),
        rs_t=sem((2,) + seq[1].shape),
        ss_c=sem((2,) + seq[0].shape),
        rs_c=sem((2,) + seq[1].shape),
        ss_w=fsdp[0],
        rs_w=fsdp[1],
        ss_m=sem((F,)),
        rs_m=sem((F,)),
        wsem=sem((4,)),
        osem=sem((per,)),
        ss_s=sem((S,)),
        rs_s=sem((S,)),
    )
    if tight(cfg):
        out.wo_g = V((cp, D), bf16)
        out.ss_o = out.rs_o = sem((F,))
    else:
        out.w_out = V((per, F, cp, D), bf16)
        out.ss_o = sem((per,) + fsdp[0].shape)
        out.rs_o = sem((per,) + fsdp[1].shape)
    return out


class Scatter:
    def __init__(self, pc, part, rx, rz, rn, sems):
        self.pc, self.part, self.rx, self.rz, self.rn = pc, part, rx, rz, rn
        self.ssx, self.rsx, self.ssz, self.rsz, self.rsn = sems
        self.near = jnp.logical_or(pc.z == 1, pc.z == 2)

    @staticmethod
    def sems(S):
        sem = pltpu.SemaphoreType.DMA
        return sem((S,)), sem((4, S // 4 - 1)), sem((4,)), sem((2,)), sem((2,))

    def got(self, ref, sem):
        rcopy(ref, ref, sem, sem, seq=self.pc.s).wait_recv()

    def across(self, b):
        pc = self.pc
        zb, xb = b // pc.X, lax.rem(b, pc.X)

        @pl.when(xb != pc.x)
        def _():
            slot = lax.rem(pc.x - xb - 1 + pc.X, pc.X)
            rcopy(
                self.part.at[b], self.rx.at[zb, slot], self.ssx.at[b], self.rsx.at[zb, slot],
                seq=pc.z * pc.X + xb,
            ).start()

    def other(self, zb):
        return zb // 2 != self.pc.z // 2

    def column(self, zb):
        pc = self.pc
        b = zb * pc.X + pc.x
        total = self.part[b].astype(f32)
        for q in range(pc.X - 1):
            self.got(self.rx.at[zb, q], self.rsx.at[zb, q])
            total = total + self.rx[zb, q].astype(f32)
        self.part[b] = total.astype(bf16)

        @pl.when(jnp.logical_and(zb != pc.z, jnp.logical_not(self.other(zb))))
        def _():
            rcopy(
                self.part.at[b], self.rz.at[0], self.ssz.at[zb], self.rsz.at[0], seq=b
            ).start()

        @pl.when(jnp.logical_and(self.other(zb), jnp.logical_not(self.near)))
        def _():
            slot = lax.rem(zb, 2)
            rcopy(
                self.part.at[b], self.rn.at[slot], self.ssz.at[zb], self.rsn.at[slot],
                seq=(pc.z + 1 - 2 * lax.rem(pc.z, 2)) * pc.X + pc.x,
            ).start()

    def merge(self, zb):
        pc = self.pc

        @pl.when(jnp.logical_and(self.other(zb), self.near))
        def _():
            b = zb * pc.X + pc.x
            slot = lax.rem(zb, 2)
            self.got(self.rn.at[slot], self.rsn.at[slot])
            total = self.part[b].astype(f32) + self.rn[slot].astype(f32)
            self.part[b] = total.astype(bf16)
            rcopy(
                self.part.at[b], self.rz.at[1], self.ssz.at[zb], self.rsz.at[1], seq=b
            ).start()

    def total(self):
        out = self.part[self.pc.s].astype(f32)
        for q in range(2):
            self.got(self.rz.at[q], self.rsz.at[q])
            out = out + self.rz[q].astype(f32)
        return out

    def drain(self):
        pc = self.pc
        r = self.rz.at[0]
        for b in range(pc.S):

            @pl.when(b % pc.X != pc.x)
            def _():
                rcopy(r, r, self.ssx.at[b], self.rsz.at[0], seq=pc.s).wait_send()

        for zb in range(pc.Z):

            @pl.when(zb != pc.z)
            def _():
                rcopy(r, r, self.ssz.at[zb], self.rsz.at[0], seq=pc.s).wait_send()


class Shared:
    def __init__(self, pc, part, recv, ss, rs):
        self.pc, self.part, self.recv, self.ss, self.rs = pc, part, recv, ss, rs

    def send(self, k):
        pc = self.pc
        to = lax.rem(pc.f + k, pc.F)
        rcopy(
            self.part.at[to], self.recv.at[k - 1], self.ss.at[k - 1], self.rs.at[k - 1], fsdp=to
        ).start()

    def total(self):
        pc = self.pc
        out = self.part[pc.f].astype(f32)
        for k in range(1, pc.F):
            r = self.recv.at[k - 1]
            rcopy(r, r, self.ss.at[k - 1], self.rs.at[k - 1], fsdp=pc.f).wait_recv()
            out = out + self.recv[k - 1].astype(f32)
        return out

    def drain(self):
        for k in range(1, self.pc.F):
            r = self.recv.at[k - 1]
            rcopy(r, r, self.ss.at[k - 1], self.rs.at[k - 1], fsdp=self.pc.f).wait_send()


def body_bwd(cfg, dims, tok, cot, wogs, R, O):
    S, F, T, D, cp, WC = cfg
    inner = float(dims[0])
    L = S * T
    C = cp + 2 * N
    Dl = D // F
    nc = L // Q
    cr = cp // F
    per = S // F
    bh = Dl // S
    pc = Place(S, F)
    small = R.small
    if tight(cfg):
        blk = Scatter(pc, R.bp, R.brx, R.brz, R.brn, (R.bs0, R.bs1, R.bs2, R.bs3, R.bs4))
    hid = Scatter(pc, R.tok_all, R.hrx, R.hrz, R.hrn, (R.hs0, R.hs1, R.hs2, R.hs3, R.hs4))
    zs = Shared(pc, R.zp, R.zr, R.zs0, R.zs1)
    os_ = Shared(pc, R.op, R.orecv, R.os0, R.os1)
    nt = cp // 128

    def xs(t):
        return Shared(pc, R.xp.at[t], R.xr.at[t], R.xs0.at[t], R.xs1.at[t])

    def xg(t):
        return Gather(pc.seq, R.xred.at[t], O.gx.at[t], (R.gx0.at[t], R.gx1.at[t]))

    def own_x(t):
        return pltpu.make_async_copy(R.xred.at[t], O.gx.at[t, pc.s], R.xsem.at[t])

    def settle(t):
        R.xred[t] = xs(t).total().astype(bf16)
        xg(t).start()
        own_x(t).start()
    bs = Shared(pc, R.cp_, R.cr_, R.cs0, R.cs1)
    zg = Gather(pc.seq, R.zred, O.gz, (R.gz0, R.gz1))
    og = Gather(pc.seq, R.ored, O.go_s, (R.go0, R.go1))
    sg = Gather(pc.seq, R.asum, O.sm, (R.as2, R.as3))

    def direct(src, dst, ss, rs, to):
        rcopy(src, dst.at[pc.s], ss.at[to], rs.at[pc.s], seq=to).start()

    def arrived(dst, ss, rs):
        for k in range(1, S):
            o = lax.rem(pc.s + k, S)
            r = dst.at[o]
            rcopy(r, r, ss.at[0], rs.at[o], seq=pc.s).wait_recv()

    def sent(src, ss, rs):
        for k in range(1, S):
            rcopy(src, src, ss.at[lax.rem(pc.s + k, S)], rs.at[0], seq=pc.s).wait_send()

    def own(src, dst, i):
        return pltpu.make_async_copy(src, dst, R.lsem.at[i])

    gate = small[5:6, :cp]
    R.acc[...] = jnp.zeros((16, D), f32)
    R.hacc[...] = jnp.zeros((2, 8, 128), f32)
    R.dstate[...] = jnp.zeros((N, cp), f32)
    R.head[...] = jnp.zeros((8, C), f32)

    def first(i, carry):
        c = lax.rem(pc.s + 1 + i, nc)
        r0 = pl.multiple_of(c * Q, Q)
        rows = pl.ds(r0, Q)
        st = jnp.concatenate([R.stats[:, rows], jnp.zeros((6, Q), f32)], axis=0).T
        scale = lax.rsqrt(st[:, 0:1] / inner + epsilon)
        mean = st[:, 1:2] / inner
        gated = R.dpx[rows, :cp].astype(f32)
        mg = R.mg[rows, :]
        ng = gated * scale
        mn = ng * gate
        R.acc[5:6, :cp] += jnp.sum(mg * ng, axis=0, keepdims=True)
        gg = (scale * (mg * gate) - scale * scale * scale * gated * mean).astype(bf16).astype(f32)
        z = R.zb[rows, :].astype(f32)
        sz = sigmoid(z)
        R.zb[rows, :] = (gg * R.y[rows, :] * (sz * (1.0 + z * (1.0 - sz)))).astype(bf16)
        R.mg[rows, :] = gg * (z * sz)
        R.mn_t[:, rows] = mn.T.astype(bf16)
        if tight(cfg):
            R.dpx[rows, :cp] = mn.astype(bf16)
        else:
            R.mn[c] = mn.astype(bf16)

            @pl.when(c != pc.s)
            def _():
                direct(R.mn.at[c], R.mall, R.ms0, R.ms1, c)

        return carry

    def block(i, carry):
        c = nc - 1 - i
        rows = pl.ds(pl.multiple_of(c * Q, Q), Q)
        R.bp[c] = mm(R.dpx[rows, :cp], R.wo_g[...]).astype(bf16)
        blk.across(c)
        return carry

    lax.fori_loop(0, nc, first, 0)

    def zpart(k, carry):
        to = lax.rem(pc.f + k, F)
        rows = pl.ds(pl.multiple_of(to * Dl, Dl), Dl)
        R.zp[to] = mm(R.hid_t[rows, :], R.zb[...]).astype(bf16)

        @pl.when(k < F)
        def _():
            rcopy(
                R.zp.at[to], R.zr.at[k - 1], R.zs0.at[k - 1], R.zs1.at[k - 1], fsdp=to
            ).start()
        return carry

    lax.fori_loop(1, F + 1, zpart, 0)
    W = 384

    def opart(j, carry):
        cols = pl.ds(pl.multiple_of(j * W, W), W)
        a = R.cot_all[:, :, cols].reshape(L, W)
        R.op[:, :, cols] = mm(R.mn_t[...], a).reshape(F, cr, W).astype(bf16)
        return carry

    lax.fori_loop(0, D // W, opart, 0)
    for g in wogs[1:]:
        for k in range(1, F // 2):
            g.relay(k)
    for k in range(1, F):
        os_.send(k)
    if tight(cfg):
        lax.fori_loop(0, nc, block, 0)

    sel = (
        lax.broadcasted_iota(jnp.int32, (8, cp), 1) // HEAD
        == lax.broadcasted_iota(jnp.int32, (8, cp), 0)
    ).astype(f32)
    sub = lax.broadcasted_iota(jnp.int32, (8, Q), 0)

    def scan(i, carry):
        c = nc - 1 - i
        r0 = pl.multiple_of(c * Q, Q)
        rows = pl.ds(r0, Q)

        if tight(cfg):

            @pl.when(i < pc.Z)
            def _():
                blk.column(pc.Z - 1 - i)

            @pl.when(jnp.logical_and(i >= pc.Z, i < 2 * pc.Z))
            def _():
                blk.merge(2 * pc.Z - 1 - i)

        @pl.when(i == 1)
        def _():
            R.zred[...] = zs.total().astype(bf16)
            zg.start()
            own(R.zred, O.gz.at[pc.s], 0).start()

        @pl.when(i == 4)
        def _():
            R.ored[...] = os_.total().astype(bf16)
            og.start()
            own(R.ored, O.go_s.at[pc.s], 5).start()

        @pl.when(jnp.logical_and(i >= 4, i < 4 + pc.Z - 1))
        def _():
            zg.relay(i - 3)

        @pl.when(i == 7)
        def _():
            og.relay(1)

        taps, summed, sig, raw, dt, rate, cum = chunk_inputs(c, R.ext, R.rawb, small, cp)
        act = summed * sig
        x = act[:, :cp]
        xb = x.astype(bf16)
        bb = act[:, cp : cp + N].astype(bf16)
        cb = act[:, cp + N :].astype(bf16)
        cum_t = cum.T
        dt_t = dt.T
        dy = R.mg[rows, :]
        dyb = dy.astype(bf16)
        last = cum[Q - 1 : Q, :]
        edy = spread(jnp.exp(cum), cp) * dy
        edyb = edy.astype(bf16)
        wdec = jnp.exp(last - cum)
        w = wdec * dt
        state = R.states[c]
        sb = state.astype(bf16)
        ds = R.dstate[...]
        dsb = ds.astype(bf16)
        ws = spread(w, cp)
        v = mm(bb, dsb)
        carr = mm(sel, edy * mm(cb, sb), 1, 1, HI)
        dw = mm(sel, x * v, 1, 1, HI)
        db = mm((ws * x).astype(bf16), dsb, 1, 1)
        dc = mm(edyb, sb, 1, 1)
        dlast = mm(sel, jnp.sum(state * ds, axis=0, keepdims=True), 1, 1, HI)
        R.dstate[...] = spread(jnp.exp(last), cp) * ds + mm(cb, edyb, 0, 0)
        scores = mm(bb, cb, 1, 1)
        seen = tri((Q, Q), True)
        dtb = dt_t[0:8].astype(bf16)
        dsc = jnp.zeros((Q, Q), f32)
        direct = jnp.zeros((8, Q), f32)
        onto = jnp.zeros((8, Q), f32)
        parts = []
        for p in range(cp // 128):
            cols = slice(128 * p, 128 * p + 128)
            g2 = mm(split(x[:, cols]).astype(bf16), dyb[:, cols], 1, 1)
            mix = []
            for h in (2 * p, 2 * p + 1):
                g = g2[:Q] if h % 2 == 0 else g2[Q:]
                decay = jnp.exp(jnp.where(seen, cum_t[h : h + 1, :] - cum[:, h : h + 1], -1e30))
                ls = decay * scores
                mix.append((ls * dt[:, h : h + 1]).astype(bf16))
                e = (g * ls).astype(bf16)
                dsc = dsc + g * decay * dt[:, h : h + 1]
                direct = direct + mm(jnp.where(sub == h, 1.0, 0.0).astype(bf16), e, 1, 1)
                onto = onto + mm(jnp.where(sub == h, dtb.astype(f32), 0.0).astype(bf16), e)
            parts.append(mm(jnp.concatenate(mix, axis=1), split(dy[:, cols]).astype(bf16)))
        dscb = dsc.astype(bf16)
        db = db + mm(dscb, cb)
        dc = dc + mm(dscb, bb, 0, 0)
        dx = skip_row(small, cp) * dy + ws * v + jnp.concatenate(parts, axis=1)
        R.acc[7:8, :cp] += jnp.sum(dy * x, axis=0, keepdims=True)
        dt_r = dt_t[0:8]
        wdec_r = wdec.T[0:8]
        w_r = wdec_r * dt_r
        rate_r = jnp.broadcast_to(rate, (128, 128)).T[0:8, 0:1]
        last_r = jnp.exp(cum_t[0:8, Q - 1 : Q])
        dcum = carr + onto - dtb.astype(f32) * direct - w_r * dw
        end = jnp.sum(w_r * dw, axis=1, keepdims=True) + last_r * dlast
        da = mm(dcum, tri((Q, Q)).astype(f32), precision=HI) + end
        ddt = direct + wdec_r * dw + rate_r * da
        draw = ddt * sigmoid(raw).T[0:8]
        R.hacc[0] += draw
        R.hacc[1] += da * dt_r * rate_r
        dact = jnp.concatenate([dx, db, dc], axis=1)
        dsum = dact * (sig * (1.0 + summed * (1.0 - sig)))
        full = jnp.concatenate([dsum, R.head[...]], axis=0)
        dxbc = jnp.zeros((Q, C), f32)
        for k in range(4):
            R.acc[k : k + 1, :C] += jnp.sum(dsum * taps[k], axis=0, keepdims=True)
            moved = pltpu.roll(full, Q + 8 - (3 - k), 0)[:Q] if k < 3 else dsum
            dxbc = dxbc + small[k : k + 1, :C] * moved
        R.acc[4:5, :C] += jnp.sum(dsum, axis=0, keepdims=True)
        R.head[...] = dsum[:8]
        R.dpx[rows, :C] = dxbc.astype(bf16)
        R.acc[8:16, :] += mm(draw.astype(bf16), R.hid_t[:, rows], 1, 1)
        pad = jnp.concatenate([draw, jnp.zeros((120, Q), f32)], axis=0).T
        R.dpx[rows, C:] = pad.astype(bf16)
        grad = jnp.concatenate([R.zb[rows, :], R.dpx[rows, :]], axis=1)
        hp = mm(grad, R.w_all[...].reshape(D, WC), 1, 1)
        r = R.tok_all[c].astype(f32)
        scale = lax.rsqrt(jnp.mean(r * r, axis=1, keepdims=True) + epsilon)
        R.acc[6:7, :] += jnp.sum(hp * r * scale, axis=0, keepdims=True)
        R.tok_all[c] = hp.astype(bf16)
        hid.across(c)
        return carry

    lax.fori_loop(0, nc, scan, 0)

    diag = lax.broadcasted_iota(jnp.int32, (8, 128), 0) == lax.broadcasted_iota(
        jnp.int32, (8, 128), 1
    )

    def along(v):
        return jnp.sum(jnp.where(diag, jnp.sum(v, axis=1, keepdims=True), 0.0), axis=0, keepdims=True)

    dskip = jnp.sum(
        jnp.where(diag, mm(sel, R.acc[7:8, :cp], 1, 1, HI), 0.0), axis=0, keepdims=True
    )
    R.acc[7:8, :] = jnp.concatenate(
        [along(R.hacc[0]), along(R.hacc[1]), dskip, jnp.zeros((1, D - 384), f32)], axis=1
    )
    R.accb[...] = R.acc[...].astype(bf16)
    for k in range(1, F):
        to = lax.rem(pc.f + k, F)
        rcopy(
            R.accb, R.ar.at[k - 1], R.as0.at[k - 1], R.as1.at[k - 1], fsdp=to
        ).start()

    for t in range(nt):

        def xpart(k, carry):
            to = lax.rem(pc.f + k, F)
            rows = pl.ds(pl.multiple_of(to * Dl, Dl), Dl)
            R.xp[t, to] = mm(R.hid_t[rows, :], R.dpx[:, 128 * t : 128 * t + 128]).astype(bf16)

            @pl.when(k < F)
            def _():
                rcopy(
                    R.xp.at[t, to], R.xr.at[t, k - 1], R.xs0.at[t, k - 1], R.xs1.at[t, k - 1],
                    fsdp=to,
                ).start()
            return carry

        lax.fori_loop(1, F + 1, xpart, 0)

    def lower(k, carry):
        to = lax.rem(pc.f + k, F)
        rows = pl.ds(pl.multiple_of(to * Dl, Dl), Dl)
        R.cp_[to] = mm(R.hid_t[rows, :], R.dpx[:, cp:C]).astype(bf16)

        @pl.when(k < F)
        def _():
            rcopy(
                R.cp_.at[to], R.cr_.at[k - 1], R.cs0.at[k - 1], R.cs1.at[k - 1], fsdp=to
            ).start()
        return carry

    lax.fori_loop(1, F + 1, lower, 0)
    def hid_column(i, carry):
        hid.column(pc.Z - 1 - i)
        return carry

    total = R.acc[...]
    for k in range(1, F):
        r = R.ar.at[k - 1]
        rcopy(r, r, R.as0.at[k - 1], R.as1.at[k - 1], fsdp=pc.f).wait_recv()
        total = total + R.ar[k - 1].astype(f32)
    R.asum[...] = total.astype(bf16)
    sg.start()
    own(R.asum, O.sm.at[pc.s], 1).start()
    og.relay(2)
    settle(0)
    og.relay(3)
    for t in range(1, nt):
        settle(t)
    low = bs.total()
    for g in range(S):
        R.cb[g] = low[g * bh : (g + 1) * bh].astype(bf16)
    for k in range(1, S):
        to = lax.rem(pc.s + k, S)
        direct(R.cb.at[to], R.cbr, R.cb0, R.cb1, to)
    lax.fori_loop(0, 2, hid_column, 0)
    sg.relay(1)
    for t in range(nt):
        xg(t).relay(1)
    mine = tok[...].astype(f32)
    if tight(cfg):
        O.block[...] = (mine + blk.total()).astype(bf16)
    else:
        for g in wogs[1:]:
            g.wait_across()
        arrived(R.mall, R.ms0, R.ms1)
        R.mall[pc.s] = R.mn[pc.s]
        R.total[...] = mine

        def add(g, carry):
            w = R.w_out[lax.rem(g, per), g // per]
            R.total[...] += mm(R.mall[g], w)
            return carry

        lax.fori_loop(0, S, add, 0)
        O.block[...] = R.total[...].astype(bf16)
    lax.fori_loop(2, pc.Z, hid_column, 0)
    for zb in (3, 2):
        hid.merge(zb)
    sg.relay(2)
    for t in range(nt):
        xg(t).relay(2)
    arrived(R.cbr, R.cb0, R.cb1)
    R.cbr[pc.s] = R.cb[pc.s]
    low = R.cbr[0].astype(f32)
    for g in range(1, S):
        low = low + R.cbr[g].astype(f32)
    R.cbd[...] = low.astype(bf16)
    for k in range(1, S):
        direct(R.cbd, O.gbc, R.cd0, R.cd1, lax.rem(pc.s + k, S))
    own(R.cbd, O.gbc.at[pc.s], 4).start()
    own(R.ored, O.go_s.at[pc.s], 5).wait()
    og.wait_across()
    for k in range(1, F):
        to = lax.rem(pc.f + k, F)
        rcopy(
            O.go_s.at[pl.ds(to * per, per)], O.go.at[pc.f], R.gs0.at[k], R.gs1.at[pc.f],
            fsdp=to,
        ).start()
    own(O.go_s.at[pl.ds(pc.f * per, per)], O.go.at[pc.f], 3).start()
    sg.relay(3)
    for t in range(nt):
        xg(t).relay(3)
    for zb in (1, 0):
        hid.merge(zb)

    scale = lax.rsqrt(jnp.mean(mine * mine, axis=1, keepdims=True) + epsilon)
    e = hid.total() * small[6:7, :]
    mean = jnp.mean(e * mine, axis=1, keepdims=True)
    O.input[...] = cot[...].astype(f32) + scale * e - scale * scale * scale * mine * mean

    zg.wait_across()
    for k in range(1, F):
        o = lax.rem(pc.f + k, F)
        r = O.go.at[o]
        rcopy(r, r, R.gs0.at[0], R.gs1.at[o], fsdp=pc.f).wait_recv()
    arrived(O.gbc, R.cd0, R.cd1)
    sg.wait_across()
    for t in range(nt):
        xg(t).wait_across()
        own_x(t).wait()
    own(R.zred, O.gz.at[pc.s], 0).wait()
    own(R.asum, O.sm.at[pc.s], 1).wait()
    own(O.go_s.at[pl.ds(pc.f * per, per)], O.go.at[pc.f], 3).wait()
    own(R.cbd, O.gbc.at[pc.s], 4).wait()
    if tight(cfg):
        blk.drain()
    else:
        sent(R.mn.at[0], R.ms0, R.ms1)
    sent(R.cb.at[0], R.cb0, R.cb1)
    sent(R.cbd, R.cd0, R.cd1)
    for a in [hid, zs, os_, bs, zg, og, sg] + wogs:
        a.drain()
    for t in range(nt):
        xs(t).drain()
        xg(t).drain()
    for k in range(1, F):
        r = R.ar.at[k - 1]
        rcopy(r, r, R.as0.at[k - 1], R.as1.at[0], fsdp=pc.f).wait_send()
        r = O.go.at[0]
        rcopy(r, r, R.gs0.at[k], R.gs1.at[0], fsdp=pc.f).wait_send()


def bwd_scratch(cfg):
    S, F, T, D, cp, WC = cfg
    L = S * T
    Dl = D // F
    C = cp + 2 * N
    Z, X = 4, S // 4
    cr = cp // F
    bh = Dl // S
    V = pltpu.VMEM
    sem = pltpu.SemaphoreType.DMA
    seq = gather_sems(4, S // 4)
    nt = cp // 128
    out = SimpleNamespace(
        acc=V((16, D), f32),
        asum=V((16, D), bf16),
        accb=V((16, D), bf16),
        ar=V((F - 1, 16, D), bf16),
        hacc=V((2, 8, 128), f32),
        dstate=V((N, cp), f32),
        head=V((8, C), f32),
        mn_t=V((cp, L), bf16),
        dpx=V((L, WC - cp), bf16),
        hrx=V((Z, X - 1, T, D), bf16),
        hrz=V((2, T, D), bf16),
        hrn=V((2, T, D), bf16),
        zp=V((F, Dl, cp), bf16),
        zr=V((F - 1, Dl, cp), bf16),
        zred=V((Dl, cp), bf16),
        op=V((F, cr, D), bf16),
        orecv=V((F - 1, cr, D), bf16),
        ored=V((cr, D), bf16),
        xp=V((nt, F, Dl, 128), bf16),
        xr=V((nt, F - 1, Dl, 128), bf16),
        xred=V((nt, Dl, 128), bf16),
        cp_=V((F, Dl, 2 * N), bf16),
        cr_=V((F - 1, Dl, 2 * N), bf16),
        cb=V((S, bh, 2 * N), bf16),
        cbr=V((S, bh, 2 * N), bf16),
        cbd=V((bh, 2 * N), bf16),
        lsem=sem((6,)),
        as0=sem((F,)), as1=sem((F,)), as2=seq[0], as3=seq[1],
        gs0=sem((F,)), gs1=sem((F,)), cs0=sem((F,)), cs1=sem((F,)),
        cb0=sem((S,)), cb1=sem((S,)), cd0=sem((S,)), cd1=sem((S,)),
        zs0=sem((F,)), zs1=sem((F,)), gz0=seq[0], gz1=seq[1],
        os0=sem((F,)), os1=sem((F,)), go0=seq[0], go1=seq[1],
        xs0=sem((nt, F)), xs1=sem((nt, F)), xsem=sem((nt,)),
        gx0=sem((nt,) + seq[0].shape), gx1=sem((nt,) + seq[1].shape),
    )
    out.hs0, out.hs1, out.hs2, out.hs3, out.hs4 = Scatter.sems(S)
    if tight(cfg):
        out.brx = V((Z, X - 1, T, D), bf16)
        out.brz = V((2, T, D), bf16)
        out.brn = V((2, T, D), bf16)
        out.bs0, out.bs1, out.bs2, out.bs3, out.bs4 = Scatter.sems(S)
    else:
        out.mn = V((S, T, cp), bf16)
        out.mall = V((S, T, cp), bf16)
        out.total = V((T, D), f32)
        out.ms0 = out.ms1 = sem((S,))
    return out


def assemble(cfg, dims, gz, gx, gbc, go, sm, *refs):
    S, F, T, D, cp, WC = cfg
    n = (len(refs) - 10) // 2
    for a, b in zip(refs[:n], refs[n + 10 :]):
        b[...] = a[...]
    win, step, conv, bias, gate, norm, h0, h1, h2, wout = refs[n : n + 10]
    inner, nheads, cols = dims
    for g in range(S):
        win[:, g * cols : (g + 1) * cols] = gz[g, :, :cols].astype(f32)
        for t in range(gx.shape[0]):
            n = min(128, cols - 128 * t)
            at = inner + g * cols + 128 * t
            win[:, at : at + n] = gx[t, g, :, :n].astype(f32)
    wout[...] = go[0, 0].astype(f32)
    C = cp + 2 * N
    hg = nheads // S
    Dl = D // F
    win[:, 2 * inner :] = gbc[...].astype(f32)

    @pl.when(pl.program_id(0) == 2)
    def _():
        f = lax.axis_index("fsdp")

        def mine(v, size):
            n = v.shape[1]
            return pltpu.roll(v, lax.rem(n - size * f, n), 1)[:, :size]

        v = [sm[g].astype(f32) for g in range(S)]
        total = v[0]
        for g in range(1, S):
            total = total + v[g]
        xs = jnp.concatenate([a[0:8, :cols] for a in v] + [total[0:8, cp:C]], axis=1)
        xs = mine(xs, (inner + 2 * N) // F)
        conv[...] = xs[0:4]
        bias[...] = xs[4]
        gate[...] = mine(jnp.concatenate([a[0:8, :cols] for a in v], axis=1), inner // F)[5]
        norm[...] = mine(total[0:8], Dl)[6]
        n = nheads // F
        zero = jnp.zeros((8, 128 - nheads), f32)
        for i, ref in enumerate((h0, h1, h2)):
            hs = [a[0:8, 128 * i : 128 * i + hg] for a in v]
            ref[...] = mine(jnp.concatenate(hs + [zero], axis=1), n)[7]
        step[...] = jnp.concatenate([mine(a[8:16], Dl)[:hg] for a in v], axis=0)


def shards(tokens, in_weight, step_weight, conv_kernel, conv_bias, step_bias, log_decay,
           skip_gain, gate_gain, norm_gain, out_weight, cotangent):
    S = lax.axis_size("seq")
    F = lax.axis_size("fsdp")
    _, T, D = tokens.shape
    inner = out_weight.shape[0] * F
    heads = step_weight.shape[1]
    cols = inner // S
    cp = -(-cols // 128) * 128
    WC = 2 * cp + 2 * N + 128
    Dl = D // F
    cr = cp // F
    per = S // F
    bh = Dl // S
    cfg = (S, F, T, D, cp, WC)
    dims = (inner, heads, cols)
    s = lax.axis_index("seq")

    def padc(a, to):
        return jnp.pad(a, [(0, 0)] * (a.ndim - 1) + [(0, to - a.shape[-1])])

    def part(a, start, size, axis):
        return lax.dynamic_slice_in_dim(a, start, size, axis)

    if cols % 128 == 0:
        wsrc = (in_weight,)
    else:
        wsrc = (
            jnp.concatenate(
                [
                    padc(part(in_weight, s * cols, cols, 1), cp),
                    padc(part(in_weight, inner + s * cols, cols, 1), cp),
                    in_weight[:, 2 * inner :],
                ],
                axis=1,
            ),
        )
    if tight(cfg):
        wo = jnp.pad(
            part(out_weight, lax.rem(s, per) * cols, cols, 0), [(0, cp - cols), (0, 0)]
        )
    else:
        wo = out_weight.reshape(per, cols, D)
    flat = (conv_kernel, conv_bias, gate_gain, norm_gain, step_bias, log_decay, skip_gain)
    nt = cp // 128
    scratch = {**vars(fwd_scratch(cfg)), **vars(bwd_scratch(cfg))}
    names = list(scratch)
    outs = dict(
        block=jax.ShapeDtypeStruct((T, D), bf16),
        input=jax.ShapeDtypeStruct((T, D), f32),
        gz=jax.ShapeDtypeStruct((S, Dl, cp), bf16),
        gx=jax.ShapeDtypeStruct((nt, S, Dl, 128), bf16),
        gbc=jax.ShapeDtypeStruct((S, bh, 2 * N), bf16),
        go=jax.ShapeDtypeStruct((F, per, cr, D), bf16),
        go_s=jax.ShapeDtypeStruct((S, cr, D), bf16),
        sm=jax.ShapeDtypeStruct((S, 16, D), bf16),
    )
    on = list(outs)
    nw = 1
    nf = len(flat)

    def kern(tok, cot, wo, step, *rest):
        flat, rest = rest[:nf], rest[nf:]
        O = SimpleNamespace(**dict(zip(on, rest[nw : nw + len(on)])))
        R = SimpleNamespace(**dict(zip(names, rest[nw + len(on) :])))
        if tight(cfg):
            R.bp = R.cot_all
        wogs = body_fwd(cfg, dims, tok, cot, rest[:nw], wo, step, flat, R)
        body_bwd(cfg, dims, tok, cot, wogs, R, O)

    v = pl.BlockSpec(memory_space=pltpu.VMEM)
    hbm = pl.BlockSpec(memory_space=pl.ANY)
    res = pl.pallas_call(
        kern,
        out_shape=[outs[n] for n in on],
        in_specs=[v, v, hbm, v] + [v] * nf + [hbm] * nw,
        out_specs=[v, v] + [hbm] * (len(on) - 2),
        scratch_shapes=[scratch[n] for n in names],
        compiler_params=pltpu.CompilerParams(
            collective_id=0, has_side_effects=True, vmem_limit_bytes=VMEM_LIMIT
        ),
    )(tokens[0], cotangent[0], wo, step_weight.T, *flat, *wsrc)
    G = SimpleNamespace(**dict(zip(on, res)))
    pieces = cols // cr
    steps = per * pieces
    rows = Dl // steps
    cl, gl, hl = (inner + 2 * N) // F, inner // F, heads // F

    def whole(*shape):
        return pl.BlockSpec(shape, lambda i: (0,) * len(shape))

    def out(*shape):
        return jax.ShapeDtypeStruct(shape, f32)

    through = [G.block, G.input] if T % (16 * steps) == 0 else []
    tok_rows = [pl.BlockSpec((T // steps, D), lambda i: (i, 0)) for _ in through]
    joined = pl.pallas_call(
        lambda *refs: assemble(cfg, dims, *refs),
        grid=(steps,),
        out_shape=[
            out(Dl, 2 * inner + 2 * N), out(heads, Dl), out(4, cl), out(cl), out(gl),
            out(Dl), out(hl), out(hl), out(hl), out(per * cols, D),
        ]
        + [jax.ShapeDtypeStruct(a.shape, a.dtype) for a in through],
        in_specs=[
            pl.BlockSpec((S, rows, cp), lambda i: (0, i, 0)),
            pl.BlockSpec((nt, S, rows, 128), lambda i: (0, 0, i, 0)),
            pl.BlockSpec((rows, 2 * N), lambda i: (i, 0)),
            pl.BlockSpec((1, 1, cr, D), lambda i: (lax.rem(i, pieces), i // pieces, 0, 0)),
            whole(S, 16, D),
        ]
        + tok_rows,
        out_specs=[
            pl.BlockSpec((rows, 2 * inner + 2 * N), lambda i: (i, 0)),
            whole(heads, Dl), whole(4, cl), whole(cl), whole(gl), whole(Dl), whole(hl),
            whole(hl), whole(hl),
            pl.BlockSpec((cr, D), lambda i: (i, 0)),
        ]
        + tok_rows,
    )(G.gz, G.gx, G.gbc.reshape(Dl, 2 * N), G.go, G.sm, *through)
    win, stepg, conv, bias, gate, norm, hd0, hd1, hd2, wout = joined[:10]
    block, grad = joined[10:] if through else (G.block, G.input)
    return (
        block[None],
        grad[None],
        win,
        stepg.T,
        conv,
        bias,
        hd0,
        hd1,
        hd2,
        gate,
        norm,
        wout,
    )


def solution(mesh):
    row = P("fsdp", None)
    tok = P("fsdp", "seq", None)
    one = P("fsdp")
    return jax.shard_map(
        shards,
        mesh=mesh,
        in_specs=(tok, row, row, P(None, "fsdp"), one, one, one, one, one, one, row, tok),
        out_specs=(tok, tok, row, row, P(None, "fsdp"), one, one, one, one, one, one, row),
        check_vma=False,
    )
```
